256 devices in a mesh: row: 16 (over x, y), col: 16 (over z, core).
Axes of the slice: x: 4, y: 4, z: 8, core: 2. Of those that a mesh axis runs over, the one named last changes fastest.
Arguments:
- points: bfloat16 [40960, 64], P(('row', 'col')), may hold values from -5 to 5
- start_vectors: bfloat16 [40960, 32], P(('row', 'col')), may hold values from -12 to 12
Outputs:
- basis: float32 [40960, 32], P(('row', 'col'))
The draws below stay inside these ranges and needn't reach their ends.
All inputs are finite; a program needn't handle non-finite values.
Results may differ from the reference program's by a relative error of at most 0.007.
Values may be sent and summed in bfloat16 or wider, within the bound.
A program may use at most 64 MiB of HBM per device.

```python
import jax
import jax.numpy as jnp
from jax import lax

F = 64
K = 32
ITERS = 2
PTS_BLK = 2560
POINTS = 40960


def draw_points(key, part):
    order_key, center_key, noise_key, sigma_key = jax.random.split(jax.random.fold_in(key, 11), 4)
    pairs = POINTS // 2
    order = jax.random.permutation(order_key, POINTS)
    pair_of = jnp.zeros((POINTS,), jnp.int32).at[order].set(jnp.arange(POINTS, dtype=jnp.int32) // 2)
    sigma = jnp.exp(jax.random.uniform(sigma_key, (pairs, 1), jnp.float32, jnp.log(0.15), jnp.log(0.4)))
    centers = jnp.clip(jax.random.normal(center_key, (pairs, F), jnp.float32), -4.0, 4.0)
    noise = jnp.clip(jax.random.normal(noise_key, (POINTS, F), jnp.float32), -3.0, 3.0)
    values = centers[pair_of] + sigma[pair_of] * noise
    return jnp.clip(values, -5.0, 5.0).astype(jnp.bfloat16)


def draw_start_vectors(key, part):
    position = jnp.arange(POINTS, dtype=jnp.float32)[:, None] / POINTS
    base = jnp.clip(jax.random.normal(key, (POINTS, K), jnp.float32), -3.0, 3.0)
    values = base * jnp.exp(jnp.log(4.0) * position)
    return jnp.clip(values, -12.0, 12.0).astype(jnp.bfloat16)


def setup_inputs(seed: int = 0) -> dict:
    key_of = jax.random.split(jax.random.key(seed), 3)
    return {
        "points": draw_points(jax.random.fold_in(key_of[2], 71), 0),
        "start_vectors": draw_start_vectors(jax.random.fold_in(key_of[2], 71), 0),
    }


KERNEL_SCALE = 5.12

def kernel_block(block_pts, block_sq, all_pts, all_sq):
    cross = jnp.dot(block_pts.astype(jnp.float32), all_pts.T.astype(jnp.float32), preferred_element_type=jnp.float32)
    dist = block_sq[:, None] + all_sq[None, :] - 2.0 * cross
    return jnp.exp(dist * (-KERNEL_SCALE / F)).astype(jnp.bfloat16)

def reference(points, start_vectors):
    sq_norms = jnp.sum(jnp.square(points.astype(jnp.float32)), axis=1)
    height = min(512, PTS_BLK)
    count = POINTS // height
    stacked = (points.reshape(count, height, F), sq_norms.reshape(count, height))

    def degree_block(item):
        weights = kernel_block(item[0], item[1], points, sq_norms)
        return jnp.sum(weights, axis=1, dtype=jnp.float32)
    degree = lax.map(degree_block, stacked).reshape(POINTS)
    vectors = start_vectors
    ortho = jnp.zeros((POINTS, K), jnp.float32)
    for step in range(ITERS):

        def product_block(item, panel=vectors):
            weights = kernel_block(item[0], item[1], points, sq_norms)
            return jnp.dot(weights.astype(jnp.float32), panel.astype(jnp.float32), preferred_element_type=jnp.float32)
        product = lax.map(product_block, stacked).reshape(POINTS, K)
        scaled = product / degree[:, None]
        gram = jnp.dot(scaled.T.astype(jnp.float32), scaled.astype(jnp.float32), precision=lax.Precision.HIGHEST, preferred_element_type=jnp.float32) / POINTS
        lower = jnp.linalg.cholesky(gram)
        ortho = lax.linalg.triangular_solve(lower, scaled, left_side=False, lower=True, transpose_a=True)
        vectors = ortho.astype(jnp.bfloat16)
    return ortho
```

```python
import functools
import math

import jax
import jax.numpy as jnp
from jax import lax
from jax.experimental import pallas as pl
from jax.experimental.pallas import tpu as pltpu
from jax.sharding import PartitionSpec as P

MESH = pl.DeviceIdType.MESH
F32 = jnp.float32
BF16 = jnp.bfloat16
HIGHEST = lax.Precision.HIGHEST

KERNEL_SCALE = 5.12
F = 64
K = 32
OWN = 160
LANES = 128
TAIL = OWN - LANES
GROUP = 4 * OWN
NZ = 8
NX = 4
NY = 4
NXY = NX * NY
NCOL = 2 * NZ
ROWS_I = NZ * OWN
COLS_J = 2 * NXY * OWN
TOTAL = 256 * OWN


def lane_block():
    return lax.broadcasted_iota(jnp.int32, (8, LANES), 1) // TAIL


def roll_lanes(x, shift):
    shift = shift % LANES
    return x if shift == 0 else pltpu.roll(x, shift, 1)


def pick(blocks, pieces):
    out = pieces[3]
    for b in (2, 1, 0):
        out = jnp.where(blocks == b, pieces[b], out)
    return out


def transposed_blocks(tiles):
    rows = tiles[0].shape[0]
    blocks = lax.broadcasted_iota(jnp.int32, (rows, LANES), 1) // TAIL
    return [
        pick(blocks, [roll_lanes(tiles[b], TAIL * (b - g)) for b in range(4)]) for g in range(4)
    ]


def packed_tail(tail, rows):
    groups = tail.shape[0] // rows
    return sum(roll_lanes(tail[g * rows : (g + 1) * rows], TAIL * g) for g in range(groups))


def unpacked_tail(packed, groups):
    rows = packed.shape[0]
    keep = lax.broadcasted_iota(jnp.int32, (rows, LANES), 1) < TAIL
    return jnp.concatenate(
        [jnp.where(keep, roll_lanes(packed, -TAIL * g), 0.0) for g in range(groups)], axis=0
    )


def bf16_pieces(x):
    hi = x.astype(BF16).astype(F32)
    rest = x - hi
    mid = rest.astype(BF16).astype(F32)
    return hi, mid, rest - mid


def extended(x, for_rows):
    hi, mid, lo = bf16_pieces(jnp.sum(x * x, axis=0, keepdims=True))
    r = lax.broadcasted_iota(jnp.int32, (8, LANES), 0)
    if for_rows:
        x = 2.0 * x
        head = jnp.where(r == 3, -hi, jnp.where(r == 4, -mid, jnp.where(r == 5, -lo, 0.0)))
        extra = jnp.where(r < 3, -1.0, head)
    else:
        head = jnp.where(r == 0, hi, jnp.where(r == 1, mid, jnp.where(r == 2, lo, 0.0)))
        extra = jnp.where((r >= 3) & (r < 6), 1.0, head)
    return jnp.concatenate([x, extra, jnp.zeros((LANES - F - 8, LANES), F32)], axis=0)


def eliminate(gram, right):
    cols = [jnp.broadcast_to(gram[:, m : m + 1], (K, LANES)) for m in range(K)]
    width = right.shape[1] // LANES
    sub = lax.broadcasted_iota(jnp.int32, (8, LANES), 0)
    cols = [[c[8 * g : 8 * g + 8] for g in range(4)] for c in cols]
    rt = [
        [right[8 * g : 8 * g + 8, w * LANES : (w + 1) * LANES] for w in range(width)]
        for g in range(4)
    ]
    out_rows = []
    for k in range(K):
        kg, kr = k // 8, k % 8
        pivot = cols[k][kg][kr : kr + 1]
        inv = 1.0 / pivot
        factor = [None] * 4
        for g in range(kg, 4):
            f = cols[k][g] * inv
            if g == kg:
                f = jnp.where(sub > kr, f, 0.0)
            factor[g] = f
        for m in range(k + 1, K):
            mg, mr = m // 8, m % 8
            upper = cols[k][mg][mr : mr + 1]
            for g in range(mg, 4):
                cols[m][g] = cols[m][g] - factor[g] * upper
        rows = [rt[kg][w][kr : kr + 1] for w in range(width)]
        scale = lax.rsqrt(pivot)
        out_rows.append([row * scale for row in rows])
        for g in range(kg, 4):
            for w in range(width):
                rt[g][w] = rt[g][w] - factor[g] * rows[w]
    tiles = []
    for g in range(4):
        tile = []
        for w in range(width):
            acc = jnp.broadcast_to(out_rows[8 * g][w], (8, LANES))
            for r in range(1, 8):
                acc = jnp.where(sub == r, out_rows[8 * g + r][w], acc)
            tile.append(acc)
        tiles.append(jnp.concatenate(tile, axis=1) if width > 1 else tile[0])
    return jnp.concatenate(tiles, axis=0)


def kernel(
    pts_ref, vec_ref, out_ref,
    stage, zbuf, jbuf, xi, xj, panel, aff, acc, psend, precv, sbuf, gsend, grecv,
    z_s, z_r, xy_s, xy_r, f_s, f_r, p_s, p_r, s_s, s_r, sf_s, sf_r, ga_s, ga_r, gb_s, gb_r,
):
    row = lax.axis_index("row")
    col = lax.axis_index("col")
    x, y = row // NY, lax.rem(row, NY)
    z, core = col // 2, lax.rem(col, 2)

    def xy_peer(e):
        to_x = lax.rem(x + e // NY, NX)
        to_y = lax.rem(y + e % NY, NY)
        return (to_x * NY + to_y, col)

    def z_peer(d):
        return (row, lax.rem(z + d + NZ, NZ) * 2 + core)

    def col_peer(d):
        return (row, lax.rem(col + d, NCOL))

    partner = (row, z * 2 + 1 - core)

    def remote(src, dst, send, recv, to):
        return pltpu.make_async_remote_copy(
            src_ref=src, dst_ref=dst, send_sem=send, recv_sem=recv,
            device_id=to, device_id_type=MESH,
        )

    barrier = pltpu.get_barrier_semaphore()
    for d in range(1, NCOL):
        pl.semaphore_signal(barrier, inc=1, device_id=col_peer(d), device_id_type=MESH)
    for e in range(1, NXY):
        pl.semaphore_signal(barrier, inc=1, device_id=xy_peer(e), device_id_type=MESH)

    stage[...] = jnp.zeros_like(stage)
    stage[0:OWN, 0:F] = pts_ref[...].astype(F32)
    stage[0:OWN, F : F + K] = vec_ref[...].astype(F32)
    t = stage[...].T
    jbuf[0, 0, 0:64, :] = t[0:F, 0:LANES].astype(BF16)
    jbuf[0, 0, 64:80, :] = packed_tail(t[0:F, LANES:], 16).astype(BF16)
    jbuf[0, 0, 80:112, :] = t[F : F + K, 0:LANES].astype(BF16)
    jbuf[0, 0, 112:128, :] = packed_tail(t[F : F + K, LANES:], 16).astype(BF16)

    pl.semaphore_wait(barrier, NCOL - 1 + NXY - 1)

    def z_copy(d):
        return remote(jbuf.at[0, 0, pl.ds(0, 80)], zbuf.at[d], z_s.at[d], z_r.at[d], z_peer(d))

    def xy_copy(e):
        return remote(jbuf.at[0, 0], jbuf.at[0, e], xy_s.at[e], xy_r.at[e], xy_peer(e))

    def forward(e):
        return remote(jbuf.at[0, e], jbuf.at[1, e], f_s.at[e], f_r.at[e], partner)

    for d in range(1, NZ):
        z_copy(d).start()
    for e in range(1, NXY):
        xy_copy(e).start()
    forward(0).start()

    def tails_of(tiles):
        return transposed_blocks([tile.astype(F32) for tile in tiles])

    for d in range(NZ):
        if d == 0:
            src = jbuf[0, 0, 0:64, :]
        else:
            z_copy(d).wait_recv()
            src = zbuf[d, 0:64, :]
        xi[:, d * LANES : (d + 1) * LANES] = extended(src.astype(F32), True).astype(BF16)
    for q in range(NZ // 4):
        tiles = [
            jbuf[0, 0, 64:80, :] if 4 * q + b == 0 else zbuf[4 * q + b, 64:80, :] for b in range(4)
        ]
        tile = jnp.concatenate(tails_of(tiles), axis=0)
        at = NZ * LANES + q * LANES
        xi[:, at : at + LANES] = extended(tile, True).astype(BF16)

    ones_row = (lax.broadcasted_iota(jnp.int32, (16, GROUP), 0) == 0).astype(F32).astype(BF16)

    def group_of(half, q):
        base = pl.multiple_of((half * 4 + q) * GROUP, GROUP)
        first = q * 4
        for b in range(4):
            src = jbuf[half, first + b, 0:64, :].astype(F32)
            xj[pl.ds(base + b * LANES, LANES), :] = extended(src, False).T.astype(BF16)
            panel[0:K, pl.ds(base + b * LANES, LANES)] = jbuf[half, first + b, 80:112, :]
        tile = jnp.concatenate(tails_of([jbuf[half, first + b, 64:80, :] for b in range(4)]), axis=0)
        xj[pl.ds(base + 4 * LANES, LANES), :] = extended(tile, False).T.astype(BF16)
        tile = tails_of([jbuf[half, first + b, 112:128, :] for b in range(4)])[0:2]
        panel[0:K, pl.ds(base + 4 * LANES, LANES)] = jnp.concatenate(tile, axis=0).astype(BF16)
        panel[K : K + 16, pl.ds(base, GROUP)] = ones_row
        for c in range(ROWS_I // 256):
            dist = jnp.dot(
                xj[pl.ds(base, GROUP), :],
                xi[:, c * 256 : (c + 1) * 256],
                preferred_element_type=F32,
            )
            weights = jnp.exp2(dist * (KERNEL_SCALE / F * math.log2(math.e)))
            aff[pl.ds(base, GROUP), c * 256 : (c + 1) * 256] = weights.astype(BF16)

    def direct(q, carry):
        for b in range(4):
            e = q * 4 + b

            @pl.when(e > 0)
            def _():
                xy_copy(e).wait_recv()
                forward(e).start()

        group_of(0, q)
        return carry

    def forwarded(q, carry):
        for b in range(4):
            forward(q * 4 + b).wait_recv()
        group_of(1, q)
        return carry

    lax.fori_loop(0, 4, direct, 0)
    lax.fori_loop(0, 4, forwarded, 0)

    def product(rows):
        acc[0:rows, :] = jnp.zeros((rows, ROWS_I), F32)

        def step(s, carry):
            at = pl.multiple_of(s * 2 * GROUP, 2 * GROUP)
            acc[0:rows, :] += jnp.dot(
                panel[0:rows, pl.ds(at, 2 * GROUP)],
                aff[pl.ds(at, 2 * GROUP), :],
                preferred_element_type=F32,
            )
            return carry

        lax.fori_loop(0, COLS_J // (2 * GROUP), step, 0)

    blocks8 = lane_block()

    def p_copy(it, d):
        return remote(
            psend.at[it, d], precv.at[it, d], p_s.at[it, d], p_r.at[it, d], z_peer(-d)
        )

    def reduce_product(it, with_degree):
        for q in range(NZ // 4):
            at = NZ * LANES + q * LANES
            tail = acc[0:K, at : at + LANES]
            if it == 1:
                tail = tail + acc[K : 2 * K, at : at + LANES]
            packed = [
                pick(blocks8, [roll_lanes(tail[8 * g : 8 * g + 8], TAIL * (g - b)) for g in range(4)])
                for b in range(4)
            ]
            for b in range(4):
                d = 4 * q + b
                main = acc[0:K, d * LANES : (d + 1) * LANES]
                if it == 1:
                    main = main + acc[K : 2 * K, d * LANES : (d + 1) * LANES]
                psend[it, d, 0:K, :] = main
                psend[it, d, K : K + 8, :] = packed[b]
                if with_degree:
                    psend[it, d, K + 8 : K + 9, :] = acc[K : K + 1, d * LANES : (d + 1) * LANES]
                    psend[it, d, K + 9 : K + 10, :] = roll_lanes(
                        acc[K : K + 8, at : at + LANES], -TAIL * b
                    )[0:1]
                    psend[it, d, K + 10 : K + 16, :] = jnp.zeros((6, LANES), F32)
                else:
                    psend[it, d, K + 8 : K + 16, :] = jnp.zeros((8, LANES), F32)
        for d in range(1, NZ):
            p_copy(it, d).start()
        total = psend[it, 0]
        for d in range(1, NZ):
            p_copy(it, d).wait_recv()
            total = total + precv[it, d]
        return total

    def gram_of(scaled):
        wide = jnp.concatenate([scaled, jnp.zeros((LANES - K, 2 * LANES), F32)], axis=0)
        part = lax.dot_general(
            scaled, wide, (((1,), (1,)), ((), ())), precision=HIGHEST, preferred_element_type=F32
        )
        return packed_tail(part, 8)

    def ga_copy(it, d):
        return remote(gsend.at[it, 0], grecv.at[it, 0, d], ga_s.at[it, d], ga_r.at[it, d], col_peer(d))

    def gb_copy(it, e):
        return remote(gsend.at[it, 1], grecv.at[it, 1, e], gb_s.at[it, e], gb_r.at[it, e], xy_peer(e))

    def gram_first(it, scaled):
        gsend[it, 0] = gram_of(scaled)
        for d in range(1, NCOL):
            ga_copy(it, d).start()

    def gram_second(it):
        total = gsend[it, 0]
        for d in range(1, NCOL):
            ga_copy(it, d).wait_recv()
            total = total + grecv[it, 0, d]
        gsend[it, 1] = total
        for e in range(1, NXY):
            gb_copy(it, e).start()

    def gram_last(it):
        total = gsend[it, 1]
        for e in range(1, NXY):
            gb_copy(it, e).wait_recv()
            total = total + grecv[it, 1, e]
        return unpacked_tail(total, 4) * (1.0 / TOTAL)

    def s_copy(e):
        return remote(sbuf.at[0, 0], sbuf.at[0, e], s_s.at[e], s_r.at[e], xy_peer(e))

    def s_forward(e):
        return remote(sbuf.at[0, e], sbuf.at[1, e], sf_s.at[e], sf_r.at[e], partner)

    product(K + 16)
    total = reduce_product(0, True)
    keep = lax.broadcasted_iota(jnp.int32, (K, LANES), 1) < TAIL
    deg_main = total[K + 8 : K + 9]
    deg_tail = jnp.where(keep[0:1], total[K + 9 : K + 10], 1.0)
    scaled_main = total[0:K] / deg_main
    scaled_tail = unpacked_tail(total[K : K + 8], 4) / deg_tail
    scaled = jnp.concatenate([scaled_main, scaled_tail], axis=1)

    hi = scaled.astype(BF16).astype(F32)
    lo = scaled - hi
    both = jnp.concatenate([hi, lo], axis=0)
    sbuf[0, 0, 0:64, :] = both[:, 0:LANES].astype(BF16)
    sbuf[0, 0, 64:80, :] = packed_tail(both[:, LANES:], 16).astype(BF16)
    for e in range(1, NXY):
        s_copy(e).start()
    s_forward(0).start()
    gram_first(0, scaled)
    for e in range(1, NXY):
        s_copy(e).wait_recv()
        s_forward(e).start()
    gram_second(0)

    def fill(half, q, carry):
        base = pl.multiple_of((half * 4 + q) * GROUP, GROUP)
        first = q * 4
        for b in range(4):
            panel[0 : 2 * K, pl.ds(base + b * LANES, LANES)] = sbuf[half, first + b, 0:64, :]
        tile = tails_of([sbuf[half, first + b, 64:80, :] for b in range(4)])
        panel[0 : 2 * K, pl.ds(base + 4 * LANES, LANES)] = jnp.concatenate(tile, axis=0).astype(BF16)
        return carry

    lax.fori_loop(0, 4, functools.partial(fill, 0), 0)
    for e in range(NXY):
        s_forward(e).wait_recv()
    lax.fori_loop(0, 4, functools.partial(fill, 1), 0)

    product(2 * K)
    eye = (
        lax.broadcasted_iota(jnp.int32, (K, LANES), 0)
        == lax.broadcasted_iota(jnp.int32, (K, LANES), 1)
    ).astype(F32)
    total = reduce_product(1, False)
    inverse = eliminate(gram_last(0), eye)
    scaled = jnp.concatenate([total[0:K] / deg_main, unpacked_tail(total[K : K + 8], 4) / deg_tail], axis=1)
    tall = jnp.concatenate([scaled, jnp.zeros((LANES - K, 2 * LANES), F32)], axis=0)
    scaled = jnp.dot(inverse, tall, precision=HIGHEST, preferred_element_type=F32)
    gram_first(1, scaled)
    gram_second(1)
    ortho = eliminate(gram_last(1), scaled)
    wide = jnp.concatenate([ortho, jnp.zeros((LANES - K, 2 * LANES), F32)], axis=0)
    out_ref[...] = wide.T[0:OWN, 0:K]

    for d in range(1, NZ):
        z_copy(d).wait_send()
        for it in range(2):
            p_copy(it, d).wait_send()
    for e in range(NXY):
        forward(e).wait_send()
        s_forward(e).wait_send()
    for e in range(1, NXY):
        xy_copy(e).wait_send()
        s_copy(e).wait_send()
        for it in range(2):
            ga_copy(it, e).wait_send()
            gb_copy(it, e).wait_send()


def solution(mesh):
    dma = pltpu.SemaphoreType.DMA

    def shards(points, start_vectors):
        return pl.pallas_call(
            kernel,
            out_shape=jax.ShapeDtypeStruct((OWN, K), F32),
            in_specs=[pl.BlockSpec(memory_space=pltpu.VMEM)] * 2,
            out_specs=pl.BlockSpec(memory_space=pltpu.VMEM),
            scratch_shapes=[
                pltpu.VMEM((2 * LANES, LANES), F32),
                pltpu.VMEM((NZ, 80, LANES), BF16),
                pltpu.VMEM((2, NXY, LANES, LANES), BF16),
                pltpu.VMEM((LANES, ROWS_I), BF16),
                pltpu.VMEM((COLS_J, LANES), BF16),
                pltpu.VMEM((2 * K, COLS_J), BF16),
                pltpu.VMEM((COLS_J, ROWS_I), BF16),
                pltpu.VMEM((2 * K, ROWS_I), F32),
                pltpu.VMEM((2, NZ, K + 16, LANES), F32),
                pltpu.VMEM((2, NZ, K + 16, LANES), F32),
                pltpu.VMEM((2, NXY, 80, LANES), BF16),
                pltpu.VMEM((2, 2, 8, LANES), F32),
                pltpu.VMEM((2, 2, 16, 8, LANES), F32),
                dma((NZ,)), dma((NZ,)),
                dma((NXY,)), dma((NXY,)),
                dma((NXY,)), dma((NXY,)),
                dma((2, NZ)), dma((2, NZ)),
                dma((NXY,)), dma((NXY,)),
                dma((NXY,)), dma((NXY,)),
                dma((2, NCOL)), dma((2, NCOL)),
                dma((2, NXY)), dma((2, NXY)),
            ],
            compiler_params=pltpu.CompilerParams(
                collective_id=0, has_side_effects=True, vmem_limit_bytes=48 * 1024 * 1024
            ),
        )(points, start_vectors)

    spec = P(("row", "col"), None)
    return jax.shard_map(
        shards, mesh=mesh, in_specs=(spec, spec), out_specs=spec, check_vma=False
    )
```

```python
import functools
import math

import jax
import jax.numpy as jnp
from jax import lax
from jax.experimental import pallas as pl
from jax.experimental.pallas import tpu as pltpu
from jax.sharding import PartitionSpec as P

MESH = pl.DeviceIdType.MESH
F32 = jnp.float32
BF16 = jnp.bfloat16
HIGHEST = lax.Precision.HIGHEST

KERNEL_SCALE = 5.12
F = 64
K = 32
OWN = 160
LANES = 128
TAIL = OWN - LANES
GROUP = 4 * OWN
NZ = 8
NX = 4
NY = 4
NXY = NX * NY
NCOL = 2 * NZ
ROWS_I = NZ * OWN
COLS_J = 2 * NXY * OWN
TOTAL = 256 * OWN


def lane_block():
    return lax.broadcasted_iota(jnp.int32, (8, LANES), 1) // TAIL


def roll_lanes(x, shift):
    shift = shift % LANES
    return x if shift == 0 else pltpu.roll(x, shift, 1)


def pick(blocks, pieces):
    out = pieces[3]
    for b in (2, 1, 0):
        out = jnp.where(blocks == b, pieces[b], out)
    return out


def transposed_blocks(tiles):
    rows = tiles[0].shape[0]
    blocks = lax.broadcasted_iota(jnp.int32, (rows, LANES), 1) // TAIL
    return [
        pick(blocks, [roll_lanes(tiles[b], TAIL * (b - g)) for b in range(4)]) for g in range(4)
    ]


def packed_tail(tail, rows):
    groups = tail.shape[0] // rows
    return sum(roll_lanes(tail[g * rows : (g + 1) * rows], TAIL * g) for g in range(groups))


def unpacked_tail(packed, groups):
    rows = packed.shape[0]
    keep = lax.broadcasted_iota(jnp.int32, (rows, LANES), 1) < TAIL
    return jnp.concatenate(
        [jnp.where(keep, roll_lanes(packed, -TAIL * g), 0.0) for g in range(groups)], axis=0
    )


def bf16_pieces(x):
    hi = x.astype(BF16).astype(F32)
    rest = x - hi
    mid = rest.astype(BF16).astype(F32)
    return hi, mid, rest - mid


def extended(x, for_rows):
    hi, mid, lo = bf16_pieces(jnp.sum(x * x, axis=0, keepdims=True))
    r = lax.broadcasted_iota(jnp.int32, (8, LANES), 0)
    if for_rows:
        x = 2.0 * x
        head = jnp.where(r == 3, -hi, jnp.where(r == 4, -mid, jnp.where(r == 5, -lo, 0.0)))
        extra = jnp.where(r < 3, -1.0, head)
    else:
        head = jnp.where(r == 0, hi, jnp.where(r == 1, mid, jnp.where(r == 2, lo, 0.0)))
        extra = jnp.where((r >= 3) & (r < 6), 1.0, head)
    return jnp.concatenate([x, extra, jnp.zeros((LANES - F - 8, LANES), F32)], axis=0)


def eliminate(gram, right):
    cols = [jnp.broadcast_to(gram[:, m : m + 1], (K, LANES)) for m in range(K)]
    width = right.shape[1] // LANES
    sub = lax.broadcasted_iota(jnp.int32, (8, LANES), 0)
    cols = [[c[8 * g : 8 * g + 8] for g in range(4)] for c in cols]
    rt = [
        [right[8 * g : 8 * g + 8, w * LANES : (w + 1) * LANES] for w in range(width)]
        for g in range(4)
    ]
    out_rows = []
    for k in range(K):
        kg, kr = k // 8, k % 8
        pivot = cols[k][kg][kr : kr + 1]
        inv = 1.0 / pivot
        factor = [None] * 4
        for g in range(kg, 4):
            f = cols[k][g] * inv
            if g == kg:
                f = jnp.where(sub > kr, f, 0.0)
            factor[g] = f
        for m in range(k + 1, K):
            mg, mr = m // 8, m % 8
            upper = cols[k][mg][mr : mr + 1]
            for g in range(mg, 4):
                cols[m][g] = cols[m][g] - factor[g] * upper
        rows = [rt[kg][w][kr : kr + 1] for w in range(width)]
        scale = lax.rsqrt(pivot)
        out_rows.append([row * scale for row in rows])
        for g in range(kg, 4):
            for w in range(width):
                rt[g][w] = rt[g][w] - factor[g] * rows[w]
    tiles = []
    for g in range(4):
        tile = []
        for w in range(width):
            acc = jnp.broadcast_to(out_rows[8 * g][w], (8, LANES))
            for r in range(1, 8):
                acc = jnp.where(sub == r, out_rows[8 * g + r][w], acc)
            tile.append(acc)
        tiles.append(jnp.concatenate(tile, axis=1) if width > 1 else tile[0])
    return jnp.concatenate(tiles, axis=0)


def kernel(
    pts_hbm, vec_hbm, out_ref,
    pts_ref, vec_ref, stage, zbuf, jbuf, vbuf, xi, xj, panel, aff, acc, psend, precv, sbuf, gsend, grecv,
    in_s, z_s, z_r, xy_s, xy_r, f_s, f_r, v_s, v_r, vf_s, vf_r,
    p_s, p_r, s_s, s_r, sf_s, sf_r, ga_s, ga_r, gb_s, gb_r,
):
    row = lax.axis_index("row")
    col = lax.axis_index("col")
    x, y = row // NY, lax.rem(row, NY)
    z, core = col // 2, lax.rem(col, 2)

    def xy_peer(e):
        q = e // NY
        to_x = lax.rem(x + q + (q // 2) * (5 - 2 * q), NX)
        to_y = lax.rem(y + e % NY, NY)
        return (to_x * NY + to_y, col)

    def z_peer(d):
        return (row, lax.rem(z + d + NZ, NZ) * 2 + core)

    def col_peer(d):
        return (row, lax.rem(col + d, NCOL))

    partner = (row, z * 2 + 1 - core)

    def remote(src, dst, send, recv, to):
        return pltpu.make_async_remote_copy(
            src_ref=src, dst_ref=dst, send_sem=send, recv_sem=recv,
            device_id=to, device_id_type=MESH,
        )

    pts_copy = pltpu.make_async_copy(pts_hbm, pts_ref, in_s.at[0])
    vec_copy = pltpu.make_async_copy(vec_hbm, vec_ref, in_s.at[1])
    pts_copy.start()
    vec_copy.start()
    barrier = pltpu.get_barrier_semaphore()
    with jax.named_scope("signal"):
        for d in range(1, NCOL):
            pl.semaphore_signal(barrier, inc=1, device_id=col_peer(d), device_id_type=MESH)
        for e in range(1, NXY):
            pl.semaphore_signal(barrier, inc=1, device_id=xy_peer(e), device_id_type=MESH)

    with jax.named_scope("prepare"):
        stage[...] = jnp.zeros_like(stage)
        pts_copy.wait()
        vec_copy.wait()
        stage[0:F, 0:OWN] = pts_ref[...].astype(F32)
        stage[F : F + K, 0:OWN] = vec_ref[...].astype(F32)
        t = stage[...]
        jbuf[0, 0, 0:64, :] = t[0:F, 0:LANES].astype(BF16)
        jbuf[0, 0, 64:80, :] = packed_tail(t[0:F, LANES:], 16).astype(BF16)
        vbuf[0, 0, 0:32, :] = t[F : F + K, 0:LANES].astype(BF16)
        vbuf[0, 0, 32:48, :] = packed_tail(t[F : F + K, LANES:], 16).astype(BF16)
        acc[...] = jnp.zeros_like(acc)
        for h in range(COLS_J // GROUP):
            panel[K : K + 16, h * GROUP : (h + 1) * GROUP] = (
                lax.broadcasted_iota(jnp.int32, (16, GROUP), 0) == 0
            ).astype(F32).astype(BF16)

    with jax.named_scope("barrier_wait"):
        pl.semaphore_wait(barrier, NCOL - 1 + NXY - 1)

    def z_copy(d):
        return remote(jbuf.at[0, 0], zbuf.at[d], z_s.at[d], z_r.at[d], z_peer(d))

    def xy_copy(e):
        return remote(jbuf.at[0, 0], jbuf.at[0, e], xy_s.at[e], xy_r.at[e], xy_peer(e))

    def forward(e):
        return remote(jbuf.at[0, e], jbuf.at[1, e], f_s.at[e], f_r.at[e], partner)

    def v_copy(e):
        return remote(vbuf.at[0, 0], vbuf.at[0, e], v_s.at[e], v_r.at[e], xy_peer(e))

    def v_forward(e):
        return remote(vbuf.at[0, e], vbuf.at[1, e], vf_s.at[e], vf_r.at[e], partner)

    def s_copy(e):
        return remote(sbuf.at[0, 0], sbuf.at[0, e], s_s.at[e], s_r.at[e], xy_peer(e))

    def s_forward(e):
        return remote(sbuf.at[0, e], sbuf.at[1, e], sf_s.at[e], sf_r.at[e], partner)

    def pass_on(q, copies):
        for copy, onward in copies:
            for b in range(4):
                e = q * 4 + b

                if isinstance(q, int):
                    if e > 0:
                        copy(e).wait_recv()
                    onward(e).start()
                else:
                    copy(e).wait_recv()
                    onward(e).start()

    def in_groups(copies, work, name):
        with jax.named_scope(name + "_first"):
            pass_on(0, copies)

        def step(q, carry):
            with jax.named_scope(name + "_wait"):
                pass_on(q + 1, copies)
                for _, onward in copies:
                    for b in range(4):
                        onward(q * 4 + b).wait_recv()
            with jax.named_scope(name + "_work"):
                work(q)
            return carry

        lax.fori_loop(0, 3, step, 0)
        with jax.named_scope(name + "_lastwait"):
            for _, onward in copies:
                for b in range(4):
                    onward(12 + b).wait_recv()
        with jax.named_scope(name + "_lastwork"):
            work(3)

    with jax.named_scope("send_points"):
        for d in (4, 3, 5, 2, 6, 1, 7):
            z_copy(d).start()
        for e in range(1, NXY):
            xy_copy(e).start()
        for e in range(1, NXY):
            v_copy(e).start()

    def tails_of(tiles):
        return transposed_blocks([tile.astype(F32) for tile in tiles])

    with jax.named_scope("row_side"):
        for d in range(NZ):
            if d == 0:
                src = jbuf[0, 0, 0:64, :]
            else:
                z_copy(d).wait_recv()
                src = zbuf[d, 0:64, :]
            xi[:, d * LANES : (d + 1) * LANES] = extended(src.astype(F32), True).astype(BF16)
        for q in range(NZ // 4):
            tiles = [
                jbuf[0, 0, 64:80, :] if 4 * q + b == 0 else zbuf[4 * q + b, 64:80, :]
                for b in range(4)
            ]
            tile = jnp.concatenate(tails_of(tiles), axis=0)
            at = NZ * LANES + q * LANES
            xi[:, at : at + LANES] = extended(tile, True).astype(BF16)

    def first_work(q):
        base = pl.multiple_of(q * 2 * GROUP, 2 * GROUP)
        for half in range(2):
            for b in range(4):
                e = q * 4 + b
                at = half * GROUP + b * LANES
                src = jbuf[half, e, 0:64, :].astype(F32)
                xj[at : at + LANES, :] = extended(src, False).T.astype(BF16)
                panel[0:K, pl.ds(base + at, LANES)] = vbuf[half, e, 0:32, :]
            at = half * GROUP + 4 * LANES
            tile = tails_of([jbuf[half, q * 4 + b, 64:80, :] for b in range(4)])
            xj[at : at + LANES, :] = extended(jnp.concatenate(tile, axis=0), False).T.astype(BF16)
            tile = tails_of([vbuf[half, q * 4 + b, 32:48, :] for b in range(4)])[0:2]
            panel[0:K, pl.ds(base + at, LANES)] = jnp.concatenate(tile, axis=0).astype(BF16)
        vectors = panel[0 : K + 16, pl.ds(base, 2 * GROUP)]
        for c in range(ROWS_I // 256):
            here = slice(c * 256, (c + 1) * 256)
            dist = jnp.dot(xj[...], xi[:, here], preferred_element_type=F32)
            weights = jnp.exp2(dist * (KERNEL_SCALE / F * math.log2(math.e))).astype(BF16)
            aff[pl.ds(base, 2 * GROUP), here] = weights
            acc[0 : K + 16, here] += jnp.dot(vectors, weights, preferred_element_type=F32)

    in_groups([(xy_copy, forward), (v_copy, v_forward)], first_work, "a")

    blocks8 = lane_block()

    def p_copy(it, d):
        rows = K + 16 - 8 * it
        return remote(
            psend.at[it, d, pl.ds(0, rows)], precv.at[it, d, pl.ds(0, rows)],
            p_s.at[it, d], p_r.at[it, d], z_peer(-d),
        )

    def send_product(it):
        for q in range(NZ // 4):
            at = NZ * LANES + q * LANES
            tail = acc[0:K, at : at + LANES]
            if it == 1:
                tail = tail + acc[K : 2 * K, at : at + LANES]
            packed = [
                pick(blocks8, [roll_lanes(tail[8 * g : 8 * g + 8], TAIL * (g - b)) for g in range(4)])
                for b in range(4)
            ]
            for b in range(4):
                d = 4 * q + b
                main = acc[0:K, d * LANES : (d + 1) * LANES]
                if it == 1:
                    main = main + acc[K : 2 * K, d * LANES : (d + 1) * LANES]
                psend[it, d, 0:K, :] = main
                psend[it, d, K : K + 8, :] = packed[b]
                if it == 0:
                    psend[it, d, K + 8 : K + 9, :] = acc[K : K + 1, d * LANES : (d + 1) * LANES]
                    psend[it, d, K + 9 : K + 10, :] = roll_lanes(
                        acc[K : K + 8, at : at + LANES], -TAIL * b
                    )[0:1]
                    psend[it, d, K + 10 : K + 16, :] = jnp.zeros((6, LANES), F32)
        for d in (4, 3, 5, 2, 6, 1, 7):
            p_copy(it, d).start()

    def received_product(it):
        rows = K + 16 - 8 * it
        total = psend[it, 0, 0:rows]
        for d in (1, 7, 2, 6, 3, 5, 4):
            p_copy(it, d).wait_recv()
            total = total + precv[it, d, 0:rows]
        return total

    def gram_of(scaled):
        wide = jnp.concatenate([scaled, jnp.zeros((LANES - K, 2 * LANES), F32)], axis=0)
        part = lax.dot_general(
            scaled, wide, (((1,), (1,)), ((), ())), precision=HIGHEST, preferred_element_type=F32
        )
        return packed_tail(part, 8)

    def ga_copy(it, d):
        return remote(gsend.at[it, 0], grecv.at[it, 0, d], ga_s.at[it, d], ga_r.at[it, d], col_peer(d))

    def gb_copy(it, e):
        return remote(gsend.at[it, 1], grecv.at[it, 1, e], gb_s.at[it, e], gb_r.at[it, e], xy_peer(e))

    def gram_first(it, scaled):
        gsend[it, 0] = gram_of(scaled)
        for d in range(1, NCOL):
            ga_copy(it, d).start()

    def gram_second(it):
        total = gsend[it, 0]
        for d in range(1, NCOL):
            ga_copy(it, d).wait_recv()
            total = total + grecv[it, 0, d]
        gsend[it, 1] = total
        for e in range(1, NXY):
            gb_copy(it, e).start()

    def gram_last(it):
        total = gsend[it, 1]
        for e in range(1, NXY):
            gb_copy(it, e).wait_recv()
            total = total + grecv[it, 1, e]
        return unpacked_tail(total, 4) * (1.0 / TOTAL)

    with jax.named_scope("send1"):
        send_product(0)
    with jax.named_scope("reduce1"):
        total = received_product(0)
    with jax.named_scope("scale1"):
        keep = lax.broadcasted_iota(jnp.int32, (1, LANES), 1) < TAIL
        deg_main = total[K + 8 : K + 9]
        deg_tail = jnp.where(keep, total[K + 9 : K + 10], 1.0)
        scaled_main = total[0:K] / deg_main
        scaled_tail = unpacked_tail(total[K : K + 8], 4) / deg_tail
        scaled = jnp.concatenate([scaled_main, scaled_tail], axis=1)

        hi = scaled.astype(BF16).astype(F32)
        lo = scaled - hi
        both = jnp.concatenate([hi, lo], axis=0)
        sbuf[0, 0, 0:64, :] = both[:, 0:LANES].astype(BF16)
        sbuf[0, 0, 64:80, :] = packed_tail(both[:, LANES:], 16).astype(BF16)
        for e in range(1, NXY):
            s_copy(e).start()
    with jax.named_scope("gram_first1"):
        gram_first(0, scaled)
        acc[...] = jnp.zeros_like(acc)

    def second_work(q):
        base = pl.multiple_of(q * 2 * GROUP, 2 * GROUP)
        for half in range(2):
            for b in range(4):
                at = base + half * GROUP + b * LANES
                panel[0 : 2 * K, pl.ds(at, LANES)] = sbuf[half, q * 4 + b, 0:64, :]
            tile = tails_of([sbuf[half, q * 4 + b, 64:80, :] for b in range(4)])
            at = base + half * GROUP + 4 * LANES
            panel[0 : 2 * K, pl.ds(at, LANES)] = jnp.concatenate(tile, axis=0).astype(BF16)
        acc[...] += jnp.dot(
            panel[:, pl.ds(base, 2 * GROUP)],
            aff[pl.ds(base, 2 * GROUP), :],
            preferred_element_type=F32,
        )

    in_groups([(s_copy, s_forward)], second_work, "b")

    eye = (
        lax.broadcasted_iota(jnp.int32, (K, LANES), 0)
        == lax.broadcasted_iota(jnp.int32, (K, LANES), 1)
    ).astype(F32)
    with jax.named_scope("send2"):
        send_product(1)
    with jax.named_scope("gram_second1"):
        gram_second(0)
    with jax.named_scope("gram_last1"):
        last = gram_last(0)
    with jax.named_scope("eliminate1"):
        inverse = eliminate(last, eye)
    with jax.named_scope("reduce2"):
        total = received_product(1)
    with jax.named_scope("scale2"):
        scaled = jnp.concatenate(
            [total[0:K] / deg_main, unpacked_tail(total[K : K + 8], 4) / deg_tail], axis=1
        )
        tall = jnp.concatenate([scaled, jnp.zeros((LANES - K, 2 * LANES), F32)], axis=0)
        scaled = jnp.dot(inverse, tall, precision=HIGHEST, preferred_element_type=F32)
    with jax.named_scope("gram_first2"):
        gram_first(1, scaled)
    with jax.named_scope("gram_second2"):
        gram_second(1)
    with jax.named_scope("gram_last2"):
        last = gram_last(1)
    with jax.named_scope("eliminate2"):
        ortho = eliminate(last, scaled)
        out_ref[...] = ortho[:, 0:OWN]

    for d in range(1, NZ):
        z_copy(d).wait_send()
        for it in range(2):
            p_copy(it, d).wait_send()
    for e in range(NXY):
        forward(e).wait_send()
        v_forward(e).wait_send()
        s_forward(e).wait_send()
    for e in range(1, NXY):
        xy_copy(e).wait_send()
        v_copy(e).wait_send()
        s_copy(e).wait_send()
        for it in range(2):
            ga_copy(it, e).wait_send()
            gb_copy(it, e).wait_send()


def solution(mesh):
    dma = pltpu.SemaphoreType.DMA

    def shards(points, start_vectors):
        return pl.pallas_call(
            kernel,
            out_shape=jax.ShapeDtypeStruct((K, OWN), F32),
            in_specs=[pl.BlockSpec(memory_space=pltpu.HBM)] * 2,
            out_specs=pl.BlockSpec(memory_space=pltpu.VMEM),
            scratch_shapes=[
                pltpu.VMEM((F, OWN), BF16),
                pltpu.VMEM((K, OWN), BF16),
                pltpu.VMEM((F + K, 2 * LANES), F32),
                pltpu.VMEM((NZ, 80, LANES), BF16),
                pltpu.VMEM((2, NXY, 80, LANES), BF16),
                pltpu.VMEM((2, NXY, 48, LANES), BF16),
                pltpu.VMEM((LANES, ROWS_I), BF16),
                pltpu.VMEM((2 * GROUP, LANES), BF16),
                pltpu.VMEM((2 * K, COLS_J), BF16),
                pltpu.VMEM((COLS_J, ROWS_I), BF16),
                pltpu.VMEM((2 * K, ROWS_I), F32),
                pltpu.VMEM((2, NZ, K + 16, LANES), F32),
                pltpu.VMEM((2, NZ, K + 16, LANES), F32),
                pltpu.VMEM((2, NXY, 80, LANES), BF16),
                pltpu.VMEM((2, 2, 8, LANES), F32),
                pltpu.VMEM((2, 2, 16, 8, LANES), F32),
                dma((2,)),
                dma((NZ,)), dma((NZ,)),
                dma((NXY,)), dma((NXY,)),
                dma((NXY,)), dma((NXY,)),
                dma((NXY,)), dma((NXY,)),
                dma((NXY,)), dma((NXY,)),
                dma((2, NZ)), dma((2, NZ)),
                dma((NXY,)), dma((NXY,)),
                dma((NXY,)), dma((NXY,)),
                dma((2, NCOL)), dma((2, NCOL)),
                dma((2, NXY)), dma((2, NXY)),
            ],
            compiler_params=pltpu.CompilerParams(
                collective_id=0, has_side_effects=True, vmem_limit_bytes=48 * 1024 * 1024
            ),
        )(points.T, start_vectors.T).T

    spec = P(("row", "col"), None)
    return jax.shard_map(
        shards, mesh=mesh, in_specs=(spec, spec), out_specs=spec, check_vma=False
    )
```

```python
import functools
import math

import jax
import jax.numpy as jnp
from jax import lax
from jax.experimental import pallas as pl
from jax.experimental.pallas import tpu as pltpu
from jax.sharding import PartitionSpec as P

MESH = pl.DeviceIdType.MESH
F32 = jnp.float32
BF16 = jnp.bfloat16
HIGHEST = lax.Precision.HIGHEST

KERNEL_SCALE = 5.12
F = 64
K = 32
OWN = 160
LANES = 128
TAIL = OWN - LANES
GROUP = 4 * OWN
NZ = 8
NX = 4
NY = 4
NXY = NX * NY
NCOL = 2 * NZ
ROWS_I = NZ * OWN
COLS_J = 2 * NXY * OWN
TOTAL = 256 * OWN


def lane_block():
    return lax.broadcasted_iota(jnp.int32, (8, LANES), 1) // TAIL


def roll_lanes(x, shift):
    shift = shift % LANES
    return x if shift == 0 else pltpu.roll(x, shift, 1)


def pick(blocks, pieces):
    out = pieces[3]
    for b in (2, 1, 0):
        out = jnp.where(blocks == b, pieces[b], out)
    return out


def transposed_blocks(tiles):
    rows = tiles[0].shape[0]
    blocks = lax.broadcasted_iota(jnp.int32, (rows, LANES), 1) // TAIL
    return [
        pick(blocks, [roll_lanes(tiles[b], TAIL * (b - g)) for b in range(4)]) for g in range(4)
    ]


def packed_tail(tail, rows):
    groups = tail.shape[0] // rows
    return sum(roll_lanes(tail[g * rows : (g + 1) * rows], TAIL * g) for g in range(groups))


def unpacked_tail(packed, groups):
    rows = packed.shape[0]
    keep = lax.broadcasted_iota(jnp.int32, (rows, LANES), 1) < TAIL
    return jnp.concatenate(
        [jnp.where(keep, roll_lanes(packed, -TAIL * g), 0.0) for g in range(groups)], axis=0
    )


def bf16_pieces(x):
    hi = x.astype(BF16).astype(F32)
    rest = x - hi
    mid = rest.astype(BF16).astype(F32)
    return hi, mid, rest - mid


def extended(x, for_rows):
    hi, mid, lo = bf16_pieces(jnp.sum(x * x, axis=0, keepdims=True))
    r = lax.broadcasted_iota(jnp.int32, (8, LANES), 0)
    if for_rows:
        x = 2.0 * x
        head = jnp.where(r == 3, -hi, jnp.where(r == 4, -mid, jnp.where(r == 5, -lo, 0.0)))
        extra = jnp.where(r < 3, -1.0, head)
    else:
        head = jnp.where(r == 0, hi, jnp.where(r == 1, mid, jnp.where(r == 2, lo, 0.0)))
        extra = jnp.where((r >= 3) & (r < 6), 1.0, head)
    return jnp.concatenate([x, extra, jnp.zeros((LANES - F - 8, LANES), F32)], axis=0)


def eliminate(gram, right):
    cols = [jnp.broadcast_to(gram[:, m : m + 1], (K, LANES)) for m in range(K)]
    width = right.shape[1] // LANES
    sub = lax.broadcasted_iota(jnp.int32, (8, LANES), 0)
    cols = [[c[8 * g : 8 * g + 8] for g in range(4)] for c in cols]
    rt = [
        [right[8 * g : 8 * g + 8, w * LANES : (w + 1) * LANES] for w in range(width)]
        for g in range(4)
    ]
    out_rows = []
    for k in range(K):
        kg, kr = k // 8, k % 8
        pivot = cols[k][kg][kr : kr + 1]
        inv = 1.0 / pivot
        factor = [None] * 4
        for g in range(kg, 4):
            f = cols[k][g] * inv
            if g == kg:
                f = jnp.where(sub > kr, f, 0.0)
            factor[g] = f
        for m in range(k + 1, K):
            mg, mr = m // 8, m % 8
            upper = cols[k][mg][mr : mr + 1]
            for g in range(mg, 4):
                cols[m][g] = cols[m][g] - factor[g] * upper
        rows = [rt[kg][w][kr : kr + 1] for w in range(width)]
        scale = lax.rsqrt(pivot)
        out_rows.append([row * scale for row in rows])
        for g in range(kg, 4):
            for w in range(width):
                rt[g][w] = rt[g][w] - factor[g] * rows[w]
    tiles = []
    for g in range(4):
        tile = []
        for w in range(width):
            acc = jnp.broadcast_to(out_rows[8 * g][w], (8, LANES))
            for r in range(1, 8):
                acc = jnp.where(sub == r, out_rows[8 * g + r][w], acc)
            tile.append(acc)
        tiles.append(jnp.concatenate(tile, axis=1) if width > 1 else tile[0])
    return jnp.concatenate(tiles, axis=0)


def kernel(
    pts_hbm, vec_hbm, out_ref,
    pts_ref, vec_ref, stage, zbuf, jbuf, vbuf, xi, xj, panel, aff, acc, psend, precv, sbuf, gsend, grecv,
    in_s, z_s, z_r, xy_s, xy_r, f_s, f_r, v_s, v_r, vf_s, vf_r,
    p_s, p_r, s_s, s_r, sf_s, sf_r, ga_s, ga_r, gb_s, gb_r,
):
    row = lax.axis_index("row")
    col = lax.axis_index("col")
    x, y = row // NY, lax.rem(row, NY)
    z, core = col // 2, lax.rem(col, 2)

    def xy_peer(e):
        q = e // NY
        to_x = lax.rem(x + q + (q // 2) * (5 - 2 * q), NX)
        to_y = lax.rem(y + e % NY, NY)
        return (to_x * NY + to_y, col)

    def z_peer(d):
        return (row, lax.rem(z + d + NZ, NZ) * 2 + core)

    def col_peer(d):
        return (row, lax.rem(col + d, NCOL))

    partner = (row, z * 2 + 1 - core)

    def remote(src, dst, send, recv, to):
        return pltpu.make_async_remote_copy(
            src_ref=src, dst_ref=dst, send_sem=send, recv_sem=recv,
            device_id=to, device_id_type=MESH,
        )

    pts_copy = pltpu.make_async_copy(pts_hbm, pts_ref, in_s.at[0])
    vec_copy = pltpu.make_async_copy(vec_hbm, vec_ref, in_s.at[1])
    pts_copy.start()
    vec_copy.start()
    barrier = pltpu.get_barrier_semaphore()
    with jax.named_scope("signal"):
        for d in range(1, NCOL):
            pl.semaphore_signal(barrier, inc=1, device_id=col_peer(d), device_id_type=MESH)
        for e in range(1, NXY):
            pl.semaphore_signal(barrier, inc=1, device_id=xy_peer(e), device_id_type=MESH)

    with jax.named_scope("prepare"):
        stage[...] = jnp.zeros_like(stage)
        pts_copy.wait()
        vec_copy.wait()
        stage[0:F, 0:OWN] = pts_ref[...].astype(F32)
        stage[F : F + K, 0:OWN] = vec_ref[...].astype(F32)
        t = stage[...]
        jbuf[0, 0, 0:64, :] = t[0:F, 0:LANES].astype(BF16)
        jbuf[0, 0, 64:80, :] = packed_tail(t[0:F, LANES:], 16).astype(BF16)
        vbuf[0, 0, 0:32, :] = t[F : F + K, 0:LANES].astype(BF16)
        vbuf[0, 0, 32:48, :] = packed_tail(t[F : F + K, LANES:], 16).astype(BF16)
        acc[...] = jnp.zeros_like(acc)
        for h in range(COLS_J // GROUP):
            panel[K : K + 16, h * GROUP : (h + 1) * GROUP] = (
                lax.broadcasted_iota(jnp.int32, (16, GROUP), 0) == 0
            ).astype(F32).astype(BF16)

    with jax.named_scope("barrier_wait"):
        pl.semaphore_wait(barrier, NCOL - 1 + NXY - 1)

    def z_copy(d):
        return remote(jbuf.at[0, 0], zbuf.at[d], z_s.at[d], z_r.at[d], z_peer(d))

    def xy_copy(e):
        return remote(jbuf.at[0, 0], jbuf.at[0, e], xy_s.at[e], xy_r.at[e], xy_peer(e))

    def forward(e):
        return remote(jbuf.at[0, e], jbuf.at[1, e], f_s.at[e], f_r.at[e], partner)

    def v_copy(e):
        return remote(vbuf.at[0, 0], vbuf.at[0, e], v_s.at[e], v_r.at[e], xy_peer(e))

    def v_forward(e):
        return remote(vbuf.at[0, e], vbuf.at[1, e], vf_s.at[e], vf_r.at[e], partner)

    def s_copy(e):
        return remote(sbuf.at[0, 0], sbuf.at[0, e], s_s.at[e], s_r.at[e], xy_peer(e))

    def s_forward(e):
        return remote(sbuf.at[0, e], sbuf.at[1, e], sf_s.at[e], sf_r.at[e], partner)

    def pass_on(q, copies):
        for copy, onward in copies:
            for b in range(4):
                e = q * 4 + b

                if isinstance(q, int):
                    if e > 0:
                        copy(e).wait_recv()
                    onward(e).start()
                else:
                    copy(e).wait_recv()
                    onward(e).start()

    def in_groups(copies, work, name, before_last=None):
        with jax.named_scope(name + "_first"):
            pass_on(0, copies)

        def step(q, carry):
            with jax.named_scope(name + "_wait"):
                pass_on(q + 1, copies)
                for _, onward in copies:
                    for b in range(4):
                        onward(q * 4 + b).wait_recv()
            with jax.named_scope(name + "_work"):
                work(q)
            return carry

        lax.fori_loop(0, 3, step, 0)
        if before_last is not None:
            before_last()
        with jax.named_scope(name + "_lastwait"):
            for _, onward in copies:
                for b in range(4):
                    onward(12 + b).wait_recv()
        with jax.named_scope(name + "_lastwork"):
            work(3)

    with jax.named_scope("send_points"):
        for d in (4, 3, 5, 2, 6, 1, 7):
            z_copy(d).start()
        for e in range(1, NXY):
            xy_copy(e).start()
        for e in range(1, NXY):
            v_copy(e).start()

    def tails_of(tiles):
        return transposed_blocks([tile.astype(F32) for tile in tiles])

    with jax.named_scope("row_side"):
        for d in range(NZ):
            if d == 0:
                src = jbuf[0, 0, 0:64, :]
            else:
                z_copy(d).wait_recv()
                src = zbuf[d, 0:64, :]
            xi[:, d * LANES : (d + 1) * LANES] = extended(src.astype(F32), True).astype(BF16)
        for q in range(NZ // 4):
            tiles = [
                jbuf[0, 0, 64:80, :] if 4 * q + b == 0 else zbuf[4 * q + b, 64:80, :]
                for b in range(4)
            ]
            tile = jnp.concatenate(tails_of(tiles), axis=0)
            at = NZ * LANES + q * LANES
            xi[:, at : at + LANES] = extended(tile, True).astype(BF16)

    def first_work(q):
        base = pl.multiple_of(q * 2 * GROUP, 2 * GROUP)
        for half in range(2):
            for b in range(4):
                e = q * 4 + b
                at = half * GROUP + b * LANES
                src = jbuf[half, e, 0:64, :].astype(F32)
                xj[at : at + LANES, :] = extended(src, False).T.astype(BF16)
                panel[0:K, pl.ds(base + at, LANES)] = vbuf[half, e, 0:32, :]
            at = half * GROUP + 4 * LANES
            tile = tails_of([jbuf[half, q * 4 + b, 64:80, :] for b in range(4)])
            xj[at : at + LANES, :] = extended(jnp.concatenate(tile, axis=0), False).T.astype(BF16)
            tile = tails_of([vbuf[half, q * 4 + b, 32:48, :] for b in range(4)])[0:2]
            panel[0:K, pl.ds(base + at, LANES)] = jnp.concatenate(tile, axis=0).astype(BF16)
        for c in range(ROWS_I // 256):
            here = slice(c * 256, (c + 1) * 256)
            dist = jnp.dot(xj[...], xi[:, here], preferred_element_type=F32)
            weights = jnp.exp2(dist * (KERNEL_SCALE / F * math.log2(math.e)))
            aff[pl.ds(base, 2 * GROUP), here] = weights.astype(BF16)
        for c in range(ROWS_I // 256):
            here = slice(c * 256, (c + 1) * 256)
            acc[0 : K + 16, here] += jnp.dot(
                panel[0 : K + 16, pl.ds(base, 2 * GROUP)],
                aff[pl.ds(base, 2 * GROUP), here],
                preferred_element_type=F32,
            )

    in_groups([(xy_copy, forward), (v_copy, v_forward)], first_work, "a")

    blocks8 = lane_block()

    def p_copy(it, d):
        rows = K + 16 - 8 * it
        return remote(
            psend.at[it, d, pl.ds(0, rows)], precv.at[it, d, pl.ds(0, rows)],
            p_s.at[it, d], p_r.at[it, d], z_peer(-d),
        )

    def send_product(it):
        for q in range(NZ // 4):
            at = NZ * LANES + q * LANES
            tail = acc[0:K, at : at + LANES]
            if it == 1:
                tail = tail + acc[K : 2 * K, at : at + LANES]
            packed = [
                pick(blocks8, [roll_lanes(tail[8 * g : 8 * g + 8], TAIL * (g - b)) for g in range(4)])
                for b in range(4)
            ]
            for b in range(4):
                d = 4 * q + b
                main = acc[0:K, d * LANES : (d + 1) * LANES]
                if it == 1:
                    main = main + acc[K : 2 * K, d * LANES : (d + 1) * LANES]
                psend[it, d, 0:K, :] = main
                psend[it, d, K : K + 8, :] = packed[b]
                if it == 0:
                    psend[it, d, K + 8 : K + 9, :] = acc[K : K + 1, d * LANES : (d + 1) * LANES]
                    psend[it, d, K + 9 : K + 10, :] = roll_lanes(
                        acc[K : K + 8, at : at + LANES], -TAIL * b
                    )[0:1]
                    psend[it, d, K + 10 : K + 16, :] = jnp.zeros((6, LANES), F32)
        for d in (4, 3, 5, 2, 6, 1, 7):
            p_copy(it, d).start()

    def received_product(it):
        rows = K + 16 - 8 * it
        total = psend[it, 0, 0:rows]
        for d in (1, 7, 2, 6, 3, 5, 4):
            p_copy(it, d).wait_recv()
            total = total + precv[it, d, 0:rows]
        return total

    def gram_of(scaled):
        wide = jnp.concatenate([scaled, jnp.zeros((LANES - K, 2 * LANES), F32)], axis=0)
        part = lax.dot_general(
            scaled, wide, (((1,), (1,)), ((), ())), precision=HIGHEST, preferred_element_type=F32
        )
        return packed_tail(part, 8)

    def ga_copy(it, d):
        return remote(gsend.at[it, 0], grecv.at[it, 0, d], ga_s.at[it, d], ga_r.at[it, d], col_peer(d))

    def gb_copy(it, e):
        return remote(gsend.at[it, 1], grecv.at[it, 1, e], gb_s.at[it, e], gb_r.at[it, e], xy_peer(e))

    def gram_first(it, scaled):
        gsend[it, 0] = gram_of(scaled)
        for d in range(1, NCOL):
            ga_copy(it, d).start()

    def gram_second(it):
        total = gsend[it, 0]
        for d in range(1, NCOL):
            ga_copy(it, d).wait_recv()
            total = total + grecv[it, 0, d]
        gsend[it, 1] = total
        for e in range(1, NXY):
            gb_copy(it, e).start()

    def gram_last(it):
        total = gsend[it, 1]
        for e in range(1, NXY):
            gb_copy(it, e).wait_recv()
            total = total + grecv[it, 1, e]
        return unpacked_tail(total, 4) * (1.0 / TOTAL)

    with jax.named_scope("send1"):
        send_product(0)
    with jax.named_scope("reduce1"):
        total = received_product(0)
    with jax.named_scope("scale1"):
        keep = lax.broadcasted_iota(jnp.int32, (1, LANES), 1) < TAIL
        deg_main = total[K + 8 : K + 9]
        deg_tail = jnp.where(keep, total[K + 9 : K + 10], 1.0)
        scaled_main = total[0:K] / deg_main
        scaled_tail = unpacked_tail(total[K : K + 8], 4) / deg_tail
        scaled = jnp.concatenate([scaled_main, scaled_tail], axis=1)

        hi = scaled.astype(BF16).astype(F32)
        lo = scaled - hi
        both = jnp.concatenate([hi, lo], axis=0)
        sbuf[0, 0, 0:64, :] = both[:, 0:LANES].astype(BF16)
        sbuf[0, 0, 64:80, :] = packed_tail(both[:, LANES:], 16).astype(BF16)
        for e in range(1, NXY):
            s_copy(e).start()
    with jax.named_scope("gram_first1"):
        gram_first(0, scaled)
        acc[...] = jnp.zeros_like(acc)

    def second_work(q):
        base = pl.multiple_of(q * 2 * GROUP, 2 * GROUP)
        for half in range(2):
            for b in range(4):
                at = base + half * GROUP + b * LANES
                panel[0 : 2 * K, pl.ds(at, LANES)] = sbuf[half, q * 4 + b, 0:64, :]
            tile = tails_of([sbuf[half, q * 4 + b, 64:80, :] for b in range(4)])
            at = base + half * GROUP + 4 * LANES
            panel[0 : 2 * K, pl.ds(at, LANES)] = jnp.concatenate(tile, axis=0).astype(BF16)
        acc[...] += jnp.dot(
            panel[:, pl.ds(base, 2 * GROUP)],
            aff[pl.ds(base, 2 * GROUP), :],
            preferred_element_type=F32,
        )

    in_groups([(s_copy, s_forward)], second_work, "b", lambda: gram_second(0))

    eye = (
        lax.broadcasted_iota(jnp.int32, (K, LANES), 0)
        == lax.broadcasted_iota(jnp.int32, (K, LANES), 1)
    ).astype(F32)
    with jax.named_scope("send2"):
        send_product(1)
    with jax.named_scope("gram_last1"):
        last = gram_last(0)
    with jax.named_scope("eliminate1"):
        inverse = eliminate(last, eye)
    with jax.named_scope("reduce2"):
        total = received_product(1)
    with jax.named_scope("scale2"):
        scaled = jnp.concatenate(
            [total[0:K] / deg_main, unpacked_tail(total[K : K + 8], 4) / deg_tail], axis=1
        )
        tall = jnp.concatenate([scaled, jnp.zeros((LANES - K, 2 * LANES), F32)], axis=0)
        scaled = jnp.dot(inverse, tall, precision=HIGHEST, preferred_element_type=F32)
    with jax.named_scope("gram_first2"):
        gram_first(1, scaled)
    with jax.named_scope("gram_second2"):
        gram_second(1)
    with jax.named_scope("gram_last2"):
        last = gram_last(1)
    with jax.named_scope("eliminate2"):
        ortho = eliminate(last, scaled)
        out_ref[...] = ortho[:, 0:OWN]

    for d in range(1, NZ):
        z_copy(d).wait_send()
        for it in range(2):
            p_copy(it, d).wait_send()
    for e in range(NXY):
        forward(e).wait_send()
        v_forward(e).wait_send()
        s_forward(e).wait_send()
    for e in range(1, NXY):
        xy_copy(e).wait_send()
        v_copy(e).wait_send()
        s_copy(e).wait_send()
        for it in range(2):
            ga_copy(it, e).wait_send()
            gb_copy(it, e).wait_send()


def solution(mesh):
    dma = pltpu.SemaphoreType.DMA

    def shards(points, start_vectors):
        return pl.pallas_call(
            kernel,
            out_shape=jax.ShapeDtypeStruct((K, OWN), F32),
            in_specs=[pl.BlockSpec(memory_space=pltpu.HBM)] * 2,
            out_specs=pl.BlockSpec(memory_space=pltpu.VMEM),
            scratch_shapes=[
                pltpu.VMEM((F, OWN), BF16),
                pltpu.VMEM((K, OWN), BF16),
                pltpu.VMEM((F + K, 2 * LANES), F32),
                pltpu.VMEM((NZ, 80, LANES), BF16),
                pltpu.VMEM((2, NXY, 80, LANES), BF16),
                pltpu.VMEM((2, NXY, 48, LANES), BF16),
                pltpu.VMEM((LANES, ROWS_I), BF16),
                pltpu.VMEM((2 * GROUP, LANES), BF16),
                pltpu.VMEM((2 * K, COLS_J), BF16),
                pltpu.VMEM((COLS_J, ROWS_I), BF16),
                pltpu.VMEM((2 * K, ROWS_I), F32),
                pltpu.VMEM((2, NZ, K + 16, LANES), F32),
                pltpu.VMEM((2, NZ, K + 16, LANES), F32),
                pltpu.VMEM((2, NXY, 80, LANES), BF16),
                pltpu.VMEM((2, 2, 8, LANES), F32),
                pltpu.VMEM((2, 2, 16, 8, LANES), F32),
                dma((2,)),
                dma((NZ,)), dma((NZ,)),
                dma((NXY,)), dma((NXY,)),
                dma((NXY,)), dma((NXY,)),
                dma((NXY,)), dma((NXY,)),
                dma((NXY,)), dma((NXY,)),
                dma((2, NZ)), dma((2, NZ)),
                dma((NXY,)), dma((NXY,)),
                dma((NXY,)), dma((NXY,)),
                dma((2, NCOL)), dma((2, NCOL)),
                dma((2, NXY)), dma((2, NXY)),
            ],
            compiler_params=pltpu.CompilerParams(
                collective_id=0, has_side_effects=True, vmem_limit_bytes=48 * 1024 * 1024
            ),
        )(points.T, start_vectors.T).T

    spec = P(("row", "col"), None)
    return jax.shard_map(
        shards, mesh=mesh, in_specs=(spec, spec), out_specs=spec, check_vma=False
    )
```

```python
import functools
import math

import jax
import jax.numpy as jnp
from jax import lax
from jax.experimental import pallas as pl
from jax.experimental.pallas import tpu as pltpu
from jax.sharding import PartitionSpec as P

MESH = pl.DeviceIdType.MESH
F32 = jnp.float32
BF16 = jnp.bfloat16
HIGHEST = lax.Precision.HIGHEST

KERNEL_SCALE = 5.12
WIDE = 1
F = 64
K = 32
OWN = 160
LANES = 128
TAIL = OWN - LANES
GROUP = 4 * OWN
NZ = 8
NX = 4
NY = 4
NXY = NX * NY
NCOL = 2 * NZ
ROWS_I = NZ * OWN
COLS_J = 2 * NXY * OWN
TOTAL = 256 * OWN


def roll_lanes(x, shift):
    shift = shift % LANES
    return x if shift == 0 else pltpu.roll(x, shift, 1)


def pick(blocks, pieces):
    out = pieces[3]
    for b in (2, 1, 0):
        out = jnp.where(blocks == b, pieces[b], out)
    return out


def transposed_blocks(tiles):
    rows = tiles[0].shape[0]
    blocks = lax.broadcasted_iota(jnp.int32, (rows, LANES), 1) // TAIL
    return [
        pick(blocks, [roll_lanes(tiles[b], TAIL * (b - g)) for b in range(4)]) for g in range(4)
    ]


def packed_tail(tail, rows):
    groups = tail.shape[0] // rows
    return sum(roll_lanes(tail[g * rows : (g + 1) * rows], TAIL * g) for g in range(groups))


def unpacked_tail(packed, groups):
    rows = packed.shape[0]
    keep = lax.broadcasted_iota(jnp.int32, (rows, LANES), 1) < TAIL
    return jnp.concatenate(
        [jnp.where(keep, roll_lanes(packed, -TAIL * g), 0.0) for g in range(groups)], axis=0
    )


def bf16_pieces(x):
    hi = x.astype(BF16).astype(F32)
    rest = x - hi
    mid = rest.astype(BF16).astype(F32)
    return hi, mid, rest - mid


def extended(x, for_rows):
    hi, mid, lo = bf16_pieces(jnp.sum(x * x, axis=0, keepdims=True))
    r = lax.broadcasted_iota(jnp.int32, (8, LANES), 0)
    if for_rows:
        x = 2.0 * x
        head = jnp.where(r == 3, -hi, jnp.where(r == 4, -mid, jnp.where(r == 5, -lo, 0.0)))
        extra = jnp.where(r < 3, -1.0, head)
    else:
        head = jnp.where(r == 0, hi, jnp.where(r == 1, mid, jnp.where(r == 2, lo, 0.0)))
        extra = jnp.where((r >= 3) & (r < 6), 1.0, head)
    return jnp.concatenate([x, extra, jnp.zeros((LANES - F - 8, LANES), F32)], axis=0)


def eliminate(gram, right):
    cols = [jnp.broadcast_to(gram[:, m : m + 1], (K, LANES)) for m in range(K)]
    width = right.shape[1] // LANES
    sub = lax.broadcasted_iota(jnp.int32, (8, LANES), 0)
    cols = [[c[8 * g : 8 * g + 8] for g in range(4)] for c in cols]
    rt = [
        [right[8 * g : 8 * g + 8, w * LANES : (w + 1) * LANES] for w in range(width)]
        for g in range(4)
    ]
    out_rows = []
    for k in range(K):
        kg, kr = k // 8, k % 8
        pivot = cols[k][kg][kr : kr + 1]
        inv = 1.0 / pivot
        factor = [None] * 4
        for g in range(kg, 4):
            f = cols[k][g] * inv
            if g == kg:
                f = jnp.where(sub > kr, f, 0.0)
            factor[g] = f
        for m in range(k + 1, K):
            mg, mr = m // 8, m % 8
            upper = cols[k][mg][mr : mr + 1]
            for g in range(mg, 4):
                cols[m][g] = cols[m][g] - factor[g] * upper
        rows = [rt[kg][w][kr : kr + 1] for w in range(width)]
        scale = lax.rsqrt(pivot)
        out_rows.append([row * scale for row in rows])
        for g in range(kg, 4):
            for w in range(width):
                rt[g][w] = rt[g][w] - factor[g] * rows[w]
    tiles = []
    for g in range(4):
        tile = []
        for w in range(width):
            acc = jnp.broadcast_to(out_rows[8 * g][w], (8, LANES))
            for r in range(1, 8):
                acc = jnp.where(sub == r, out_rows[8 * g + r][w], acc)
            tile.append(acc)
        tiles.append(jnp.concatenate(tile, axis=1) if width > 1 else tile[0])
    return jnp.concatenate(tiles, axis=0)


def kernel(
    pts_hbm, vec_hbm, out_ref,
    pts_ref, vec_ref, stage, zbuf, jbuf, vbuf, xi, xj, panel, aff, acc, psend, precv, sbuf, gsend, grecv,
    in_s, z_s, z_r, xy_s, xy_r, f_s, f_r, v_s, v_r, vf_s, vf_r,
    p_s, p_r, s_s, s_r, sf_s, sf_r, ga_s, ga_r, gb_s, gb_r,
):
    row = lax.axis_index("row")
    col = lax.axis_index("col")
    x, y = row // NY, lax.rem(row, NY)
    z, core = col // 2, lax.rem(col, 2)

    def xy_peer(e):
        q = e // NY
        to_x = lax.rem(x + q + (q // 2) * (5 - 2 * q), NX)
        to_y = lax.rem(y + e % NY, NY)
        return (to_x * NY + to_y, col)

    def z_peer(d):
        return (row, lax.rem(z + d + NZ, NZ) * 2 + core)

    def col_peer(d):
        return (row, lax.rem(col + d, NCOL))

    partner = (row, z * 2 + 1 - core)

    def remote(src, dst, send, recv, to):
        return pltpu.make_async_remote_copy(
            src_ref=src, dst_ref=dst, send_sem=send, recv_sem=recv,
            device_id=to, device_id_type=MESH,
        )

    pts_copy = pltpu.make_async_copy(pts_hbm, pts_ref, in_s.at[0])
    vec_copy = pltpu.make_async_copy(vec_hbm, vec_ref, in_s.at[1])
    pts_copy.start()
    vec_copy.start()
    barrier = pltpu.get_barrier_semaphore()
    with jax.named_scope("signal"):
        for d in range(1, NCOL):
            pl.semaphore_signal(barrier, inc=1, device_id=col_peer(d), device_id_type=MESH)
        for e in range(1, NXY):
            pl.semaphore_signal(barrier, inc=1, device_id=xy_peer(e), device_id_type=MESH)

    with jax.named_scope("prepare"):
        stage[...] = jnp.zeros_like(stage)
        pts_copy.wait()
        vec_copy.wait()
        stage[0:F, 0:OWN] = pts_ref[...].astype(F32)
        stage[F : F + K, 0:OWN] = vec_ref[...].astype(F32)
        t = stage[...]
        jbuf[0, 0, 0:64, :] = t[0:F, 0:LANES].astype(BF16)
        jbuf[0, 0, 64:80, :] = packed_tail(t[0:F, LANES:], 16).astype(BF16)
        vbuf[0, 0, 0:32, :] = t[F : F + K, 0:LANES].astype(BF16)
        vbuf[0, 0, 32:48, :] = packed_tail(t[F : F + K, LANES:], 16).astype(BF16)
        acc[...] = jnp.zeros_like(acc)
        for h in range(COLS_J // GROUP):
            panel[K : K + 16, h * GROUP : (h + 1) * GROUP] = (
                lax.broadcasted_iota(jnp.int32, (16, GROUP), 0) == 0
            ).astype(F32).astype(BF16)

    with jax.named_scope("barrier_wait"):
        pl.semaphore_wait(barrier, NCOL - 1 + NXY - 1)

    def z_copy(d):
        return remote(jbuf.at[0, 0], zbuf.at[d], z_s.at[d], z_r.at[d], z_peer(d))

    def xy_copy(e):
        return remote(jbuf.at[0, 0], jbuf.at[0, e], xy_s.at[e], xy_r.at[e], xy_peer(e))

    def forward(e):
        return remote(jbuf.at[0, e], jbuf.at[1, e], f_s.at[e], f_r.at[e], partner)

    def v_copy(e):
        return remote(vbuf.at[0, 0], vbuf.at[0, e], v_s.at[e], v_r.at[e], xy_peer(e))

    def v_forward(e):
        return remote(vbuf.at[0, e], vbuf.at[1, e], vf_s.at[e], vf_r.at[e], partner)

    def s_copy(e):
        return remote(sbuf.at[0, 0], sbuf.at[0, e], s_s.at[e], s_r.at[e], xy_peer(e))

    def s_forward(e):
        return remote(sbuf.at[0, e], sbuf.at[1, e], sf_s.at[e], sf_r.at[e], partner)

    def arrived(q, copy, onward):
        for b in range(4):
            e = q * 4 + b
            if isinstance(e, int) and e == 0:
                continue
            copy(e).wait_recv()
            onward(e).start()

    def forwarded(q, onward):
        for b in range(4):
            onward(q * 4 + b).wait_recv()

    with jax.named_scope("send_points"):
        for d in (4, 3, 5, 2, 6, 1, 7):
            z_copy(d).start()
        for e in range(1, NXY):
            xy_copy(e).start()
        forward(0).start()
        for e in range(1, NXY):
            v_copy(e).start()
        v_forward(0).start()

    def tails_of(tiles):
        return transposed_blocks([tile.astype(F32) for tile in tiles])

    with jax.named_scope("first_points"):
        arrived(0, xy_copy, forward)

    with jax.named_scope("row_side"):
        for d in range(NZ):
            if d == 0:
                src = jbuf[0, 0, 0:64, :]
            else:
                z_copy(d).wait_recv()
                src = zbuf[d, 0:64, :]
            xi[:, d * LANES : (d + 1) * LANES] = extended(src.astype(F32), True).astype(BF16)
        for q in range(NZ // 4):
            tiles = [
                jbuf[0, 0, 64:80, :] if 4 * q + b == 0 else zbuf[4 * q + b, 64:80, :]
                for b in range(4)
            ]
            tile = jnp.concatenate(tails_of(tiles), axis=0)
            at = NZ * LANES + q * LANES
            xi[:, at : at + LANES] = extended(tile, True).astype(BF16)

    def affinity(q):
        base = pl.multiple_of(q * 2 * GROUP, 2 * GROUP)
        for half in range(2):
            for b in range(4):
                at = half * GROUP + b * LANES
                src = jbuf[half, q * 4 + b, 0:64, :].astype(F32)
                xj[at : at + LANES, :] = extended(src, False).T.astype(BF16)
            at = half * GROUP + 4 * LANES
            tile = tails_of([jbuf[half, q * 4 + b, 64:80, :] for b in range(4)])
            xj[at : at + LANES, :] = extended(jnp.concatenate(tile, axis=0), False).T.astype(BF16)
        for c in range(ROWS_I // 256):
            here = slice(c * 256, (c + 1) * 256)
            dist = jnp.dot(xj[...], xi[:, here], preferred_element_type=F32)
            weights = jnp.exp2(dist * (KERNEL_SCALE / F * math.log2(math.e)))
            aff[pl.ds(base, 2 * GROUP), here] = weights.astype(BF16)

    def vector_tiles(q, src, rows):
        base = pl.multiple_of(q * 2 * GROUP, 2 * GROUP)
        groups = rows // 16
        for half in range(2):
            for b in range(4):
                at = base + half * GROUP + b * LANES
                panel[0:rows, pl.ds(at, LANES)] = src[half, q * 4 + b, 0:rows, :]
            tile = tails_of([src[half, q * 4 + b, rows : rows + 16, :] for b in range(4)])[0:groups]
            at = base + half * GROUP + 4 * LANES
            panel[0:rows, pl.ds(at, LANES)] = jnp.concatenate(tile, axis=0).astype(BF16)

    def product(q, rows):
        base = pl.multiple_of(q * 2 * GROUP, 2 * GROUP)
        for c in range(ROWS_I // 256):
            here = slice(c * 256, (c + 1) * 256)
            acc[0:rows, here] += jnp.dot(
                panel[0:rows, pl.ds(base, 2 * GROUP)],
                aff[pl.ds(base, 2 * GROUP), here],
                preferred_element_type=F32,
            )

    with jax.named_scope("a_first_wait"):
        arrived(0, v_copy, v_forward)

    def work(q):
        vector_tiles(q, vbuf, K)
        affinity(q)
        product(q, K + 16)

    def step(q, carry):
        with jax.named_scope("a_wait"):
            arrived(q + 1, xy_copy, forward)
            arrived(q + 1, v_copy, v_forward)
            forwarded(q, forward)
            forwarded(q, v_forward)
        with jax.named_scope("a_work"):
            work(q)
        return carry

    lax.fori_loop(0, 3, step, 0)
    with jax.named_scope("a_last_wait"):
        forwarded(3, forward)
        forwarded(3, v_forward)
    with jax.named_scope("a_last"):
        work(3)

    def p_copy(it, d):
        return remote(psend.at[it, d], precv.at[it, d], p_s.at[it, d], p_r.at[it, d], z_peer(-d))

    blocks16 = lax.broadcasted_iota(jnp.int32, (16, LANES), 1) // TAIL
    rows16 = lax.broadcasted_iota(jnp.int32, (16, LANES), 0)

    def send_product(it):
        for q in range(NZ // 4):
            at = NZ * LANES + q * LANES
            for b in range(4):
                d = 4 * q + b
                here = slice(d * LANES, (d + 1) * LANES)
                psend[it, d, 0:K, :] = acc[0:K, here].astype(BF16)
                last = jnp.zeros((16, LANES), F32)
                if it == 0:
                    hi, mid, _ = bf16_pieces(acc[K : K + 8, here])
                    hi_t, mid_t, _ = bf16_pieces(acc[K : K + 8, at : at + LANES])
                    lines = [
                        roll_lanes(hi_t, TAIL * (2 - b)), roll_lanes(mid_t, TAIL * (2 - b)),
                        roll_lanes(hi, 64), hi, roll_lanes(mid, 64), mid,
                    ]
                    for r, line in enumerate(lines):
                        last = jnp.where(rows16 == r, line[0:1], last)
                last = jnp.where(blocks16 == 0, roll_lanes(acc[0:16, at : at + LANES], -TAIL * b), last)
                last = jnp.where(blocks16 == 1, roll_lanes(acc[16:32, at : at + LANES], TAIL * (1 - b)), last)
                psend[it, d, K : K + 16, :] = last.astype(BF16)
        for d in (4, 3, 5, 2, 6, 1, 7):
            p_copy(it, d).start()

    def received_product(it):
        total = psend[it, 0].astype(F32)
        for d in (1, 7, 2, 6, 3, 5, 4):
            p_copy(it, d).wait_recv()
            total = total + precv[it, d].astype(F32)
        return total

    def degree_of(total):
        tail = roll_lanes(total[K : K + 1] + total[K + 1 : K + 2], 64)
        low = roll_lanes(total[K + 2 : K + 3] + total[K + 4 : K + 5], 64)
        high = total[K + 3 : K + 4] + total[K + 5 : K + 6]
        lane = lax.broadcasted_iota(jnp.int32, (1, LANES), 1)
        return jnp.where(lane < 64, low, high), jnp.where(lane < TAIL, tail, 1.0)

    def gram_of(scaled):
        wide = jnp.concatenate([scaled, jnp.zeros((LANES - K, 2 * LANES), F32)], axis=0)
        part = lax.dot_general(
            scaled, wide, (((1,), (1,)), ((), ())), precision=HIGHEST, preferred_element_type=F32
        )
        return packed_tail(part, 8)

    def ga_copy(it, d):
        return remote(gsend.at[it, 0], grecv.at[it, 0, d], ga_s.at[it, d], ga_r.at[it, d], col_peer(d))

    def gb_copy(it, e):
        return remote(gsend.at[it, 1], grecv.at[it, 1, e], gb_s.at[it, e], gb_r.at[it, e], xy_peer(e))

    def gram_first(it, scaled):
        gsend[it, 0] = gram_of(scaled)
        for d in range(1, NCOL):
            ga_copy(it, d).start()

    def gram_second(it):
        total = gsend[it, 0]
        for d in range(1, NCOL):
            ga_copy(it, d).wait_recv()
            total = total + grecv[it, 0, d]
        gsend[it, 1] = total
        for e in range(1, NXY):
            gb_copy(it, e).start()

    def gram_last(it):
        total = gsend[it, 1]
        for e in range(1, NXY):
            gb_copy(it, e).wait_recv()
            total = total + grecv[it, 1, e]
        return unpacked_tail(total, 4) * (1.0 / TOTAL)

    with jax.named_scope("send1"):
        send_product(0)
    with jax.named_scope("reduce1"):
        total = received_product(0)
    with jax.named_scope("scale1"):
        deg_main, deg_tail = degree_of(total)
        scaled_main = total[0:K] / deg_main
        scaled_tail = unpacked_tail(total[K : K + 16], 2) / deg_tail
        scaled = jnp.concatenate([scaled_main, scaled_tail], axis=1)

        both = scaled
        if WIDE == 2:
            hi = scaled.astype(BF16).astype(F32)
            both = jnp.concatenate([hi, scaled - hi], axis=0)
        sbuf[0, 0, 0 : WIDE * K, :] = both[:, 0:LANES].astype(BF16)
        sbuf[0, 0, WIDE * K : WIDE * K + 16, :] = packed_tail(both[:, LANES:], 16).astype(BF16)
        for e in range(1, NXY):
            s_copy(e).start()
        s_forward(0).start()
    with jax.named_scope("gram_first1"):
        gram_first(0, scaled)
        acc[...] = jnp.zeros_like(acc)

    with jax.named_scope("b_first_wait"):
        arrived(0, s_copy, s_forward)
        arrived(1, s_copy, s_forward)
        forwarded(0, s_forward)
    with jax.named_scope("b_first"):
        vector_tiles(0, sbuf, WIDE * K)
        product(0, WIDE * K)
    with jax.named_scope("b_second_wait"):
        arrived(2, s_copy, s_forward)
        forwarded(1, s_forward)
    with jax.named_scope("b_second"):
        vector_tiles(1, sbuf, WIDE * K)
        product(1, WIDE * K)
    with jax.named_scope("b_third_wait"):
        arrived(3, s_copy, s_forward)
        forwarded(2, s_forward)
    with jax.named_scope("b_third"):
        vector_tiles(2, sbuf, WIDE * K)
        product(2, WIDE * K)
    gram_second(0)
    with jax.named_scope("b_last_wait"):
        forwarded(3, s_forward)
    with jax.named_scope("b_last"):
        vector_tiles(3, sbuf, WIDE * K)
        product(3, WIDE * K)

    eye = (
        lax.broadcasted_iota(jnp.int32, (K, LANES), 0)
        == lax.broadcasted_iota(jnp.int32, (K, LANES), 1)
    ).astype(F32)
    with jax.named_scope("send2"):
        send_product(1)
    with jax.named_scope("gram_last1"):
        last = gram_last(0)
    with jax.named_scope("eliminate1"):
        inverse = eliminate(last, eye)
    with jax.named_scope("reduce2"):
        total = received_product(1)
    with jax.named_scope("scale2"):
        scaled = jnp.concatenate(
            [total[0:K] / deg_main, unpacked_tail(total[K : K + 16], 2) / deg_tail], axis=1
        )
        tall = jnp.concatenate([scaled, jnp.zeros((LANES - K, 2 * LANES), F32)], axis=0)
        scaled = jnp.dot(inverse, tall, precision=HIGHEST, preferred_element_type=F32)
    with jax.named_scope("gram_first2"):
        gram_first(1, scaled)
    with jax.named_scope("gram_second2"):
        gram_second(1)
    with jax.named_scope("gram_last2"):
        last = gram_last(1)
    with jax.named_scope("eliminate2"):
        ortho = eliminate(last, scaled)
        out_ref[...] = ortho[:, 0:OWN]

    for d in range(1, NZ):
        z_copy(d).wait_send()
        for it in range(2):
            p_copy(it, d).wait_send()
    for e in range(NXY):
        forward(e).wait_send()
        v_forward(e).wait_send()
        s_forward(e).wait_send()
    for e in range(1, NXY):
        xy_copy(e).wait_send()
        v_copy(e).wait_send()
        s_copy(e).wait_send()
        for it in range(2):
            ga_copy(it, e).wait_send()
            gb_copy(it, e).wait_send()


def solution(mesh):
    dma = pltpu.SemaphoreType.DMA

    def shards(points, start_vectors):
        return pl.pallas_call(
            kernel,
            out_shape=jax.ShapeDtypeStruct((K, OWN), F32),
            in_specs=[pl.BlockSpec(memory_space=pltpu.HBM)] * 2,
            out_specs=pl.BlockSpec(memory_space=pltpu.VMEM),
            scratch_shapes=[
                pltpu.VMEM((F, OWN), BF16),
                pltpu.VMEM((K, OWN), BF16),
                pltpu.VMEM((F + K, 2 * LANES), F32),
                pltpu.VMEM((NZ, 80, LANES), BF16),
                pltpu.VMEM((2, NXY, 80, LANES), BF16),
                pltpu.VMEM((2, NXY, 48, LANES), BF16),
                pltpu.VMEM((LANES, ROWS_I), BF16),
                pltpu.VMEM((2 * GROUP, LANES), BF16),
                pltpu.VMEM((2 * K, COLS_J), BF16),
                pltpu.VMEM((COLS_J, ROWS_I), BF16),
                pltpu.VMEM((2 * K, ROWS_I), F32),
                pltpu.VMEM((2, NZ, K + 16, LANES), BF16),
                pltpu.VMEM((2, NZ, K + 16, LANES), BF16),
                pltpu.VMEM((2, NXY, WIDE * K + 16, LANES), BF16),
                pltpu.VMEM((2, 2, 8, LANES), F32),
                pltpu.VMEM((2, 2, 16, 8, LANES), F32),
                dma((2,)),
                dma((NZ,)), dma((NZ,)),
                dma((NXY,)), dma((NXY,)),
                dma((NXY,)), dma((NXY,)),
                dma((NXY,)), dma((NXY,)),
                dma((NXY,)), dma((NXY,)),
                dma((2, NZ)), dma((2, NZ)),
                dma((NXY,)), dma((NXY,)),
                dma((NXY,)), dma((NXY,)),
                dma((2, NCOL)), dma((2, NCOL)),
                dma((2, NXY)), dma((2, NXY)),
            ],
            compiler_params=pltpu.CompilerParams(
                collective_id=0, has_side_effects=True, vmem_limit_bytes=48 * 1024 * 1024
            ),
        )(points.T, start_vectors.T).T

    spec = P(("row", "col"), None)
    return jax.shard_map(
        shards, mesh=mesh, in_specs=(spec, spec), out_specs=spec, check_vma=False
    )
```

```python
import functools
import math

import jax
import jax.numpy as jnp
from jax import lax
from jax.experimental import pallas as pl
from jax.experimental.pallas import tpu as pltpu
from jax.sharding import PartitionSpec as P

MESH = pl.DeviceIdType.MESH
F32 = jnp.float32
BF16 = jnp.bfloat16
HIGHEST = lax.Precision.HIGHEST

KERNEL_SCALE = 5.12
WIDE = 1
F = 64
K = 32
OWN = 160
LANES = 128
TAIL = OWN - LANES
GROUP = 4 * OWN
NZ = 8
NX = 4
NY = 4
NXY = NX * NY
NCOL = 2 * NZ
ROWS_I = NZ * OWN
COLS_J = 2 * NXY * OWN
TOTAL = 256 * OWN


def roll_lanes(x, shift):
    shift = shift % LANES
    return x if shift == 0 else pltpu.roll(x, shift, 1)


def pick(blocks, pieces):
    out = pieces[3]
    for b in (2, 1, 0):
        out = jnp.where(blocks == b, pieces[b], out)
    return out


def transposed_blocks(tiles):
    rows = tiles[0].shape[0]
    blocks = lax.broadcasted_iota(jnp.int32, (rows, LANES), 1) // TAIL
    return [
        pick(blocks, [roll_lanes(tiles[b], TAIL * (b - g)) for b in range(4)]) for g in range(4)
    ]


def packed_tail(tail, rows):
    groups = tail.shape[0] // rows
    return sum(roll_lanes(tail[g * rows : (g + 1) * rows], TAIL * g) for g in range(groups))


def unpacked_tail(packed, groups):
    rows = packed.shape[0]
    keep = lax.broadcasted_iota(jnp.int32, (rows, LANES), 1) < TAIL
    return jnp.concatenate(
        [jnp.where(keep, roll_lanes(packed, -TAIL * g), 0.0) for g in range(groups)], axis=0
    )


def bf16_pieces(x):
    hi = x.astype(BF16).astype(F32)
    rest = x - hi
    mid = rest.astype(BF16).astype(F32)
    return hi, mid, rest - mid


def extended(x, for_rows):
    hi, mid, lo = bf16_pieces(jnp.sum(x * x, axis=0, keepdims=True))
    r = lax.broadcasted_iota(jnp.int32, (8, LANES), 0)
    if for_rows:
        x = 2.0 * x
        head = jnp.where(r == 3, -hi, jnp.where(r == 4, -mid, jnp.where(r == 5, -lo, 0.0)))
        extra = jnp.where(r < 3, -1.0, head)
    else:
        head = jnp.where(r == 0, hi, jnp.where(r == 1, mid, jnp.where(r == 2, lo, 0.0)))
        extra = jnp.where((r >= 3) & (r < 6), 1.0, head)
    return jnp.concatenate([x, extra, jnp.zeros((LANES - F - 8, LANES), F32)], axis=0)


def eliminate(gram, right):
    cols = [jnp.broadcast_to(gram[:, m : m + 1], (K, LANES)) for m in range(K)]
    width = right.shape[1] // LANES
    sub = lax.broadcasted_iota(jnp.int32, (8, LANES), 0)
    cols = [[c[8 * g : 8 * g + 8] for g in range(4)] for c in cols]
    rt = [
        [right[8 * g : 8 * g + 8, w * LANES : (w + 1) * LANES] for w in range(width)]
        for g in range(4)
    ]
    out_rows = []
    for k in range(K):
        kg, kr = k // 8, k % 8
        pivot = cols[k][kg][kr : kr + 1]
        inv = 1.0 / pivot
        factor = [None] * 4
        for g in range(kg, 4):
            f = cols[k][g] * inv
            if g == kg:
                f = jnp.where(sub > kr, f, 0.0)
            factor[g] = f
        for m in range(k + 1, K):
            mg, mr = m // 8, m % 8
            upper = cols[k][mg][mr : mr + 1]
            for g in range(mg, 4):
                cols[m][g] = cols[m][g] - factor[g] * upper
        rows = [rt[kg][w][kr : kr + 1] for w in range(width)]
        scale = lax.rsqrt(pivot)
        out_rows.append([row * scale for row in rows])
        for g in range(kg, 4):
            for w in range(width):
                rt[g][w] = rt[g][w] - factor[g] * rows[w]
    tiles = []
    for g in range(4):
        tile = []
        for w in range(width):
            acc = jnp.broadcast_to(out_rows[8 * g][w], (8, LANES))
            for r in range(1, 8):
                acc = jnp.where(sub == r, out_rows[8 * g + r][w], acc)
            tile.append(acc)
        tiles.append(jnp.concatenate(tile, axis=1) if width > 1 else tile[0])
    return jnp.concatenate(tiles, axis=0)


def kernel(
    pts_hbm, vec_hbm, out_ref,
    pts_ref, vec_ref, stage, zbuf, jbuf, vbuf, xi, xj, panel, aff, acc, kept, psend, precv, sbuf, gsend, grecv,
    in_s, z_s, z_r, xy_s, xy_r, f_s, f_r, v_s, v_r, vf_s, vf_r,
    p_s, p_r, s_s, s_r, sf_s, sf_r, g_s, g_r,
):
    row = lax.axis_index("row")
    col = lax.axis_index("col")
    x, y = row // NY, lax.rem(row, NY)
    z, core = col // 2, lax.rem(col, 2)

    def xy_peer(e):
        q = e // NY
        to_x = lax.rem(x + q + (q // 2) * (5 - 2 * q), NX)
        to_y = lax.rem(y + e % NY, NY)
        return (to_x * NY + to_y, col)

    def z_peer(d):
        return (row, lax.rem(z + d + NZ, NZ) * 2 + core)

    def col_peer(d):
        return (row, lax.rem(col + d, NCOL))

    partner = (row, z * 2 + 1 - core)

    def remote(src, dst, send, recv, to):
        return pltpu.make_async_remote_copy(
            src_ref=src, dst_ref=dst, send_sem=send, recv_sem=recv,
            device_id=to, device_id_type=MESH,
        )

    pts_copy = pltpu.make_async_copy(pts_hbm, pts_ref, in_s.at[0])
    vec_copy = pltpu.make_async_copy(vec_hbm, vec_ref, in_s.at[1])
    pts_copy.start()
    vec_copy.start()
    barrier = pltpu.get_barrier_semaphore()
    with jax.named_scope("signal"):
        for d in range(1, NCOL):
            pl.semaphore_signal(barrier, inc=1, device_id=col_peer(d), device_id_type=MESH)
        for e in range(1, NXY):
            pl.semaphore_signal(barrier, inc=1, device_id=xy_peer(e), device_id_type=MESH)

    with jax.named_scope("prepare"):
        stage[...] = jnp.zeros_like(stage)
        pts_copy.wait()
        vec_copy.wait()
        stage[0:F, 0:OWN] = pts_ref[...].astype(F32)
        stage[F : F + K, 0:OWN] = vec_ref[...].astype(F32)
        t = stage[...]
        jbuf[0, 0, 0:64, :] = t[0:F, 0:LANES].astype(BF16)
        jbuf[0, 0, 64:80, :] = packed_tail(t[0:F, LANES:], 16).astype(BF16)
        vbuf[0, 0, 0:32, :] = t[F : F + K, 0:LANES].astype(BF16)
        vbuf[0, 0, 32:48, :] = packed_tail(t[F : F + K, LANES:], 16).astype(BF16)
        acc[...] = jnp.zeros_like(acc)
        for h in range(COLS_J // GROUP):
            panel[K : K + 16, h * GROUP : (h + 1) * GROUP] = (
                lax.broadcasted_iota(jnp.int32, (16, GROUP), 0) == 0
            ).astype(F32).astype(BF16)

    with jax.named_scope("barrier_wait"):
        pl.semaphore_wait(barrier, NCOL - 1 + NXY - 1)

    def z_copy(d):
        return remote(jbuf.at[0, 0], zbuf.at[d], z_s, z_r.at[d], z_peer(d))

    class Gathered:
        def __init__(self, buf, send, recv, on_send, on_recv):
            self.buf, self.send, self.recv, self.on_send, self.on_recv = buf, send, recv, on_send, on_recv

        def start(self, e):
            buf = self.buf
            remote(buf.at[0, 0], buf.at[0, e], self.send, self.recv.at[e // 4], xy_peer(e)).start()

        def group(self, q):
            pieces = [self.buf.at[half, pl.ds(q * 4, 4)] for half in range(2)]
            return remote(*pieces, self.on_send, self.on_recv.at[q], partner)

        def arrived(self, q):
            first, count = (1, 3) if isinstance(q, int) and q == 0 else (q * 4, 4)
            piece = self.buf.at[0, pl.ds(first, count)]
            remote(piece, piece, self.send, self.recv.at[q], partner).wait_recv()
            self.group(q).start()

        def forwarded(self, q):
            self.group(q).wait_recv()

        def sent(self):
            piece = self.buf.at[0, pl.ds(1, NXY - 1)]
            remote(piece, piece, self.send, self.recv.at[0], partner).wait_send()
            piece = self.buf.at[0]
            remote(piece, piece, self.on_send, self.on_recv.at[0], partner).wait_send()

    points = Gathered(jbuf, xy_s, xy_r, f_s, f_r)
    vectors = Gathered(vbuf, v_s, v_r, vf_s, vf_r)
    scaleds = Gathered(sbuf, s_s, s_r, sf_s, sf_r)

    with jax.named_scope("send_points"):
        for d in (4, 3, 5, 2, 6, 1, 7):
            z_copy(d).start()
        for q in range(NXY // 4):
            for gathered in (points, vectors):
                for e in range(max(1, 4 * q), 4 * q + 4):
                    gathered.start(e)

    def tails_of(tiles):
        return transposed_blocks([tile.astype(F32) for tile in tiles])

    with jax.named_scope("first_points"):
        points.arrived(0)

    with jax.named_scope("row_side"):
        for d in range(NZ):
            if d == 0:
                src = jbuf[0, 0, 0:64, :]
            else:
                z_copy(d).wait_recv()
                src = zbuf[d, 0:64, :]
            xi[:, d * LANES : (d + 1) * LANES] = extended(src.astype(F32), True).astype(BF16)
        for q in range(NZ // 4):
            tiles = [
                jbuf[0, 0, 64:80, :] if 4 * q + b == 0 else zbuf[4 * q + b, 64:80, :]
                for b in range(4)
            ]
            tile = jnp.concatenate(tails_of(tiles), axis=0)
            at = NZ * LANES + q * LANES
            xi[:, at : at + LANES] = extended(tile, True).astype(BF16)

    def affinity(q):
        base = pl.multiple_of(q * 2 * GROUP, 2 * GROUP)
        for half in range(2):
            for b in range(4):
                at = half * GROUP + b * LANES
                src = jbuf[half, q * 4 + b, 0:64, :].astype(F32)
                xj[at : at + LANES, :] = extended(src, False).T.astype(BF16)
            at = half * GROUP + 4 * LANES
            tile = tails_of([jbuf[half, q * 4 + b, 64:80, :] for b in range(4)])
            xj[at : at + LANES, :] = extended(jnp.concatenate(tile, axis=0), False).T.astype(BF16)
        for c in range(ROWS_I // 256):
            here = slice(c * 256, (c + 1) * 256)
            dist = jnp.dot(xj[...], xi[:, here], preferred_element_type=F32)
            weights = jnp.exp2(dist * (KERNEL_SCALE / F * math.log2(math.e)))
            aff[pl.ds(base, 2 * GROUP), here] = weights.astype(BF16)

    def vector_tiles(q, src, rows):
        base = pl.multiple_of(q * 2 * GROUP, 2 * GROUP)
        groups = rows // 16
        for half in range(2):
            for b in range(4):
                at = base + half * GROUP + b * LANES
                panel[0:rows, pl.ds(at, LANES)] = src[half, q * 4 + b, 0:rows, :]
            tile = tails_of([src[half, q * 4 + b, rows : rows + 16, :] for b in range(4)])[0:groups]
            at = base + half * GROUP + 4 * LANES
            panel[0:rows, pl.ds(at, LANES)] = jnp.concatenate(tile, axis=0).astype(BF16)

    def product(q, rows):
        base = pl.multiple_of(q * 2 * GROUP, 2 * GROUP)
        for c in range(ROWS_I // 256):
            here = slice(c * 256, (c + 1) * 256)
            acc[0:rows, here] += jnp.dot(
                panel[0:rows, pl.ds(base, 2 * GROUP)],
                aff[pl.ds(base, 2 * GROUP), here],
                preferred_element_type=F32,
            )

    with jax.named_scope("a_first_wait"):
        vectors.arrived(0)

    def work(q):
        vector_tiles(q, vbuf, K)
        affinity(q)
        product(q, K + 16)

    def step(q, carry):
        with jax.named_scope("a_wait"):
            points.arrived(q + 1)
            vectors.arrived(q + 1)
            points.forwarded(q)
            vectors.forwarded(q)
        with jax.named_scope("a_work"):
            work(q)
        return carry

    lax.fori_loop(0, 3, step, 0)
    with jax.named_scope("a_last_wait"):
        points.forwarded(3)
        vectors.forwarded(3)
    with jax.named_scope("a_last"):
        work(3)

    def p_copy(it, d):
        return remote(psend.at[it, d], precv.at[it, d], p_s.at[it], p_r.at[it], z_peer(-d))

    def p_all(it):
        return remote(
            psend.at[it, pl.ds(1, NZ - 1)], precv.at[it, pl.ds(1, NZ - 1)], p_s.at[it], p_r.at[it], partner
        )

    blocks16 = lax.broadcasted_iota(jnp.int32, (16, LANES), 1) // TAIL
    rows16 = lax.broadcasted_iota(jnp.int32, (16, LANES), 0)

    def send_product(it):
        for q in range(NZ // 4):
            at = NZ * LANES + q * LANES
            for b in range(4):
                d = 4 * q + b
                here = slice(d * LANES, (d + 1) * LANES)
                if d > 0:
                    psend[it, d, 0:K, :] = acc[0:K, here].astype(BF16)
                last = jnp.zeros((16, LANES), F32)
                if it == 0:
                    hi, mid, _ = bf16_pieces(acc[K : K + 8, here])
                    hi_t, mid_t, _ = bf16_pieces(acc[K : K + 8, at : at + LANES])
                    lines = [
                        roll_lanes(hi_t, TAIL * (2 - b)), roll_lanes(mid_t, TAIL * (2 - b)),
                        roll_lanes(hi, 64), hi, roll_lanes(mid, 64), mid,
                    ]
                    for r, line in enumerate(lines):
                        last = jnp.where(rows16 == r, line[0:1], last)
                last = jnp.where(blocks16 == 0, roll_lanes(acc[0:16, at : at + LANES], -TAIL * b), last)
                last = jnp.where(blocks16 == 1, roll_lanes(acc[16:32, at : at + LANES], TAIL * (1 - b)), last)
                if d > 0:
                    psend[it, d, K : K + 16, :] = last.astype(BF16)
                else:
                    kept[0:K, :] = acc[0:K, here]
                    kept[K : K + 16, :] = last
        for d in (4, 3, 5, 2, 6, 1, 7):
            p_copy(it, d).start()

    def received_product(it):
        p_all(it).wait_recv()
        total = kept[...]
        for d in range(1, NZ):
            total = total + precv[it, d].astype(F32)
        return total

    def degree_of(total):
        tail = roll_lanes(total[K : K + 1] + total[K + 1 : K + 2], 64)
        low = roll_lanes(total[K + 2 : K + 3] + total[K + 4 : K + 5], 64)
        high = total[K + 3 : K + 4] + total[K + 5 : K + 6]
        lane = lax.broadcasted_iota(jnp.int32, (1, LANES), 1)
        return jnp.where(lane < 64, low, high), jnp.where(lane < TAIL, tail, 1.0)

    def gram_of(scaled):
        wide = jnp.concatenate([scaled, jnp.zeros((LANES - K, 2 * LANES), F32)], axis=0)
        part = lax.dot_general(
            scaled, wide, (((1,), (1,)), ((), ())), precision=HIGHEST, preferred_element_type=F32
        )
        return packed_tail(part, 8)

    def g_copy(it, stage, n, to):
        return remote(gsend.at[it, stage], grecv.at[it, stage, n], g_s.at[it, stage], g_r.at[it, stage], to)

    def g_all(it, stage):
        piece = grecv.at[it, stage, pl.ds(1, 15)]
        return remote(piece, piece, g_s.at[it, stage], g_r.at[it, stage], partner)

    def g_total(it, stage):
        g_all(it, stage).wait_recv()
        terms = [gsend[it, stage]] + [grecv[it, stage, n] for n in range(1, 16)]
        while len(terms) > 1:
            terms = [a + b for a, b in zip(terms[::2], terms[1::2])]
        return terms[0]

    def gram_first(it, scaled):
        gsend[it, 0] = gram_of(scaled)
        for d in (8, 7, 9, 6, 10, 5, 11, 4, 12, 3, 13, 2, 14, 1, 15):
            g_copy(it, 0, d, col_peer(d)).start()

    def gram_second(it):
        gsend[it, 1] = g_total(it, 0)
        for e in range(NXY - 1, 0, -1):
            g_copy(it, 1, e, xy_peer(e)).start()

    def gram_last(it):
        return unpacked_tail(g_total(it, 1), 4) * (1.0 / TOTAL)

    with jax.named_scope("send1"):
        send_product(0)
    with jax.named_scope("reduce1"):
        total = received_product(0)
    with jax.named_scope("scale1"):
        deg_main, deg_tail = degree_of(total)
        scaled_main = total[0:K] / deg_main
        scaled_tail = unpacked_tail(total[K : K + 16], 2) / deg_tail
        scaled = jnp.concatenate([scaled_main, scaled_tail], axis=1)

        both = scaled
        if WIDE == 2:
            hi = scaled.astype(BF16).astype(F32)
            both = jnp.concatenate([hi, scaled - hi], axis=0)
        sbuf[0, 0, 0 : WIDE * K, :] = both[:, 0:LANES].astype(BF16)
        sbuf[0, 0, WIDE * K : WIDE * K + 16, :] = packed_tail(both[:, LANES:], 16).astype(BF16)
        for e in range(1, NXY):
            scaleds.start(e)
    with jax.named_scope("gram_first1"):
        gram_first(0, scaled)
        acc[...] = jnp.zeros_like(acc)

    with jax.named_scope("b_first_wait"):
        scaleds.arrived(0)
        scaleds.arrived(1)
        scaleds.forwarded(0)
    with jax.named_scope("b_first"):
        vector_tiles(0, sbuf, WIDE * K)
        product(0, WIDE * K)
    with jax.named_scope("b_second_wait"):
        scaleds.arrived(2)
        scaleds.forwarded(1)
    with jax.named_scope("b_second"):
        vector_tiles(1, sbuf, WIDE * K)
        product(1, WIDE * K)
    with jax.named_scope("b_third_wait"):
        scaleds.arrived(3)
        scaleds.forwarded(2)
    with jax.named_scope("b_third"):
        vector_tiles(2, sbuf, WIDE * K)
        product(2, WIDE * K)
    gram_second(0)
    with jax.named_scope("b_last_wait"):
        scaleds.forwarded(3)
    with jax.named_scope("b_last"):
        vector_tiles(3, sbuf, WIDE * K)
        product(3, WIDE * K)

    eye = (
        lax.broadcasted_iota(jnp.int32, (K, LANES), 0)
        == lax.broadcasted_iota(jnp.int32, (K, LANES), 1)
    ).astype(F32)
    with jax.named_scope("send2"):
        send_product(1)
    with jax.named_scope("gram_last1"):
        last = gram_last(0)
    with jax.named_scope("eliminate1"):
        inverse = eliminate(last, eye)
    with jax.named_scope("reduce2"):
        total = received_product(1)
    with jax.named_scope("scale2"):
        scaled = jnp.concatenate(
            [total[0:K] / deg_main, unpacked_tail(total[K : K + 16], 2) / deg_tail], axis=1
        )
        tall = jnp.concatenate([scaled, jnp.zeros((LANES - K, 2 * LANES), F32)], axis=0)
        scaled = jnp.dot(inverse, tall, precision=HIGHEST, preferred_element_type=F32)
    with jax.named_scope("gram_first2"):
        gram_first(1, scaled)
    with jax.named_scope("sent"):
        piece = zbuf.at[pl.ds(1, NZ - 1)]
        remote(piece, piece, z_s, z_r.at[0], partner).wait_send()
        for gathered in (points, vectors, scaleds):
            gathered.sent()
        for it in range(2):
            p_all(it).wait_send()
        for stage in range(2):
            g_all(0, stage).wait_send()
    with jax.named_scope("gram_second2"):
        gram_second(1)
    with jax.named_scope("gram_last2"):
        g_all(1, 0).wait_send()
        last = gram_last(1)
    with jax.named_scope("eliminate2"):
        ortho = eliminate(last, scaled)
        out_ref[...] = ortho[:, 0:OWN]

    with jax.named_scope("drain"):
        g_all(1, 1).wait_send()


def solution(mesh):
    dma = pltpu.SemaphoreType.DMA

    def shards(points, start_vectors):
        return pl.pallas_call(
            kernel,
            out_shape=jax.ShapeDtypeStruct((K, OWN), F32),
            in_specs=[pl.BlockSpec(memory_space=pltpu.HBM)] * 2,
            out_specs=pl.BlockSpec(memory_space=pltpu.VMEM),
            scratch_shapes=[
                pltpu.VMEM((F, OWN), BF16),
                pltpu.VMEM((K, OWN), BF16),
                pltpu.VMEM((F + K, 2 * LANES), F32),
                pltpu.VMEM((NZ, 80, LANES), BF16),
                pltpu.VMEM((2, NXY, 80, LANES), BF16),
                pltpu.VMEM((2, NXY, 48, LANES), BF16),
                pltpu.VMEM((LANES, ROWS_I), BF16),
                pltpu.VMEM((2 * GROUP, LANES), BF16),
                pltpu.VMEM((2 * K, COLS_J), BF16),
                pltpu.VMEM((COLS_J, ROWS_I), BF16),
                pltpu.VMEM((2 * K, ROWS_I), F32),
                pltpu.VMEM((K + 16, LANES), F32),
                pltpu.VMEM((2, NZ, K + 16, LANES), BF16),
                pltpu.VMEM((2, NZ, K + 16, LANES), BF16),
                pltpu.VMEM((2, NXY, WIDE * K + 16, LANES), BF16),
                pltpu.VMEM((2, 2, 8, LANES), F32),
                pltpu.VMEM((2, 2, 16, 8, LANES), F32),
                dma((2,)),
                dma, dma((NZ,)),
                dma, dma((4,)), dma, dma((4,)),
                dma, dma((4,)), dma, dma((4,)),
                dma((2,)), dma((2,)),
                dma, dma((4,)), dma, dma((4,)),
                dma((2, 2)), dma((2, 2)),
            ],
            compiler_params=pltpu.CompilerParams(
                collective_id=0, has_side_effects=True, vmem_limit_bytes=48 * 1024 * 1024
            ),
        )(*(pltpu.with_memory_space_constraint(v.T, pltpu.HBM) for v in (points, start_vectors))).T

    spec = P(("row", "col"), None)
    return jax.shard_map(
        shards, mesh=mesh, in_specs=(spec, spec), out_specs=spec, check_vma=False
    )
```

```python
import functools
import math

import jax
import jax.numpy as jnp
from jax import lax
from jax.experimental import pallas as pl
from jax.experimental.pallas import tpu as pltpu
from jax.sharding import PartitionSpec as P

MESH = pl.DeviceIdType.MESH
F32 = jnp.float32
BF16 = jnp.bfloat16
HIGHEST = lax.Precision.HIGHEST

KERNEL_SCALE = 5.12
F = 64
K = 32
OWN = 160
LANES = 128
TAIL = OWN - LANES
GROUP = 4 * OWN
NZ = 8
NX = 4
NY = 4
NXY = NX * NY
NCOL = 2 * NZ
ROWS_I = NZ * OWN
COLS_J = 2 * NXY * OWN
TOTAL = 256 * OWN


def roll_lanes(x, shift):
    shift = shift % LANES
    return x if shift == 0 else pltpu.roll(x, shift, 1)


def pick(blocks, pieces):
    out = pieces[3]
    for b in (2, 1, 0):
        out = jnp.where(blocks == b, pieces[b], out)
    return out


def transposed_blocks(tiles):
    rows = tiles[0].shape[0]
    blocks = lax.broadcasted_iota(jnp.int32, (rows, LANES), 1) // TAIL
    return [
        pick(blocks, [roll_lanes(tiles[b], TAIL * (b - g)) for b in range(4)]) for g in range(4)
    ]


def packed_tail(tail, rows):
    groups = tail.shape[0] // rows
    return sum(roll_lanes(tail[g * rows : (g + 1) * rows], TAIL * g) for g in range(groups))


def unpacked_tail(packed, groups):
    rows = packed.shape[0]
    keep = lax.broadcasted_iota(jnp.int32, (rows, LANES), 1) < TAIL
    return jnp.concatenate(
        [jnp.where(keep, roll_lanes(packed, -TAIL * g), 0.0) for g in range(groups)], axis=0
    )


def bf16_pieces(x):
    hi = x.astype(BF16).astype(F32)
    rest = x - hi
    mid = rest.astype(BF16).astype(F32)
    return hi, mid, rest - mid


def extended(x, for_rows):
    hi, mid, lo = bf16_pieces(jnp.sum(x * x, axis=0, keepdims=True))
    r = lax.broadcasted_iota(jnp.int32, (8, LANES), 0)
    if for_rows:
        x = 2.0 * x
        head = jnp.where(r == 3, -hi, jnp.where(r == 4, -mid, jnp.where(r == 5, -lo, 0.0)))
        extra = jnp.where(r < 3, -1.0, head)
    else:
        head = jnp.where(r == 0, hi, jnp.where(r == 1, mid, jnp.where(r == 2, lo, 0.0)))
        extra = jnp.where((r >= 3) & (r < 6), 1.0, head)
    return jnp.concatenate([x, extra, jnp.zeros((LANES - F - 8, LANES), F32)], axis=0)


def eliminate(gram, right):
    cols = [jnp.broadcast_to(gram[:, m : m + 1], (K, LANES)) for m in range(K)]
    width = right.shape[1] // LANES
    sub = lax.broadcasted_iota(jnp.int32, (8, LANES), 0)
    cols = [[c[8 * g : 8 * g + 8] for g in range(4)] for c in cols]
    rt = [
        [right[8 * g : 8 * g + 8, w * LANES : (w + 1) * LANES] for w in range(width)]
        for g in range(4)
    ]
    out_rows = []
    for k in range(K):
        kg, kr = k // 8, k % 8
        pivot = cols[k][kg][kr : kr + 1]
        inv = 1.0 / pivot
        factor = [None] * 4
        for g in range(kg, 4):
            f = cols[k][g] * inv
            if g == kg:
                f = jnp.where(sub > kr, f, 0.0)
            factor[g] = f
        for m in range(k + 1, K):
            mg, mr = m // 8, m % 8
            upper = cols[k][mg][mr : mr + 1]
            for g in range(mg, 4):
                cols[m][g] = cols[m][g] - factor[g] * upper
        rows = [rt[kg][w][kr : kr + 1] for w in range(width)]
        scale = lax.rsqrt(pivot)
        out_rows.append([row * scale for row in rows])
        for g in range(kg, 4):
            for w in range(width):
                rt[g][w] = rt[g][w] - factor[g] * rows[w]
    tiles = []
    for g in range(4):
        tile = []
        for w in range(width):
            acc = jnp.broadcast_to(out_rows[8 * g][w], (8, LANES))
            for r in range(1, 8):
                acc = jnp.where(sub == r, out_rows[8 * g + r][w], acc)
            tile.append(acc)
        tiles.append(jnp.concatenate(tile, axis=1) if width > 1 else tile[0])
    return jnp.concatenate(tiles, axis=0)


def kernel(
    pts_hbm, vec_hbm, out_ref,
    pts_ref, vec_ref, stage, zbuf, jbuf, vbuf, xi, xj, panel, aff, acc, kept, psend, precv, sbuf, gsend, grecv,
    in_s, z_s, z_r, xy_s, xy_r, f_s, f_r, v_s, v_r, vf_s, vf_r,
    p_s, p_r, s_s, s_r, sf_s, sf_r, g_s, g_r,
):
    row = lax.axis_index("row")
    col = lax.axis_index("col")
    x, y = row // NY, lax.rem(row, NY)
    z, core = col // 2, lax.rem(col, 2)

    def xy_peer(e):
        q = e // NY
        to_x = lax.rem(x + q + (q // 2) * (5 - 2 * q), NX)
        to_y = lax.rem(y + e % NY, NY)
        return (to_x * NY + to_y, col)

    def z_peer(d):
        return (row, lax.rem(z + d + NZ, NZ) * 2 + core)

    def col_peer(d):
        return (row, lax.rem(col + d, NCOL))

    partner = (row, z * 2 + 1 - core)

    def remote(src, dst, send, recv, to):
        return pltpu.make_async_remote_copy(
            src_ref=src, dst_ref=dst, send_sem=send, recv_sem=recv,
            device_id=to, device_id_type=MESH,
        )

    pts_copy = pltpu.make_async_copy(pts_hbm, pts_ref, in_s.at[0])
    vec_copy = pltpu.make_async_copy(vec_hbm, vec_ref, in_s.at[1])
    pts_copy.start()
    vec_copy.start()
    barrier = pltpu.get_barrier_semaphore()
    with jax.named_scope("signal"):
        for d in range(1, NCOL):
            pl.semaphore_signal(barrier, inc=1, device_id=col_peer(d), device_id_type=MESH)
        for e in range(1, NXY):
            pl.semaphore_signal(barrier, inc=1, device_id=xy_peer(e), device_id_type=MESH)

    with jax.named_scope("prepare"):
        stage[...] = jnp.zeros_like(stage)
        pts_copy.wait()
        vec_copy.wait()
        stage[0:F, 0:OWN] = pts_ref[...].astype(F32)
        stage[F : F + K, 0:OWN] = vec_ref[...].astype(F32)
        t = stage[...]
        jbuf[0, 0, 0:64, :] = t[0:F, 0:LANES].astype(BF16)
        jbuf[0, 0, 64:80, :] = packed_tail(t[0:F, LANES:], 16).astype(BF16)
        vbuf[0, 0, 0:32, :] = t[F : F + K, 0:LANES].astype(BF16)
        vbuf[0, 0, 32:48, :] = packed_tail(t[F : F + K, LANES:], 16).astype(BF16)
        acc[...] = jnp.zeros_like(acc)
        for h in range(COLS_J // GROUP):
            panel[K : K + 16, h * GROUP : (h + 1) * GROUP] = (
                lax.broadcasted_iota(jnp.int32, (16, GROUP), 0) == 0
            ).astype(F32).astype(BF16)

    with jax.named_scope("barrier_wait"):
        pl.semaphore_wait(barrier, NCOL - 1 + NXY - 1)

    def z_copy(d):
        return remote(jbuf.at[0, 0], zbuf.at[d], z_s, z_r.at[d], z_peer(d))

    class Gathered:
        def __init__(self, buf, send, recv, on_send, on_recv):
            self.buf, self.send, self.recv, self.on_send, self.on_recv = buf, send, recv, on_send, on_recv

        def start(self, p):
            for e in range(max(1, 8 * p), 8 * p + 8):
                remote(
                    self.buf.at[0, 0], self.buf.at[0, e], self.send.at[p], self.recv.at[p], xy_peer(e)
                ).start()

        def piece(self, p):
            first = max(1, 8 * p)
            piece = self.buf.at[0, pl.ds(first, 8 * p + 8 - first)]
            return remote(piece, piece, self.send.at[p], self.recv.at[p], partner)

        def group(self, p):
            pieces = [self.buf.at[half, pl.ds(p * 8, 8)] for half in range(2)]
            return remote(*pieces, self.on_send.at[p], self.on_recv.at[p], partner)

        def arrived(self, p):
            self.piece(p).wait_recv()
            self.group(p).start()

        def forwarded(self, p):
            self.group(p).wait_recv()

        def left(self, p):
            self.piece(p).wait_send()

        def sent(self):
            for p in range(2):
                self.group(p).wait_send()

    points = Gathered(jbuf, xy_s, xy_r, f_s, f_r)
    vectors = Gathered(vbuf, v_s, v_r, vf_s, vf_r)
    scaleds = Gathered(sbuf, s_s, s_r, sf_s, sf_r)

    with jax.named_scope("send_points"):
        for d in (4, 3, 5, 2, 6, 1, 7):
            z_copy(d).start()
        points.start(0)
    with jax.named_scope("left_points"):
        points.left(0)
        vectors.start(0)
        points.start(1)
        vectors.left(0)
        vectors.start(1)

    def tails_of(tiles):
        return transposed_blocks([tile.astype(F32) for tile in tiles])

    with jax.named_scope("first_points"):
        points.arrived(0)

    with jax.named_scope("row_side"):
        for d in range(NZ):
            if d == 0:
                src = jbuf[0, 0, 0:64, :]
            else:
                z_copy(d).wait_recv()
                src = zbuf[d, 0:64, :]
            xi[:, d * LANES : (d + 1) * LANES] = extended(src.astype(F32), True).astype(BF16)
        for q in range(NZ // 4):
            tiles = [
                jbuf[0, 0, 64:80, :] if 4 * q + b == 0 else zbuf[4 * q + b, 64:80, :]
                for b in range(4)
            ]
            tile = jnp.concatenate(tails_of(tiles), axis=0)
            at = NZ * LANES + q * LANES
            xi[:, at : at + LANES] = extended(tile, True).astype(BF16)

    def slots(h, sub):
        return [(h % 2, h // 2 * 8 + sub * 4 + b) for b in range(4)]

    def affinity(h):
        base = pl.multiple_of(h * 2 * GROUP, 2 * GROUP)
        for sub in range(2):
            for b, (core_set, e) in enumerate(slots(h, sub)):
                at = sub * GROUP + b * LANES
                src = jbuf[core_set, e, 0:64, :].astype(F32)
                xj[at : at + LANES, :] = extended(src, False).T.astype(BF16)
            at = sub * GROUP + 4 * LANES
            tile = tails_of([jbuf[core_set, e, 64:80, :] for core_set, e in slots(h, sub)])
            xj[at : at + LANES, :] = extended(jnp.concatenate(tile, axis=0), False).T.astype(BF16)
        for c in range(ROWS_I // 256):
            here = slice(c * 256, (c + 1) * 256)
            dist = jnp.dot(xj[...], xi[:, here], preferred_element_type=F32)
            weights = jnp.exp2(dist * (KERNEL_SCALE / F * math.log2(math.e)))
            aff[pl.ds(base, 2 * GROUP), here] = weights.astype(BF16)

    def vector_tiles(h, src):
        base = pl.multiple_of(h * 2 * GROUP, 2 * GROUP)
        for sub in range(2):
            for b, (core_set, e) in enumerate(slots(h, sub)):
                at = base + sub * GROUP + b * LANES
                panel[0:K, pl.ds(at, LANES)] = src[core_set, e, 0:K, :]
            tile = tails_of([src[core_set, e, K : K + 16, :] for core_set, e in slots(h, sub)])[0:2]
            at = base + sub * GROUP + 4 * LANES
            panel[0:K, pl.ds(at, LANES)] = jnp.concatenate(tile, axis=0).astype(BF16)

    def product(h, rows):
        base = pl.multiple_of(h * 2 * GROUP, 2 * GROUP)
        for c in range(ROWS_I // 256):
            here = slice(c * 256, (c + 1) * 256)
            acc[0:rows, here] += jnp.dot(
                panel[0:rows, pl.ds(base, 2 * GROUP)],
                aff[pl.ds(base, 2 * GROUP), here],
                preferred_element_type=F32,
            )

    def next_wait(h, gathered):
        for step, waits in ((1, "forwarded"), (2, "arrived"), (3, "forwarded")):

            @pl.when(h == step)
            def _():
                for g in gathered:
                    getattr(g, waits)(step // 2)

    def first_step(h, carry):
        with jax.named_scope("a_wait"):
            next_wait(h, (points, vectors))
        with jax.named_scope("a_work"):
            vector_tiles(h, vbuf)
            affinity(h)
            product(h, K + 16)
        return carry

    with jax.named_scope("a_first"):
        affinity(0)
    with jax.named_scope("a_first_wait"):
        vectors.arrived(0)
    with jax.named_scope("a_first_product"):
        vector_tiles(0, vbuf)
        product(0, K + 16)
    lax.fori_loop(1, 4, first_step, 0)

    def p_copy(it, d):
        return remote(psend.at[it, d], precv.at[it, d], p_s.at[it], p_r.at[it], z_peer(-d))

    def p_all(it):
        return remote(
            psend.at[it, pl.ds(1, NZ - 1)], precv.at[it, pl.ds(1, NZ - 1)], p_s.at[it], p_r.at[it], partner
        )

    blocks16 = lax.broadcasted_iota(jnp.int32, (16, LANES), 1) // TAIL
    rows16 = lax.broadcasted_iota(jnp.int32, (16, LANES), 0)

    def send_product(it):
        for q in range(NZ // 4):
            at = NZ * LANES + q * LANES
            for b in range(4):
                d = 4 * q + b
                here = slice(d * LANES, (d + 1) * LANES)
                if d > 0:
                    psend[it, d, 0:K, :] = acc[0:K, here].astype(BF16)
                last = jnp.zeros((16, LANES), F32)
                if it == 0:
                    hi, mid, _ = bf16_pieces(acc[K : K + 8, here])
                    hi_t, mid_t, _ = bf16_pieces(acc[K : K + 8, at : at + LANES])
                    lines = [
                        roll_lanes(hi_t, TAIL * (2 - b)), roll_lanes(mid_t, TAIL * (2 - b)),
                        roll_lanes(hi, 64), hi, roll_lanes(mid, 64), mid,
                    ]
                    for r, line in enumerate(lines):
                        last = jnp.where(rows16 == r, line[0:1], last)
                last = jnp.where(blocks16 == 0, roll_lanes(acc[0:16, at : at + LANES], -TAIL * b), last)
                last = jnp.where(blocks16 == 1, roll_lanes(acc[16:32, at : at + LANES], TAIL * (1 - b)), last)
                if d > 0:
                    psend[it, d, K : K + 16, :] = last.astype(BF16)
                else:
                    kept[0:K, :] = acc[0:K, here]
                    kept[K : K + 16, :] = last
        for d in (4, 3, 5, 2, 6, 1, 7):
            p_copy(it, d).start()

    def received_product(it):
        p_all(it).wait_recv()
        total = kept[...]
        for d in range(1, NZ):
            total = total + precv[it, d].astype(F32)
        return total

    def degree_of(total):
        tail = roll_lanes(total[K : K + 1] + total[K + 1 : K + 2], 64)
        low = roll_lanes(total[K + 2 : K + 3] + total[K + 4 : K + 5], 64)
        high = total[K + 3 : K + 4] + total[K + 5 : K + 6]
        lane = lax.broadcasted_iota(jnp.int32, (1, LANES), 1)
        return jnp.where(lane < 64, low, high), jnp.where(lane < TAIL, tail, 1.0)

    def gram_of(scaled):
        wide = jnp.concatenate([scaled, jnp.zeros((LANES - K, 2 * LANES), F32)], axis=0)
        part = lax.dot_general(
            scaled, wide, (((1,), (1,)), ((), ())), precision=HIGHEST, preferred_element_type=F32
        )
        return packed_tail(part, 8)

    def g_copy(it, stage, n, to):
        return remote(gsend.at[it, stage], grecv.at[it, stage, n], g_s.at[it, stage], g_r.at[it, stage], to)

    def g_all(it, stage):
        piece = grecv.at[it, stage, pl.ds(1, 15)]
        return remote(piece, piece, g_s.at[it, stage], g_r.at[it, stage], partner)

    def g_total(it, stage):
        g_all(it, stage).wait_recv()
        terms = [gsend[it, stage]] + [grecv[it, stage, n] for n in range(1, 16)]
        while len(terms) > 1:
            terms = [a + b for a, b in zip(terms[::2], terms[1::2])]
        return terms[0]

    def gram_first(it, scaled):
        gsend[it, 0] = gram_of(scaled)
        for d in (8, 7, 9, 6, 10, 5, 11, 4, 12, 3, 13, 2, 14, 1, 15):
            g_copy(it, 0, d, col_peer(d)).start()

    def gram_second(it):
        gsend[it, 1] = g_total(it, 0)
        for e in range(NXY - 1, 0, -1):
            g_copy(it, 1, e, xy_peer(e)).start()

    def gram_last(it):
        return unpacked_tail(g_total(it, 1), 4) * (1.0 / TOTAL)

    with jax.named_scope("send1"):
        send_product(0)
    with jax.named_scope("reduce1"):
        total = received_product(0)
    with jax.named_scope("scale1"):
        deg_main, deg_tail = degree_of(total)
        scaled_main = total[0:K] / deg_main
        scaled_tail = unpacked_tail(total[K : K + 16], 2) / deg_tail
        scaled = jnp.concatenate([scaled_main, scaled_tail], axis=1)

        sbuf[0, 0, 0:K, :] = scaled[:, 0:LANES].astype(BF16)
        sbuf[0, 0, K : K + 16, :] = packed_tail(scaled[:, LANES:], 16).astype(BF16)
        scaleds.start(0)
        scaleds.start(1)
    with jax.named_scope("gram_first1"):
        gram_first(0, scaled)

    with jax.named_scope("b_left"):
        lo = (scaled - scaled.astype(BF16).astype(F32)).astype(BF16)
        acc[0:K, :] = jnp.dot(lo[:, 0:LANES], aff[0:LANES, :], preferred_element_type=F32) + jnp.dot(
            lo[:, LANES:], aff[4 * LANES : 5 * LANES, :], preferred_element_type=F32
        )
    with jax.named_scope("b_0_wait"):
        scaleds.arrived(0)
    with jax.named_scope("b_0"):
        vector_tiles(0, sbuf)
        product(0, K)
    with jax.named_scope("b_1_wait"):
        scaleds.arrived(1)
        scaleds.forwarded(0)
    with jax.named_scope("b_12"):
        for h in (1, 2):
            vector_tiles(h, sbuf)
            product(h, K)
    gram_second(0)
    with jax.named_scope("b_3_wait"):
        scaleds.forwarded(1)
    with jax.named_scope("b_3"):
        vector_tiles(3, sbuf)
        product(3, K)

    eye = (
        lax.broadcasted_iota(jnp.int32, (K, LANES), 0)
        == lax.broadcasted_iota(jnp.int32, (K, LANES), 1)
    ).astype(F32)
    with jax.named_scope("send2"):
        send_product(1)
    with jax.named_scope("gram_last1"):
        last = gram_last(0)
    with jax.named_scope("eliminate1"):
        inverse = eliminate(last, eye)
    with jax.named_scope("reduce2"):
        total = received_product(1)
    with jax.named_scope("scale2"):
        scaled = jnp.concatenate(
            [total[0:K] / deg_main, unpacked_tail(total[K : K + 16], 2) / deg_tail], axis=1
        )
        tall = jnp.concatenate([scaled, jnp.zeros((LANES - K, 2 * LANES), F32)], axis=0)
        scaled = jnp.dot(inverse, tall, precision=HIGHEST, preferred_element_type=F32)
    with jax.named_scope("gram_first2"):
        gram_first(1, scaled)
    with jax.named_scope("sent"):
        piece = zbuf.at[pl.ds(1, NZ - 1)]
        remote(piece, piece, z_s, z_r.at[0], partner).wait_send()
        points.left(1)
        vectors.left(1)
        for p in range(2):
            scaleds.left(p)
        for gathered in (points, vectors, scaleds):
            gathered.sent()
        for it in range(2):
            p_all(it).wait_send()
        for stage in range(2):
            g_all(0, stage).wait_send()
    with jax.named_scope("gram_second2"):
        gram_second(1)
    with jax.named_scope("gram_last2"):
        g_all(1, 0).wait_send()
        last = gram_last(1)
    with jax.named_scope("eliminate2"):
        ortho = eliminate(last, scaled)
        out_ref[...] = ortho[:, 0:OWN]

    with jax.named_scope("drain"):
        g_all(1, 1).wait_send()


def solution(mesh):
    dma = pltpu.SemaphoreType.DMA

    def shards(points, start_vectors):
        return pl.pallas_call(
            kernel,
            out_shape=jax.ShapeDtypeStruct((K, OWN), F32),
            in_specs=[pl.BlockSpec(memory_space=pltpu.HBM)] * 2,
            out_specs=pl.BlockSpec(memory_space=pltpu.VMEM),
            scratch_shapes=[
                pltpu.VMEM((F, OWN), BF16),
                pltpu.VMEM((K, OWN), BF16),
                pltpu.VMEM((F + K, 2 * LANES), F32),
                pltpu.VMEM((NZ, 80, LANES), BF16),
                pltpu.VMEM((2, NXY, 80, LANES), BF16),
                pltpu.VMEM((2, NXY, 48, LANES), BF16),
                pltpu.VMEM((LANES, ROWS_I), BF16),
                pltpu.VMEM((2 * GROUP, LANES), BF16),
                pltpu.VMEM((2 * K, COLS_J), BF16),
                pltpu.VMEM((COLS_J, ROWS_I), BF16),
                pltpu.VMEM((2 * K, ROWS_I), F32),
                pltpu.VMEM((K + 16, LANES), F32),
                pltpu.VMEM((2, NZ, K + 16, LANES), BF16),
                pltpu.VMEM((2, NZ, K + 16, LANES), BF16),
                pltpu.VMEM((2, NXY, K + 16, LANES), BF16),
                pltpu.VMEM((2, 2, 8, LANES), F32),
                pltpu.VMEM((2, 2, 16, 8, LANES), F32),
                dma((2,)),
                dma, dma((NZ,)),
                dma((2,)), dma((2,)), dma((2,)), dma((2,)),
                dma((2,)), dma((2,)), dma((2,)), dma((2,)),
                dma((2,)), dma((2,)),
                dma((2,)), dma((2,)), dma((2,)), dma((2,)),
                dma((2, 2)), dma((2, 2)),
            ],
            compiler_params=pltpu.CompilerParams(
                collective_id=0, has_side_effects=True, vmem_limit_bytes=48 * 1024 * 1024
            ),
        )(*(pltpu.with_memory_space_constraint(v.T, pltpu.HBM) for v in (points, start_vectors))).T

    spec = P(("row", "col"), None)
    return jax.shard_map(
        shards, mesh=mesh, in_specs=(spec, spec), out_specs=spec, check_vma=False
    )
```

```python
import functools
import math

import jax
import jax.numpy as jnp
from jax import lax
from jax.experimental import pallas as pl
from jax.experimental.pallas import tpu as pltpu
from jax.sharding import PartitionSpec as P

MESH = pl.DeviceIdType.MESH
F32 = jnp.float32
BF16 = jnp.bfloat16
HIGHEST = lax.Precision.HIGHEST

KERNEL_SCALE = 5.12
F = 64
K = 32
OWN = 160
LANES = 128
TAIL = OWN - LANES
GROUP = 4 * OWN
NZ = 8
NX = 4
NY = 4
NXY = NX * NY
NCOL = 2 * NZ
FAR_FIRST = (8, 7, 9, 6, 10, 5, 11, 4, 12, 3, 13, 2, 14, 1, 15)
ROWS_I = NZ * OWN
COLS_J = 2 * NXY * OWN
TOTAL = 256 * OWN


def roll_lanes(x, shift):
    shift = shift % LANES
    return x if shift == 0 else pltpu.roll(x, shift, 1)


def pick(blocks, pieces):
    out = pieces[3]
    for b in (2, 1, 0):
        out = jnp.where(blocks == b, pieces[b], out)
    return out


def transposed_blocks(tiles):
    rows = tiles[0].shape[0]
    blocks = lax.broadcasted_iota(jnp.int32, (rows, LANES), 1) // TAIL
    return [
        pick(blocks, [roll_lanes(tiles[b], TAIL * (b - g)) for b in range(4)]) for g in range(4)
    ]


def packed_tail(tail, rows):
    groups = tail.shape[0] // rows
    return sum(roll_lanes(tail[g * rows : (g + 1) * rows], TAIL * g) for g in range(groups))


def unpacked_tail(packed, groups):
    rows = packed.shape[0]
    keep = lax.broadcasted_iota(jnp.int32, (rows, LANES), 1) < TAIL
    return jnp.concatenate(
        [jnp.where(keep, roll_lanes(packed, -TAIL * g), 0.0) for g in range(groups)], axis=0
    )


def bf16_pieces(x):
    hi = x.astype(BF16).astype(F32)
    rest = x - hi
    mid = rest.astype(BF16).astype(F32)
    return hi, mid, rest - mid


def extended(x, for_rows):
    hi, mid, lo = bf16_pieces(jnp.sum(x * x, axis=0, keepdims=True))
    r = lax.broadcasted_iota(jnp.int32, (8, LANES), 0)
    if for_rows:
        x = 2.0 * x
        head = jnp.where(r == 3, -hi, jnp.where(r == 4, -mid, jnp.where(r == 5, -lo, 0.0)))
        extra = jnp.where(r < 3, -1.0, head)
    else:
        head = jnp.where(r == 0, hi, jnp.where(r == 1, mid, jnp.where(r == 2, lo, 0.0)))
        extra = jnp.where((r >= 3) & (r < 6), 1.0, head)
    return jnp.concatenate([x, extra, jnp.zeros((LANES - F - 8, LANES), F32)], axis=0)


def eliminate(gram, right):
    cols = [jnp.broadcast_to(gram[:, m : m + 1], (K, LANES)) for m in range(K)]
    width = right.shape[1] // LANES
    sub = lax.broadcasted_iota(jnp.int32, (8, LANES), 0)
    cols = [[c[8 * g : 8 * g + 8] for g in range(4)] for c in cols]
    rt = [
        [right[8 * g : 8 * g + 8, w * LANES : (w + 1) * LANES] for w in range(width)]
        for g in range(4)
    ]
    out_rows = []
    for k in range(K):
        kg, kr = k // 8, k % 8
        pivot = cols[k][kg][kr : kr + 1]
        inv = 1.0 / pivot
        factor = [None] * 4
        for g in range(kg, 4):
            f = cols[k][g] * inv
            if g == kg:
                f = jnp.where(sub > kr, f, 0.0)
            factor[g] = f
        for m in range(k + 1, K):
            mg, mr = m // 8, m % 8
            upper = cols[k][mg][mr : mr + 1]
            for g in range(mg, 4):
                cols[m][g] = cols[m][g] - factor[g] * upper
        rows = [rt[kg][w][kr : kr + 1] for w in range(width)]
        scale = lax.rsqrt(pivot)
        out_rows.append([row * scale for row in rows])
        for g in range(kg, 4):
            for w in range(width):
                rt[g][w] = rt[g][w] - factor[g] * rows[w]
    tiles = []
    for g in range(4):
        tile = []
        for w in range(width):
            acc = jnp.broadcast_to(out_rows[8 * g][w], (8, LANES))
            for r in range(1, 8):
                acc = jnp.where(sub == r, out_rows[8 * g + r][w], acc)
            tile.append(acc)
        tiles.append(jnp.concatenate(tile, axis=1) if width > 1 else tile[0])
    return jnp.concatenate(tiles, axis=0)


def kernel(
    pts_hbm, vec_hbm, out_ref,
    pts_ref, vec_ref, stage, zbuf, jbuf, vbuf, xi, xj, panel, aff, acc, kept, psend, precv, sbuf, gsend, grecv,
    in_s, z_s, z_r, xy_s, xy_r, f_s, f_r, v_s, v_r, vf_s, vf_r,
    p_s, p_r, s_s, s_r, sf_s, sf_r, g_s, g_r,
):
    row = lax.axis_index("row")
    col = lax.axis_index("col")
    x, y = row // NY, lax.rem(row, NY)
    z, core = col // 2, lax.rem(col, 2)

    def xy_peer(e):
        q = e // NY
        to_x = lax.rem(x + q + (q // 2) * (5 - 2 * q), NX)
        to_y = lax.rem(y + e % NY, NY)
        return (to_x * NY + to_y, col)

    def z_peer(d):
        return (row, lax.rem(z + d + NZ, NZ) * 2 + core)

    def col_peer(d):
        return (row, lax.rem(col + d, NCOL))

    partner = (row, z * 2 + 1 - core)

    def remote(src, dst, send, recv, to):
        return pltpu.make_async_remote_copy(
            src_ref=src, dst_ref=dst, send_sem=send, recv_sem=recv,
            device_id=to, device_id_type=MESH,
        )

    pts_copy = pltpu.make_async_copy(pts_hbm, pts_ref, in_s.at[0])
    vec_copy = pltpu.make_async_copy(vec_hbm, vec_ref, in_s.at[1])
    pts_copy.start()
    vec_copy.start()
    barrier = pltpu.get_barrier_semaphore()
    with jax.named_scope("signal"):
        for d in FAR_FIRST:
            pl.semaphore_signal(barrier, inc=1, device_id=col_peer(d), device_id_type=MESH)
        for e in range(NXY - 1, 0, -1):
            pl.semaphore_signal(barrier, inc=1, device_id=xy_peer(e), device_id_type=MESH)

    with jax.named_scope("prepare"):
        stage[...] = jnp.zeros_like(stage)
        pts_copy.wait()
        vec_copy.wait()
        stage[0:F, 0:OWN] = pts_ref[...].astype(F32)
        stage[F : F + K, 0:OWN] = vec_ref[...].astype(F32)
        t = stage[...]
        jbuf[0, 0, 0:64, :] = t[0:F, 0:LANES].astype(BF16)
        jbuf[0, 0, 64:80, :] = packed_tail(t[0:F, LANES:], 16).astype(BF16)
        vbuf[0, 0, 0:32, :] = t[F : F + K, 0:LANES].astype(BF16)
        vbuf[0, 0, 32:48, :] = packed_tail(t[F : F + K, LANES:], 16).astype(BF16)
        acc[...] = jnp.zeros_like(acc)
        for h in range(COLS_J // GROUP):
            panel[K : K + 16, h * GROUP : (h + 1) * GROUP] = (
                lax.broadcasted_iota(jnp.int32, (16, GROUP), 0) == 0
            ).astype(F32).astype(BF16)

    with jax.named_scope("barrier_wait"):
        pl.semaphore_wait(barrier, NCOL - 1 + NXY - 1)

    def z_copy(d):
        return remote(jbuf.at[0, 0], zbuf.at[d], z_s, z_r.at[d], z_peer(d))

    class Gathered:
        def __init__(self, buf, send, recv, on_send, on_recv):
            self.buf, self.send, self.recv, self.on_send, self.on_recv = buf, send, recv, on_send, on_recv

        def start(self, p):
            for e in range(max(1, 8 * p), 8 * p + 8):
                remote(
                    self.buf.at[0, 0], self.buf.at[0, e], self.send.at[p], self.recv.at[p], xy_peer(e)
                ).start()

        def piece(self, p):
            first = max(1, 8 * p)
            piece = self.buf.at[0, pl.ds(first, 8 * p + 8 - first)]
            return remote(piece, piece, self.send.at[p], self.recv.at[p], partner)

        def group(self, p):
            pieces = [self.buf.at[half, pl.ds(p * 8, 8)] for half in range(2)]
            return remote(*pieces, self.on_send.at[p], self.on_recv.at[p], partner)

        def arrived(self, p):
            self.piece(p).wait_recv()
            self.group(p).start()

        def forwarded(self, p):
            self.group(p).wait_recv()

        def left(self, p):
            self.piece(p).wait_send()

        def sent(self):
            for p in range(2):
                self.group(p).wait_send()

    points = Gathered(jbuf, xy_s, xy_r, f_s, f_r)
    vectors = Gathered(vbuf, v_s, v_r, vf_s, vf_r)
    scaleds = Gathered(sbuf, s_s, s_r, sf_s, sf_r)

    with jax.named_scope("send_points"):
        for d in (4, 3, 5, 2, 6, 1, 7):
            z_copy(d).start()
        points.start(0)
    with jax.named_scope("left_points"):
        points.left(0)
        vectors.start(0)
        points.start(1)
        vectors.left(0)
        vectors.start(1)

    def tails_of(tiles):
        return transposed_blocks([tile.astype(F32) for tile in tiles])

    with jax.named_scope("first_points"):
        points.arrived(0)

    with jax.named_scope("row_side"):
        for d in (0, 1, 7, 2, 6, 3, 5, 4):
            if d == 0:
                src = jbuf[0, 0, 0:64, :]
            else:
                z_copy(d).wait_recv()
                src = zbuf[d, 0:64, :]
            xi[:, d * LANES : (d + 1) * LANES] = extended(src.astype(F32), True).astype(BF16)
        for q in range(NZ // 4):
            tiles = [
                jbuf[0, 0, 64:80, :] if 4 * q + b == 0 else zbuf[4 * q + b, 64:80, :]
                for b in range(4)
            ]
            tile = jnp.concatenate(tails_of(tiles), axis=0)
            at = NZ * LANES + q * LANES
            xi[:, at : at + LANES] = extended(tile, True).astype(BF16)

    def slots(h, sub):
        return [(h % 2, h // 2 * 8 + sub * 4 + b) for b in range(4)]

    def affinity(h):
        base = pl.multiple_of(h * 2 * GROUP, 2 * GROUP)
        for sub in range(2):
            for b, (core_set, e) in enumerate(slots(h, sub)):
                at = sub * GROUP + b * LANES
                src = jbuf[core_set, e, 0:64, :].astype(F32)
                xj[at : at + LANES, :] = extended(src, False).astype(BF16).T
            at = sub * GROUP + 4 * LANES
            tile = tails_of([jbuf[core_set, e, 64:80, :] for core_set, e in slots(h, sub)])
            xj[at : at + LANES, :] = extended(jnp.concatenate(tile, axis=0), False).astype(BF16).T
        for c in range(ROWS_I // 256):
            here = slice(c * 256, (c + 1) * 256)
            dist = jnp.dot(xj[...], xi[:, here], preferred_element_type=F32)
            weights = jnp.exp2(dist * (KERNEL_SCALE / F * math.log2(math.e)))
            aff[pl.ds(base, 2 * GROUP), here] = weights.astype(BF16)

    def vector_tiles(h, src):
        base = pl.multiple_of(h * 2 * GROUP, 2 * GROUP)
        for sub in range(2):
            for b, (core_set, e) in enumerate(slots(h, sub)):
                at = base + sub * GROUP + b * LANES
                panel[0:K, pl.ds(at, LANES)] = src[core_set, e, 0:K, :]
            tile = tails_of([src[core_set, e, K : K + 16, :] for core_set, e in slots(h, sub)])[0:2]
            at = base + sub * GROUP + 4 * LANES
            panel[0:K, pl.ds(at, LANES)] = jnp.concatenate(tile, axis=0).astype(BF16)

    def product(h, rows, chunks=range(ROWS_I // 256)):
        base = pl.multiple_of(h * 2 * GROUP, 2 * GROUP)
        for c in chunks:
            here = slice(c * 256, (c + 1) * 256)
            acc[0:rows, here] += jnp.dot(
                panel[0:rows, pl.ds(base, 2 * GROUP)],
                aff[pl.ds(base, 2 * GROUP), here],
                preferred_element_type=F32,
            )

    def first_step(h, carry):
        with jax.named_scope("a_wait"):

            @pl.when(h == 1)
            def _():
                points.forwarded(0)
                vectors.arrived(0)

            @pl.when(h == 2)
            def _():
                points.arrived(1)
                vectors.forwarded(0)

            @pl.when(h == 3)
            def _():
                points.forwarded(1)
                vectors.arrived(1)

        with jax.named_scope("a_work"):
            vector_tiles(h - 1, vbuf)
            product(h - 1, K + 16)
            affinity(h)
        return carry

    with jax.named_scope("a_first"):
        affinity(0)
    lax.fori_loop(1, 4, first_step, 0)
    def p_copy(it, d):
        return remote(psend.at[it, d], precv.at[it, d], p_s.at[it], p_r.at[it], z_peer(-d))

    def p_all(it):
        return remote(
            psend.at[it, pl.ds(1, NZ - 1)], precv.at[it, pl.ds(1, NZ - 1)], p_s.at[it], p_r.at[it], partner
        )

    blocks16 = lax.broadcasted_iota(jnp.int32, (16, LANES), 1) // TAIL
    rows16 = lax.broadcasted_iota(jnp.int32, (16, LANES), 0)

    def send_piece(it, d):
        b, at = d % 4, NZ * LANES + d // 4 * LANES
        here = slice(d * LANES, (d + 1) * LANES)
        last = jnp.zeros((16, LANES), F32)
        if it == 0:
            hi, mid, _ = bf16_pieces(acc[K : K + 8, here])
            hi_t, mid_t, _ = bf16_pieces(acc[K : K + 8, at : at + LANES])
            lines = [
                roll_lanes(hi_t, TAIL * (2 - b)), roll_lanes(mid_t, TAIL * (2 - b)),
                roll_lanes(hi, 64), hi, roll_lanes(mid, 64), mid,
            ]
            for r, line in enumerate(lines):
                last = jnp.where(rows16 == r, line[0:1], last)
        last = jnp.where(blocks16 == 0, roll_lanes(acc[0:16, at : at + LANES], -TAIL * b), last)
        last = jnp.where(blocks16 == 1, roll_lanes(acc[16:32, at : at + LANES], TAIL * (1 - b)), last)
        if d == 0:
            kept[0:K, :] = acc[0:K, here]
            kept[K : K + 16, :] = last
        else:
            psend[it, d, 0:K, :] = acc[0:K, here].astype(BF16)
            psend[it, d, K : K + 16, :] = last.astype(BF16)
            p_copy(it, d).start()

    def last_product(it, rows):
        for chunks, pieces in (((4, 2, 1), (4, 3, 5, 2)), ((3, 0), (6, 7, 1, 0))):
            product(3, rows, chunks)
            for d in pieces:
                send_piece(it, d)

    def received_product(it):
        p_all(it).wait_recv()
        total = kept[...]
        for d in range(1, NZ):
            total = total + precv[it, d].astype(F32)
        return total

    def degree_of(total):
        tail = roll_lanes(total[K : K + 1] + total[K + 1 : K + 2], 64)
        low = roll_lanes(total[K + 2 : K + 3] + total[K + 4 : K + 5], 64)
        high = total[K + 3 : K + 4] + total[K + 5 : K + 6]
        lane = lax.broadcasted_iota(jnp.int32, (1, LANES), 1)
        return jnp.where(lane < 64, low, high), jnp.where(lane < TAIL, tail, 1.0)

    def gram_of(scaled):
        wide = jnp.concatenate([scaled, jnp.zeros((LANES - K, 2 * LANES), F32)], axis=0)
        part = lax.dot_general(
            scaled, wide, (((1,), (1,)), ((), ())), precision=HIGHEST, preferred_element_type=F32
        )
        return packed_tail(part, 8)

    def g_copy(it, stage, n, to):
        return remote(gsend.at[it, stage], grecv.at[it, stage, n], g_s.at[it, stage], g_r.at[it, stage], to)

    def g_all(it, stage):
        piece = grecv.at[it, stage, pl.ds(1, 15)]
        return remote(piece, piece, g_s.at[it, stage], g_r.at[it, stage], partner)

    def g_total(it, stage):
        g_all(it, stage).wait_recv()
        terms = [gsend[it, stage]] + [grecv[it, stage, n] for n in range(1, 16)]
        while len(terms) > 1:
            terms = [a + b for a, b in zip(terms[::2], terms[1::2])]
        return terms[0]

    def gram_first(it, scaled):
        gsend[it, 0] = gram_of(scaled)
        for d in FAR_FIRST:
            g_copy(it, 0, d, col_peer(d)).start()

    def gram_second(it):
        gsend[it, 1] = g_total(it, 0)
        for e in range(NXY - 1, 0, -1):
            g_copy(it, 1, e, xy_peer(e)).start()

    def gram_last(it):
        return unpacked_tail(g_total(it, 1), 4) * (1.0 / TOTAL)

    with jax.named_scope("a_last_wait"):
        vectors.forwarded(1)
    with jax.named_scope("a_last"):
        vector_tiles(3, vbuf)
        last_product(0, K + 16)
    with jax.named_scope("reduce1"):
        total = received_product(0)
    with jax.named_scope("scale1"):
        deg_main, deg_tail = degree_of(total)
        scaled_main = total[0:K] / deg_main
        scaled_tail = unpacked_tail(total[K : K + 16], 2) / deg_tail
        scaled = jnp.concatenate([scaled_main, scaled_tail], axis=1)

        sbuf[0, 0, 0:K, :] = scaled[:, 0:LANES].astype(BF16)
        sbuf[0, 0, K : K + 16, :] = packed_tail(scaled[:, LANES:], 16).astype(BF16)
        scaleds.start(0)
        scaleds.start(1)
    with jax.named_scope("gram_first1"):
        gram_first(0, scaled)

    with jax.named_scope("b_left"):
        lo = (scaled - scaled.astype(BF16).astype(F32)).astype(BF16)
        acc[0:K, :] = jnp.dot(lo[:, 0:LANES], aff[0:LANES, :], preferred_element_type=F32) + jnp.dot(
            lo[:, LANES:], aff[4 * LANES : 5 * LANES, :], preferred_element_type=F32
        )
    def second_step(h):
        with jax.named_scope("b_work"):
            vector_tiles(h, sbuf)
            product(h, K)

    scaleds.arrived(0)
    second_step(0)
    scaleds.forwarded(0)
    second_step(1)
    scaleds.arrived(1)
    second_step(2)
    gram_second(0)
    scaleds.forwarded(1)
    with jax.named_scope("b_last"):
        vector_tiles(3, sbuf)
        last_product(1, K)

    eye = (
        lax.broadcasted_iota(jnp.int32, (K, LANES), 0)
        == lax.broadcasted_iota(jnp.int32, (K, LANES), 1)
    ).astype(F32)
    with jax.named_scope("gram_last1"):
        last = gram_last(0)
    with jax.named_scope("eliminate1"):
        inverse = eliminate(last, eye)
    with jax.named_scope("reduce2"):
        total = received_product(1)
    with jax.named_scope("scale2"):
        scaled = jnp.concatenate(
            [total[0:K] / deg_main, unpacked_tail(total[K : K + 16], 2) / deg_tail], axis=1
        )
        tall = jnp.concatenate([scaled, jnp.zeros((LANES - K, 2 * LANES), F32)], axis=0)
        scaled = jnp.dot(inverse, tall, precision=HIGHEST, preferred_element_type=F32)
    with jax.named_scope("gram_first2"):
        gram_first(1, scaled)
    with jax.named_scope("sent"):
        piece = zbuf.at[pl.ds(1, NZ - 1)]
        remote(piece, piece, z_s, z_r.at[0], partner).wait_send()
        points.left(1)
        vectors.left(1)
        for p in range(2):
            scaleds.left(p)
        for gathered in (points, vectors, scaleds):
            gathered.sent()
        for it in range(2):
            p_all(it).wait_send()
        for stage in range(2):
            g_all(0, stage).wait_send()
    with jax.named_scope("gram_second2"):
        gram_second(1)
    with jax.named_scope("gram_last2"):
        g_all(1, 0).wait_send()
        last = gram_last(1)
    with jax.named_scope("eliminate2"):
        ortho = eliminate(last, scaled)
        out_ref[...] = ortho[:, 0:OWN]

    with jax.named_scope("drain"):
        g_all(1, 1).wait_send()


def solution(mesh):
    dma = pltpu.SemaphoreType.DMA

    def shards(points, start_vectors):
        return pl.pallas_call(
            kernel,
            out_shape=jax.ShapeDtypeStruct((K, OWN), F32),
            in_specs=[pl.BlockSpec(memory_space=pltpu.HBM)] * 2,
            out_specs=pl.BlockSpec(memory_space=pltpu.VMEM),
            scratch_shapes=[
                pltpu.VMEM((F, OWN), BF16),
                pltpu.VMEM((K, OWN), BF16),
                pltpu.VMEM((F + K, 2 * LANES), F32),
                pltpu.VMEM((NZ, 80, LANES), BF16),
                pltpu.VMEM((2, NXY, 80, LANES), BF16),
                pltpu.VMEM((2, NXY, 48, LANES), BF16),
                pltpu.VMEM((LANES, ROWS_I), BF16),
                pltpu.VMEM((2 * GROUP, LANES), BF16),
                pltpu.VMEM((2 * K, COLS_J), BF16),
                pltpu.VMEM((COLS_J, ROWS_I), BF16),
                pltpu.VMEM((2 * K, ROWS_I), F32),
                pltpu.VMEM((K + 16, LANES), F32),
                pltpu.VMEM((2, NZ, K + 16, LANES), BF16),
                pltpu.VMEM((2, NZ, K + 16, LANES), BF16),
                pltpu.VMEM((2, NXY, K + 16, LANES), BF16),
                pltpu.VMEM((2, 2, 8, LANES), F32),
                pltpu.VMEM((2, 2, 16, 8, LANES), F32),
                dma((2,)),
                dma, dma((NZ,)),
                dma((2,)), dma((2,)), dma((2,)), dma((2,)),
                dma((2,)), dma((2,)), dma((2,)), dma((2,)),
                dma((2,)), dma((2,)),
                dma((2,)), dma((2,)), dma((2,)), dma((2,)),
                dma((2, 2)), dma((2, 2)),
            ],
            compiler_params=pltpu.CompilerParams(
                collective_id=0, has_side_effects=True, vmem_limit_bytes=48 * 1024 * 1024
            ),
        )(*(pltpu.with_memory_space_constraint(v.T, pltpu.HBM) for v in (points, start_vectors))).T

    spec = P(("row", "col"), None)
    return jax.shard_map(
        shards, mesh=mesh, in_specs=(spec, spec), out_specs=spec, check_vma=False
    )
```

```python
import functools
import math

import jax
import jax.numpy as jnp
from jax import lax
from jax.experimental import pallas as pl
from jax.experimental.pallas import tpu as pltpu
from jax.sharding import PartitionSpec as P

MESH = pl.DeviceIdType.MESH
F32 = jnp.float32
BF16 = jnp.bfloat16
HIGHEST = lax.Precision.HIGHEST

KERNEL_SCALE = 5.12
F = 64
K = 32
OWN = 160
LANES = 128
TAIL = OWN - LANES
GROUP = 4 * OWN
NZ = 8
NX = 4
NY = 4
NXY = NX * NY
NCOL = 2 * NZ
FAR_FIRST = (8, 7, 9, 6, 10, 5, 11, 4, 12, 3, 13, 2, 14, 1, 15)
ROWS_I = NZ * OWN
COLS_J = 2 * NXY * OWN
TOTAL = 256 * OWN


def roll_lanes(x, shift):
    shift = shift % LANES
    return x if shift == 0 else pltpu.roll(x, shift, 1)


def pick(blocks, pieces):
    out = pieces[3]
    for b in (2, 1, 0):
        out = jnp.where(blocks == b, pieces[b], out)
    return out


def transposed_blocks(tiles):
    rows = tiles[0].shape[0]
    blocks = lax.broadcasted_iota(jnp.int32, (rows, LANES), 1) // TAIL
    return [
        pick(blocks, [roll_lanes(tiles[b], TAIL * (b - g)) for b in range(4)]) for g in range(4)
    ]


def packed_tail(tail, rows):
    groups = tail.shape[0] // rows
    return sum(roll_lanes(tail[g * rows : (g + 1) * rows], TAIL * g) for g in range(groups))


def unpacked_tail(packed, groups):
    rows = packed.shape[0]
    keep = lax.broadcasted_iota(jnp.int32, (rows, LANES), 1) < TAIL
    return jnp.concatenate(
        [jnp.where(keep, roll_lanes(packed, -TAIL * g), 0.0) for g in range(groups)], axis=0
    )


def bf16_pieces(x):
    hi = x.astype(BF16).astype(F32)
    rest = x - hi
    mid = rest.astype(BF16).astype(F32)
    return hi, mid, rest - mid


def extended(x, for_rows):
    hi, mid, lo = bf16_pieces(jnp.sum(x * x, axis=0, keepdims=True))
    r = lax.broadcasted_iota(jnp.int32, (8, LANES), 0)
    if for_rows:
        x = 2.0 * x
        head = jnp.where(r == 3, -hi, jnp.where(r == 4, -mid, jnp.where(r == 5, -lo, 0.0)))
        extra = jnp.where(r < 3, -1.0, head)
    else:
        head = jnp.where(r == 0, hi, jnp.where(r == 1, mid, jnp.where(r == 2, lo, 0.0)))
        extra = jnp.where((r >= 3) & (r < 6), 1.0, head)
    return jnp.concatenate([x, extra, jnp.zeros((LANES - F - 8, LANES), F32)], axis=0)


def eliminate(gram, right):
    cols = [jnp.broadcast_to(gram[:, m : m + 1], (K, LANES)) for m in range(K)]
    width = right.shape[1] // LANES
    sub = lax.broadcasted_iota(jnp.int32, (8, LANES), 0)
    cols = [[c[8 * g : 8 * g + 8] for g in range(4)] for c in cols]
    rt = [
        [right[8 * g : 8 * g + 8, w * LANES : (w + 1) * LANES] for w in range(width)]
        for g in range(4)
    ]
    out_rows = []
    for k in range(K):
        kg, kr = k // 8, k % 8
        pivot = cols[k][kg][kr : kr + 1]
        inv = 1.0 / pivot
        factor = [None] * 4
        for g in range(kg, 4):
            f = cols[k][g] * inv
            if g == kg:
                f = jnp.where(sub > kr, f, 0.0)
            factor[g] = f
        for m in range(k + 1, K):
            mg, mr = m // 8, m % 8
            upper = cols[k][mg][mr : mr + 1]
            for g in range(mg, 4):
                cols[m][g] = cols[m][g] - factor[g] * upper
        rows = [rt[kg][w][kr : kr + 1] for w in range(width)]
        scale = lax.rsqrt(pivot)
        out_rows.append([row * scale for row in rows])
        for g in range(kg, 4):
            for w in range(width):
                rt[g][w] = rt[g][w] - factor[g] * rows[w]
    tiles = []
    for g in range(4):
        tile = []
        for w in range(width):
            acc = jnp.broadcast_to(out_rows[8 * g][w], (8, LANES))
            for r in range(1, 8):
                acc = jnp.where(sub == r, out_rows[8 * g + r][w], acc)
            tile.append(acc)
        tiles.append(jnp.concatenate(tile, axis=1) if width > 1 else tile[0])
    return jnp.concatenate(tiles, axis=0)


def kernel(
    pts_hbm, vec_hbm, out_ref,
    pts_ref, vec_ref, stage, zbuf, jbuf, vbuf, xi, xj, panel, aff, acc, kept, psend, precv, sbuf, gsend, grecv,
    in_s, z_s, z_r, xy_s, xy_r, f_s, f_r, v_s, v_r, vf_s, vf_r,
    p_s, p_r, s_s, s_r, sf_s, sf_r, g_s, g_r,
):
    row = lax.axis_index("row")
    col = lax.axis_index("col")
    x, y = row // NY, lax.rem(row, NY)
    z, core = col // 2, lax.rem(col, 2)

    def xy_peer(e):
        q = e // NY
        to_x = lax.rem(x + q + (q // 2) * (5 - 2 * q), NX)
        to_y = lax.rem(y + e % NY, NY)
        return (to_x * NY + to_y, col)

    def z_peer(d):
        return (row, lax.rem(z + d + NZ, NZ) * 2 + core)

    def col_peer(d):
        return (row, lax.rem(col + d, NCOL))

    partner = (row, z * 2 + 1 - core)

    def remote(src, dst, send, recv, to):
        return pltpu.make_async_remote_copy(
            src_ref=src, dst_ref=dst, send_sem=send, recv_sem=recv,
            device_id=to, device_id_type=MESH,
        )

    pts_copy = pltpu.make_async_copy(pts_hbm, pts_ref, in_s.at[0])
    vec_copy = pltpu.make_async_copy(vec_hbm, vec_ref, in_s.at[1])
    pts_copy.start()
    vec_copy.start()
    barrier = pltpu.get_barrier_semaphore()
    with jax.named_scope("signal"):
        for d in FAR_FIRST:
            pl.semaphore_signal(barrier, inc=1, device_id=col_peer(d), device_id_type=MESH)
        for e in range(NXY - 1, 0, -1):
            pl.semaphore_signal(barrier, inc=1, device_id=xy_peer(e), device_id_type=MESH)

    with jax.named_scope("prepare"):
        stage[...] = jnp.zeros_like(stage)
        pts_copy.wait()
        vec_copy.wait()
        stage[0:F, 0:OWN] = pts_ref[...].astype(F32)
        stage[F : F + K, 0:OWN] = vec_ref[...].astype(F32)
        t = stage[...]
        jbuf[0, 0, 0:64, :] = t[0:F, 0:LANES].astype(BF16)
        jbuf[0, 0, 64:80, :] = packed_tail(t[0:F, LANES:], 16).astype(BF16)
        vbuf[0, 0, 0:32, :] = t[F : F + K, 0:LANES].astype(BF16)
        vbuf[0, 0, 32:48, :] = packed_tail(t[F : F + K, LANES:], 16).astype(BF16)
        acc[...] = jnp.zeros_like(acc)
        for h in range(COLS_J // GROUP):
            panel[K : K + 16, h * GROUP : (h + 1) * GROUP] = (
                lax.broadcasted_iota(jnp.int32, (16, GROUP), 0) == 0
            ).astype(F32).astype(BF16)

    with jax.named_scope("barrier_wait"):
        pl.semaphore_wait(barrier, NCOL - 1 + NXY - 1)

    def z_copy(d):
        return remote(jbuf.at[0, 0], zbuf.at[d], z_s, z_r.at[d], z_peer(d))

    class Gathered:
        def __init__(self, buf, send, recv, on_send, on_recv):
            self.buf, self.send, self.recv, self.on_send, self.on_recv = buf, send, recv, on_send, on_recv

        def start(self, p):
            for e in range(max(1, 8 * p), 8 * p + 8):
                remote(
                    self.buf.at[0, 0], self.buf.at[0, e], self.send.at[p], self.recv.at[p], xy_peer(e)
                ).start()

        def piece(self, p):
            first = max(1, 8 * p)
            piece = self.buf.at[0, pl.ds(first, 8 * p + 8 - first)]
            return remote(piece, piece, self.send.at[p], self.recv.at[p], partner)

        def group(self, p):
            pieces = [self.buf.at[half, pl.ds(p * 8, 8)] for half in range(2)]
            return remote(*pieces, self.on_send.at[p], self.on_recv.at[p], partner)

        def arrived(self, p):
            self.piece(p).wait_recv()
            self.group(p).start()

        def forwarded(self, p):
            self.group(p).wait_recv()

        def left(self, p):
            self.piece(p).wait_send()

        def sent(self):
            for p in range(2):
                self.group(p).wait_send()

    points = Gathered(jbuf, xy_s, xy_r, f_s, f_r)
    vectors = Gathered(vbuf, v_s, v_r, vf_s, vf_r)
    scaleds = Gathered(sbuf, s_s, s_r, sf_s, sf_r)

    with jax.named_scope("send_points"):
        for d in (4, 3, 5, 2, 6, 1, 7):
            z_copy(d).start()
        points.start(0)
    with jax.named_scope("left_points"):
        points.left(0)
        vectors.start(0)
        points.start(1)
        vectors.left(0)
        vectors.start(1)

    def tails_of(tiles):
        return transposed_blocks([tile.astype(F32) for tile in tiles])

    with jax.named_scope("first_points"):
        points.arrived(0)

    with jax.named_scope("row_side"):
        for d in (0, 1, 7, 2, 6, 3, 5, 4):
            if d == 0:
                src = jbuf[0, 0, 0:64, :]
            else:
                z_copy(d).wait_recv()
                src = zbuf[d, 0:64, :]
            xi[:, d * LANES : (d + 1) * LANES] = extended(src.astype(F32), True).astype(BF16)
        for q in range(NZ // 4):
            tiles = [
                jbuf[0, 0, 64:80, :] if 4 * q + b == 0 else zbuf[4 * q + b, 64:80, :]
                for b in range(4)
            ]
            tile = jnp.concatenate(tails_of(tiles), axis=0)
            at = NZ * LANES + q * LANES
            xi[:, at : at + LANES] = extended(tile, True).astype(BF16)

    def slots(h, sub):
        return [(h % 2, h // 2 * 8 + sub * 4 + b) for b in range(4)]

    def affinity(h):
        base = pl.multiple_of(h * 2 * GROUP, 2 * GROUP)
        for sub in range(2):
            for b, (core_set, e) in enumerate(slots(h, sub)):
                at = sub * GROUP + b * LANES
                src = jbuf[core_set, e, 0:64, :].astype(F32)
                xj[at : at + LANES, :] = extended(src, False).astype(BF16).T
            at = sub * GROUP + 4 * LANES
            tile = tails_of([jbuf[core_set, e, 64:80, :] for core_set, e in slots(h, sub)])
            xj[at : at + LANES, :] = extended(jnp.concatenate(tile, axis=0), False).astype(BF16).T
        for c in range(ROWS_I // 256):
            here = slice(c * 256, (c + 1) * 256)
            dist = jnp.dot(xj[...], xi[:, here], preferred_element_type=F32)
            weights = jnp.exp2(dist * (KERNEL_SCALE / F * math.log2(math.e)))
            aff[pl.ds(base, 2 * GROUP), here] = weights.astype(BF16)

    def vector_tiles(h, src):
        base = pl.multiple_of(h * 2 * GROUP, 2 * GROUP)
        for sub in range(2):
            for b, (core_set, e) in enumerate(slots(h, sub)):
                at = base + sub * GROUP + b * LANES
                panel[0:K, pl.ds(at, LANES)] = src[core_set, e, 0:K, :]
            tile = tails_of([src[core_set, e, K : K + 16, :] for core_set, e in slots(h, sub)])[0:2]
            at = base + sub * GROUP + 4 * LANES
            panel[0:K, pl.ds(at, LANES)] = jnp.concatenate(tile, axis=0).astype(BF16)

    def product(h, rows, chunks=range(ROWS_I // 256)):
        base = pl.multiple_of(h * 2 * GROUP, 2 * GROUP)
        for c in chunks:
            here = slice(c * 256, (c + 1) * 256)
            acc[0:rows, here] += jnp.dot(
                panel[0:rows, pl.ds(base, 2 * GROUP)],
                aff[pl.ds(base, 2 * GROUP), here],
                preferred_element_type=F32,
            )

    def first_step(h, carry):
        with jax.named_scope("a_wait"):

            @pl.when(h == 1)
            def _():
                points.forwarded(0)
                vectors.arrived(0)

            @pl.when(h == 2)
            def _():
                points.arrived(1)
                vectors.forwarded(0)

            @pl.when(h == 3)
            def _():
                points.forwarded(1)
                vectors.arrived(1)

        with jax.named_scope("a_work"):
            vector_tiles(h - 1, vbuf)
            product(h - 1, K + 16)
            affinity(h)
        return carry

    with jax.named_scope("a_first"):
        affinity(0)
    lax.fori_loop(1, 4, first_step, 0)
    def p_copy(it, d):
        return remote(psend.at[it, d], precv.at[it, d], p_s.at[it], p_r.at[it], z_peer(-d))

    def p_all(it):
        return remote(
            psend.at[it, pl.ds(1, NZ - 1)], precv.at[it, pl.ds(1, NZ - 1)], p_s.at[it], p_r.at[it], partner
        )

    blocks16 = lax.broadcasted_iota(jnp.int32, (16, LANES), 1) // TAIL
    rows16 = lax.broadcasted_iota(jnp.int32, (16, LANES), 0)

    def send_piece(it, d):
        b, at = d % 4, NZ * LANES + d // 4 * LANES
        here = slice(d * LANES, (d + 1) * LANES)
        last = jnp.zeros((16, LANES), F32)
        if it == 0:
            hi, mid, _ = bf16_pieces(acc[K : K + 8, here])
            hi_t, mid_t, _ = bf16_pieces(acc[K : K + 8, at : at + LANES])
            lines = [
                roll_lanes(hi_t, TAIL * (2 - b)), roll_lanes(mid_t, TAIL * (2 - b)),
                roll_lanes(hi, 64), hi, roll_lanes(mid, 64), mid,
            ]
            for r, line in enumerate(lines):
                last = jnp.where(rows16 == r, line[0:1], last)
        last = jnp.where(blocks16 == 0, roll_lanes(acc[0:16, at : at + LANES], -TAIL * b), last)
        last = jnp.where(blocks16 == 1, roll_lanes(acc[16:32, at : at + LANES], TAIL * (1 - b)), last)
        if d == 0:
            kept[0:K, :] = acc[0:K, here]
            kept[K : K + 16, :] = last
        else:
            psend[it, d, 0:K, :] = acc[0:K, here].astype(BF16)
            psend[it, d, K : K + 16, :] = last.astype(BF16)
            p_copy(it, d).start()

    def last_product(it, rows):
        for chunks, pieces in (((4, 2, 1), (4, 3, 5, 2)), ((3, 0), (6, 7, 1, 0))):
            product(3, rows, chunks)
            for d in pieces:
                send_piece(it, d)

    def received_product(it):
        p_all(it).wait_recv()
        total = kept[...]
        for d in range(1, NZ):
            total = total + precv[it, d].astype(F32)
        return total

    def degree_of(total):
        tail = roll_lanes(total[K : K + 1] + total[K + 1 : K + 2], 64)
        low = roll_lanes(total[K + 2 : K + 3] + total[K + 4 : K + 5], 64)
        high = total[K + 3 : K + 4] + total[K + 5 : K + 6]
        lane = lax.broadcasted_iota(jnp.int32, (1, LANES), 1)
        return jnp.where(lane < 64, low, high), jnp.where(lane < TAIL, tail, 1.0)

    def gram_of(scaled):
        wide = jnp.concatenate([scaled, jnp.zeros((LANES - K, 2 * LANES), F32)], axis=0)
        part = lax.dot_general(
            scaled, wide, (((1,), (1,)), ((), ())), precision=HIGHEST, preferred_element_type=F32
        )
        return packed_tail(part, 8)

    def g_copy(it, stage, n, to):
        return remote(gsend.at[it, stage], grecv.at[it, stage, n], g_s.at[it, stage], g_r.at[it, stage], to)

    def g_all(it, stage):
        piece = grecv.at[it, stage, pl.ds(1, 15)]
        return remote(piece, piece, g_s.at[it, stage], g_r.at[it, stage], partner)

    def g_total(it, stage):
        g_all(it, stage).wait_recv()
        terms = [gsend[it, stage]] + [grecv[it, stage, n] for n in range(1, 16)]
        while len(terms) > 1:
            terms = [a + b for a, b in zip(terms[::2], terms[1::2])]
        return terms[0]

    def gram_first(it, scaled):
        gsend[it, 0] = gram_of(scaled)
        for d in FAR_FIRST:
            g_copy(it, 0, d, col_peer(d)).start()

    def gram_second(it):
        gsend[it, 1] = g_total(it, 0)
        for e in range(NXY - 1, 0, -1):
            g_copy(it, 1, e, xy_peer(e)).start()

    def gram_last(it):
        return unpacked_tail(g_total(it, 1), 4) * (1.0 / TOTAL)

    with jax.named_scope("a_last_wait"):
        vectors.forwarded(1)
    with jax.named_scope("a_last"):
        vector_tiles(3, vbuf)
        last_product(0, K + 16)
    with jax.named_scope("reduce1"):
        total = received_product(0)
    with jax.named_scope("scale1"):
        deg_main, deg_tail = degree_of(total)
        scaled_main = total[0:K] / deg_main
        scaled_tail = unpacked_tail(total[K : K + 16], 2) / deg_tail
        scaled = jnp.concatenate([scaled_main, scaled_tail], axis=1)

        sbuf[0, 0, 0:K, :] = scaled[:, 0:LANES].astype(BF16)
        sbuf[0, 0, K : K + 16, :] = packed_tail(scaled[:, LANES:], 16).astype(BF16)
        scaleds.start(0)
    with jax.named_scope("gram_first1"):
        gram_first(0, scaled)

    scaleds.start(1)
    with jax.named_scope("b_left"):
        lo = (scaled - scaled.astype(BF16).astype(F32)).astype(BF16)
        acc[0:K, :] = jnp.dot(lo[:, 0:LANES], aff[0:LANES, :], preferred_element_type=F32) + jnp.dot(
            lo[:, LANES:], aff[4 * LANES : 5 * LANES, :], preferred_element_type=F32
        )
    def second_step(h):
        with jax.named_scope("b_work"):
            vector_tiles(h, sbuf)
            product(h, K)

    scaleds.arrived(0)
    second_step(0)
    scaleds.forwarded(0)
    second_step(1)
    scaleds.arrived(1)
    second_step(2)
    gram_second(0)
    scaleds.forwarded(1)
    with jax.named_scope("b_last"):
        vector_tiles(3, sbuf)
        last_product(1, K)

    eye = (
        lax.broadcasted_iota(jnp.int32, (K, LANES), 0)
        == lax.broadcasted_iota(jnp.int32, (K, LANES), 1)
    ).astype(F32)
    with jax.named_scope("gram_last1"):
        last = gram_last(0)
    with jax.named_scope("eliminate1"):
        inverse = eliminate(last, eye)
    with jax.named_scope("reduce2"):
        total = received_product(1)
    with jax.named_scope("scale2"):
        scaled = jnp.concatenate(
            [total[0:K] / deg_main, unpacked_tail(total[K : K + 16], 2) / deg_tail], axis=1
        )
        tall = jnp.concatenate([scaled, jnp.zeros((LANES - K, 2 * LANES), F32)], axis=0)
        scaled = jnp.dot(inverse, tall, precision=HIGHEST, preferred_element_type=F32)
    with jax.named_scope("gram_first2"):
        gram_first(1, scaled)
    with jax.named_scope("sent"):
        piece = zbuf.at[pl.ds(1, NZ - 1)]
        remote(piece, piece, z_s, z_r.at[0], partner).wait_send()
        points.left(1)
        vectors.left(1)
        for p in range(2):
            scaleds.left(p)
        for gathered in (points, vectors, scaleds):
            gathered.sent()
        for it in range(2):
            p_all(it).wait_send()
        for stage in range(2):
            g_all(0, stage).wait_send()
    with jax.named_scope("gram_second2"):
        gram_second(1)
    with jax.named_scope("gram_last2"):
        g_all(1, 0).wait_send()
        last = gram_last(1)
    with jax.named_scope("eliminate2"):
        ortho = eliminate(last, scaled)
        out_ref[...] = ortho[:, 0:OWN]

    with jax.named_scope("drain"):
        g_all(1, 1).wait_send()


def solution(mesh):
    dma = pltpu.SemaphoreType.DMA

    def shards(points, start_vectors):
        return pl.pallas_call(
            kernel,
            out_shape=jax.ShapeDtypeStruct((K, OWN), F32),
            in_specs=[pl.BlockSpec(memory_space=pltpu.HBM)] * 2,
            out_specs=pl.BlockSpec(memory_space=pltpu.VMEM),
            scratch_shapes=[
                pltpu.VMEM((F, OWN), BF16),
                pltpu.VMEM((K, OWN), BF16),
                pltpu.VMEM((F + K, 2 * LANES), F32),
                pltpu.VMEM((NZ, 80, LANES), BF16),
                pltpu.VMEM((2, NXY, 80, LANES), BF16),
                pltpu.VMEM((2, NXY, 48, LANES), BF16),
                pltpu.VMEM((LANES, ROWS_I), BF16),
                pltpu.VMEM((2 * GROUP, LANES), BF16),
                pltpu.VMEM((2 * K, COLS_J), BF16),
                pltpu.VMEM((COLS_J, ROWS_I), BF16),
                pltpu.VMEM((2 * K, ROWS_I), F32),
                pltpu.VMEM((K + 16, LANES), F32),
                pltpu.VMEM((2, NZ, K + 16, LANES), BF16),
                pltpu.VMEM((2, NZ, K + 16, LANES), BF16),
                pltpu.VMEM((2, NXY, K + 16, LANES), BF16),
                pltpu.VMEM((2, 2, 8, LANES), F32),
                pltpu.VMEM((2, 2, 16, 8, LANES), F32),
                dma((2,)),
                dma, dma((NZ,)),
                dma((2,)), dma((2,)), dma((2,)), dma((2,)),
                dma((2,)), dma((2,)), dma((2,)), dma((2,)),
                dma((2,)), dma((2,)),
                dma((2,)), dma((2,)), dma((2,)), dma((2,)),
                dma((2, 2)), dma((2, 2)),
            ],
            compiler_params=pltpu.CompilerParams(
                collective_id=0, has_side_effects=True, vmem_limit_bytes=48 * 1024 * 1024
            ),
        )(*(pltpu.with_memory_space_constraint(v.T, pltpu.HBM) for v in (points, start_vectors))).T

    spec = P(("row", "col"), None)
    return jax.shard_map(
        shards, mesh=mesh, in_specs=(spec, spec), out_specs=spec, check_vma=False
    )
```

```python
import functools
import math

import jax
import jax.numpy as jnp
from jax import lax
from jax.experimental import pallas as pl
from jax.experimental.pallas import tpu as pltpu
from jax.sharding import PartitionSpec as P

MESH = pl.DeviceIdType.MESH
F32 = jnp.float32
BF16 = jnp.bfloat16
HIGHEST = lax.Precision.HIGHEST

KERNEL_SCALE = 5.12
F = 64
K = 32
OWN = 160
LANES = 128
TAIL = OWN - LANES
GROUP = 4 * OWN
NZ = 8
NX = 4
NY = 4
NXY = NX * NY
NCOL = 2 * NZ
FAR_FIRST = (8, 7, 9, 6, 10, 5, 11, 4, 12, 3, 13, 2, 14, 1, 15)
ROWS_I = NZ * OWN
COLS_J = 2 * NXY * OWN
TOTAL = 256 * OWN


def roll_lanes(x, shift):
    shift = shift % LANES
    return x if shift == 0 else pltpu.roll(x, shift, 1)


def pick(blocks, pieces):
    out = pieces[3]
    for b in (2, 1, 0):
        out = jnp.where(blocks == b, pieces[b], out)
    return out


def transposed_blocks(tiles):
    rows = tiles[0].shape[0]
    blocks = lax.broadcasted_iota(jnp.int32, (rows, LANES), 1) // TAIL
    return [
        pick(blocks, [roll_lanes(tiles[b], TAIL * (b - g)) for b in range(4)]) for g in range(4)
    ]


def packed_tail(tail, rows):
    groups = tail.shape[0] // rows
    return sum(roll_lanes(tail[g * rows : (g + 1) * rows], TAIL * g) for g in range(groups))


def unpacked_tail(packed, groups):
    rows = packed.shape[0]
    keep = lax.broadcasted_iota(jnp.int32, (rows, LANES), 1) < TAIL
    return jnp.concatenate(
        [jnp.where(keep, roll_lanes(packed, -TAIL * g), 0.0) for g in range(groups)], axis=0
    )


def bf16_pieces(x):
    hi = x.astype(BF16).astype(F32)
    rest = x - hi
    mid = rest.astype(BF16).astype(F32)
    return hi, mid, rest - mid


def extended(x, for_rows):
    hi, mid, lo = bf16_pieces(jnp.sum(x * x, axis=0, keepdims=True))
    r = lax.broadcasted_iota(jnp.int32, (8, LANES), 0)
    if for_rows:
        x = 2.0 * x
        head = jnp.where(r == 3, -hi, jnp.where(r == 4, -mid, jnp.where(r == 5, -lo, 0.0)))
        extra = jnp.where(r < 3, -1.0, head)
    else:
        head = jnp.where(r == 0, hi, jnp.where(r == 1, mid, jnp.where(r == 2, lo, 0.0)))
        extra = jnp.where((r >= 3) & (r < 6), 1.0, head)
    return jnp.concatenate([x, extra, jnp.zeros((LANES - F - 8, LANES), F32)], axis=0)


def eliminate(gram, right):
    cols = [jnp.broadcast_to(gram[:, m : m + 1], (K, LANES)) for m in range(K)]
    width = right.shape[1] // LANES
    sub = lax.broadcasted_iota(jnp.int32, (8, LANES), 0)
    cols = [[c[8 * g : 8 * g + 8] for g in range(4)] for c in cols]
    rt = [
        [right[8 * g : 8 * g + 8, w * LANES : (w + 1) * LANES] for w in range(width)]
        for g in range(4)
    ]
    out_rows = []
    for k in range(K):
        kg, kr = k // 8, k % 8
        pivot = cols[k][kg][kr : kr + 1]
        inv = 1.0 / pivot
        factor = [None] * 4
        for g in range(kg, 4):
            f = cols[k][g] * inv
            if g == kg:
                f = jnp.where(sub > kr, f, 0.0)
            factor[g] = f
        for m in range(k + 1, K):
            mg, mr = m // 8, m % 8
            upper = cols[k][mg][mr : mr + 1]
            for g in range(mg, 4):
                cols[m][g] = cols[m][g] - factor[g] * upper
        rows = [rt[kg][w][kr : kr + 1] for w in range(width)]
        scale = lax.rsqrt(pivot)
        out_rows.append([row * scale for row in rows])
        for g in range(kg, 4):
            for w in range(width):
                rt[g][w] = rt[g][w] - factor[g] * rows[w]
    tiles = []
    for g in range(4):
        tile = []
        for w in range(width):
            acc = jnp.broadcast_to(out_rows[8 * g][w], (8, LANES))
            for r in range(1, 8):
                acc = jnp.where(sub == r, out_rows[8 * g + r][w], acc)
            tile.append(acc)
        tiles.append(jnp.concatenate(tile, axis=1) if width > 1 else tile[0])
    return jnp.concatenate(tiles, axis=0)


def kernel(
    pts_hbm, vec_hbm, out_ref,
    pts_ref, vec_ref, stage, zbuf, jbuf, vbuf, xi, xj, panel, aff, acc, kept, psend, precv, sbuf, gsend, grecv,
    in_s, z_s, z_r, xy_s, xy_r, f_s, f_r, v_s, v_r, vf_s, vf_r,
    p_s, p_r, s_s, s_r, sf_s, sf_r, g_s, g_r,
):
    row = lax.axis_index("row")
    col = lax.axis_index("col")
    x, y = row // NY, lax.rem(row, NY)
    z, core = col // 2, lax.rem(col, 2)

    def xy_peer(e):
        q = e // NY
        to_x = lax.rem(x + q + (q // 2) * (5 - 2 * q), NX)
        to_y = lax.rem(y + e % NY, NY)
        return (to_x * NY + to_y, col)

    def z_peer(d):
        return (row, lax.rem(z + d + NZ, NZ) * 2 + core)

    def col_peer(d):
        return (row, lax.rem(col + d, NCOL))

    partner = (row, z * 2 + 1 - core)

    def remote(src, dst, send, recv, to):
        return pltpu.make_async_remote_copy(
            src_ref=src, dst_ref=dst, send_sem=send, recv_sem=recv,
            device_id=to, device_id_type=MESH,
        )

    pts_copy = pltpu.make_async_copy(pts_hbm, pts_ref, in_s.at[0])
    vec_copy = pltpu.make_async_copy(vec_hbm, vec_ref, in_s.at[1])
    pts_copy.start()
    vec_copy.start()
    barrier = pltpu.get_barrier_semaphore()
    with jax.named_scope("signal"):
        for d in FAR_FIRST:
            pl.semaphore_signal(barrier, inc=1, device_id=col_peer(d), device_id_type=MESH)
        for e in range(NXY - 1, 0, -1):
            pl.semaphore_signal(barrier, inc=1, device_id=xy_peer(e), device_id_type=MESH)

    with jax.named_scope("prepare"):
        stage[...] = jnp.zeros_like(stage)
        pts_copy.wait()
        vec_copy.wait()
        stage[0:F, 0:OWN] = pts_ref[...].astype(F32)
        stage[F : F + K, 0:OWN] = vec_ref[...].astype(F32)
        t = stage[...]
        jbuf[0, 0, 0:64, :] = t[0:F, 0:LANES].astype(BF16)
        jbuf[0, 0, 64:80, :] = packed_tail(t[0:F, LANES:], 16).astype(BF16)
        vbuf[0, 0, 0:32, :] = t[F : F + K, 0:LANES].astype(BF16)
        vbuf[0, 0, K : K + 8, :] = packed_tail(t[F : F + K, LANES:], 8).astype(BF16)
        acc[...] = jnp.zeros_like(acc)
        for h in range(COLS_J // GROUP):
            panel[K : K + 16, h * GROUP : (h + 1) * GROUP] = (
                lax.broadcasted_iota(jnp.int32, (16, GROUP), 0) == 0
            ).astype(F32).astype(BF16)

    with jax.named_scope("barrier_wait"):
        pl.semaphore_wait(barrier, NCOL - 1 + NXY - 1)

    def z_copy(d):
        return remote(jbuf.at[0, 0], zbuf.at[d], z_s, z_r.at[d], z_peer(d))

    class Gathered:
        def __init__(self, buf, send, recv, on_send, on_recv):
            self.buf, self.send, self.recv, self.on_send, self.on_recv = buf, send, recv, on_send, on_recv

        def start(self, p):
            for e in range(max(1, 8 * p), 8 * p + 8):
                remote(
                    self.buf.at[0, 0], self.buf.at[0, e], self.send.at[p], self.recv.at[p], xy_peer(e)
                ).start()

        def piece(self, p):
            first = max(1, 8 * p)
            piece = self.buf.at[0, pl.ds(first, 8 * p + 8 - first)]
            return remote(piece, piece, self.send.at[p], self.recv.at[p], partner)

        def group(self, p):
            pieces = [self.buf.at[half, pl.ds(p * 8, 8)] for half in range(2)]
            return remote(*pieces, self.on_send.at[p], self.on_recv.at[p], partner)

        def arrived(self, p):
            self.piece(p).wait_recv()
            self.group(p).start()

        def forwarded(self, p):
            self.group(p).wait_recv()

        def left(self, p):
            self.piece(p).wait_send()

        def sent(self):
            for p in range(2):
                self.group(p).wait_send()

    points = Gathered(jbuf, xy_s, xy_r, f_s, f_r)
    vectors = Gathered(vbuf, v_s, v_r, vf_s, vf_r)
    scaleds = Gathered(sbuf, s_s, s_r, sf_s, sf_r)

    with jax.named_scope("send_points"):
        for d in (4, 3, 5, 2, 6, 1, 7):
            z_copy(d).start()
        points.start(0)
    with jax.named_scope("left_points"):
        points.left(0)
        vectors.start(0)
        points.start(1)
        vectors.left(0)
        vectors.start(1)

    def tails_of(tiles):
        return transposed_blocks([tile.astype(F32) for tile in tiles])

    with jax.named_scope("first_points"):
        points.arrived(0)

    with jax.named_scope("row_side"):
        for d in (0, 1, 7, 2, 6, 3, 5, 4):
            if d == 0:
                src = jbuf[0, 0, 0:64, :]
            else:
                z_copy(d).wait_recv()
                src = zbuf[d, 0:64, :]
            xi[:, d * LANES : (d + 1) * LANES] = extended(src.astype(F32), True).astype(BF16)
        for q in range(NZ // 4):
            tiles = [
                jbuf[0, 0, 64:80, :] if 4 * q + b == 0 else zbuf[4 * q + b, 64:80, :]
                for b in range(4)
            ]
            tile = jnp.concatenate(tails_of(tiles), axis=0)
            at = NZ * LANES + q * LANES
            xi[:, at : at + LANES] = extended(tile, True).astype(BF16)

    def slots(h, sub):
        return [(h % 2, h // 2 * 8 + sub * 4 + b) for b in range(4)]

    def affinity(h):
        base = pl.multiple_of(h * 2 * GROUP, 2 * GROUP)
        for sub in range(2):
            for b, (core_set, e) in enumerate(slots(h, sub)):
                at = sub * GROUP + b * LANES
                src = jbuf[core_set, e, 0:64, :].astype(F32)
                xj[at : at + LANES, :] = extended(src, False).astype(BF16).T
            at = sub * GROUP + 4 * LANES
            tile = tails_of([jbuf[core_set, e, 64:80, :] for core_set, e in slots(h, sub)])
            xj[at : at + LANES, :] = extended(jnp.concatenate(tile, axis=0), False).astype(BF16).T
        for c in range(ROWS_I // 256):
            here = slice(c * 256, (c + 1) * 256)
            dist = jnp.dot(xj[...], xi[:, here], preferred_element_type=F32)
            weights = jnp.exp2(dist * (KERNEL_SCALE / F * math.log2(math.e)))
            aff[pl.ds(base, 2 * GROUP), here] = weights.astype(BF16)

    def vector_tiles(h, src):
        base = pl.multiple_of(h * 2 * GROUP, 2 * GROUP)
        for sub in range(2):
            for b, (core_set, e) in enumerate(slots(h, sub)):
                at = base + sub * GROUP + b * LANES
                panel[0:K, pl.ds(at, LANES)] = src[core_set, e, 0:K, :]
            tile = tails_of([src[core_set, e, K : K + 8, :] for core_set, e in slots(h, sub)])
            at = base + sub * GROUP + 4 * LANES
            panel[0:K, pl.ds(at, LANES)] = jnp.concatenate(tile, axis=0).astype(BF16)

    def product(h, rows, chunks=range(ROWS_I // 256)):
        base = pl.multiple_of(h * 2 * GROUP, 2 * GROUP)
        for c in chunks:
            here = slice(c * 256, (c + 1) * 256)
            acc[0:rows, here] += jnp.dot(
                panel[0:rows, pl.ds(base, 2 * GROUP)],
                aff[pl.ds(base, 2 * GROUP), here],
                preferred_element_type=F32,
            )

    def first_step(h, carry):
        with jax.named_scope("a_wait"):

            @pl.when(h == 1)
            def _():
                points.forwarded(0)
                vectors.arrived(0)

            @pl.when(h == 2)
            def _():
                points.arrived(1)
                vectors.forwarded(0)

            @pl.when(h == 3)
            def _():
                points.forwarded(1)
                vectors.arrived(1)

        with jax.named_scope("a_work"):
            vector_tiles(h - 1, vbuf)
            product(h - 1, K + 16)
            affinity(h)
        return carry

    with jax.named_scope("a_first"):
        affinity(0)
    lax.fori_loop(1, 4, first_step, 0)
    def p_copy(it, d):
        return remote(psend.at[it, d], precv.at[it, d], p_s.at[it], p_r.at[it], z_peer(-d))

    def p_all(it):
        return remote(
            psend.at[it, pl.ds(1, NZ - 1)], precv.at[it, pl.ds(1, NZ - 1)], p_s.at[it], p_r.at[it], partner
        )

    blocks16 = lax.broadcasted_iota(jnp.int32, (16, LANES), 1) // TAIL
    rows16 = lax.broadcasted_iota(jnp.int32, (16, LANES), 0)

    def send_piece(it, d):
        b, at = d % 4, NZ * LANES + d // 4 * LANES
        here = slice(d * LANES, (d + 1) * LANES)
        last = jnp.zeros((16, LANES), F32)
        if it == 0:
            hi, mid, _ = bf16_pieces(acc[K : K + 8, here])
            hi_t, mid_t, _ = bf16_pieces(acc[K : K + 8, at : at + LANES])
            lines = [
                roll_lanes(hi_t, TAIL * (2 - b)), roll_lanes(mid_t, TAIL * (2 - b)),
                roll_lanes(hi, 64), hi, roll_lanes(mid, 64), mid,
            ]
            for r, line in enumerate(lines):
                last = jnp.where(rows16 == r, line[0:1], last)
        last = jnp.where(blocks16 == 0, roll_lanes(acc[0:16, at : at + LANES], -TAIL * b), last)
        last = jnp.where(blocks16 == 1, roll_lanes(acc[16:32, at : at + LANES], TAIL * (1 - b)), last)
        if d == 0:
            kept[0:K, :] = acc[0:K, here]
            kept[K : K + 16, :] = last
        else:
            psend[it, d, 0:K, :] = acc[0:K, here].astype(BF16)
            psend[it, d, K : K + 16, :] = last.astype(BF16)
            p_copy(it, d).start()

    def last_product(it, rows):
        for chunks, pieces in (((4, 2, 1), (4, 3, 5, 2)), ((3, 0), (6, 7, 1, 0))):
            product(3, rows, chunks)
            for d in pieces:
                send_piece(it, d)

    def received_product(it):
        p_all(it).wait_recv()
        total = kept[...]
        for d in range(1, NZ):
            total = total + precv[it, d].astype(F32)
        return total

    def degree_of(total):
        tail = roll_lanes(total[K : K + 1] + total[K + 1 : K + 2], 64)
        low = roll_lanes(total[K + 2 : K + 3] + total[K + 4 : K + 5], 64)
        high = total[K + 3 : K + 4] + total[K + 5 : K + 6]
        lane = lax.broadcasted_iota(jnp.int32, (1, LANES), 1)
        return jnp.where(lane < 64, low, high), jnp.where(lane < TAIL, tail, 1.0)

    def gram_of(scaled):
        wide = jnp.concatenate([scaled, jnp.zeros((LANES - K, 2 * LANES), F32)], axis=0)
        part = lax.dot_general(
            scaled, wide, (((1,), (1,)), ((), ())), precision=HIGHEST, preferred_element_type=F32
        )
        return packed_tail(part, 8)

    def g_copy(it, stage, n, to):
        return remote(gsend.at[it, stage], grecv.at[it, stage, n], g_s.at[it, stage], g_r.at[it, stage], to)

    def g_all(it, stage):
        piece = grecv.at[it, stage, pl.ds(1, 15)]
        return remote(piece, piece, g_s.at[it, stage], g_r.at[it, stage], partner)

    def g_total(it, stage):
        g_all(it, stage).wait_recv()
        terms = [gsend[it, stage]] + [grecv[it, stage, n] for n in range(1, 16)]
        while len(terms) > 1:
            terms = [a + b for a, b in zip(terms[::2], terms[1::2])]
        return terms[0]

    def gram_first(it, scaled):
        gsend[it, 0] = gram_of(scaled)
        for d in FAR_FIRST:
            g_copy(it, 0, d, col_peer(d)).start()

    def gram_second(it):
        gsend[it, 1] = g_total(it, 0)
        for e in range(NXY - 1, 0, -1):
            g_copy(it, 1, e, xy_peer(e)).start()

    def gram_last(it):
        return unpacked_tail(g_total(it, 1), 4) * (1.0 / TOTAL)

    with jax.named_scope("a_last_wait"):
        vectors.forwarded(1)
    with jax.named_scope("a_last"):
        vector_tiles(3, vbuf)
        last_product(0, K + 16)
    with jax.named_scope("reduce1"):
        total = received_product(0)
    with jax.named_scope("scale1"):
        deg_main, deg_tail = degree_of(total)
        scaled_main = total[0:K] / deg_main
        scaled_tail = unpacked_tail(total[K : K + 16], 2) / deg_tail
        scaled = jnp.concatenate([scaled_main, scaled_tail], axis=1)

        sbuf[0, 0, 0:K, :] = scaled[:, 0:LANES].astype(BF16)
        sbuf[0, 0, K : K + 8, :] = packed_tail(scaled[:, LANES:], 8).astype(BF16)
        scaleds.start(0)
    with jax.named_scope("gram_first1"):
        gram_first(0, scaled)

    scaleds.start(1)
    with jax.named_scope("b_left"):
        lo = (scaled - scaled.astype(BF16).astype(F32)).astype(BF16)
        acc[0:K, :] = jnp.dot(lo[:, 0:LANES], aff[0:LANES, :], preferred_element_type=F32) + jnp.dot(
            lo[:, LANES:], aff[4 * LANES : 5 * LANES, :], preferred_element_type=F32
        )
    def second_step(h):
        with jax.named_scope("b_work"):
            vector_tiles(h, sbuf)
            product(h, K)

    scaleds.arrived(0)
    second_step(0)
    scaleds.forwarded(0)
    second_step(1)
    scaleds.arrived(1)
    second_step(2)
    gram_second(0)
    scaleds.forwarded(1)
    with jax.named_scope("b_last"):
        vector_tiles(3, sbuf)
        last_product(1, K)

    eye = (
        lax.broadcasted_iota(jnp.int32, (K, LANES), 0)
        == lax.broadcasted_iota(jnp.int32, (K, LANES), 1)
    ).astype(F32)
    with jax.named_scope("gram_last1"):
        last = gram_last(0)
    with jax.named_scope("eliminate1"):
        inverse = eliminate(last, eye)
    with jax.named_scope("reduce2"):
        total = received_product(1)
    with jax.named_scope("scale2"):
        scaled = jnp.concatenate(
            [total[0:K] / deg_main, unpacked_tail(total[K : K + 16], 2) / deg_tail], axis=1
        )
        tall = jnp.concatenate([scaled, jnp.zeros((LANES - K, 2 * LANES), F32)], axis=0)
        scaled = jnp.dot(inverse, tall, precision=HIGHEST, preferred_element_type=F32)
    with jax.named_scope("gram_first2"):
        gram_first(1, scaled)
    with jax.named_scope("sent"):
        piece = zbuf.at[pl.ds(1, NZ - 1)]
        remote(piece, piece, z_s, z_r.at[0], partner).wait_send()
        points.left(1)
        vectors.left(1)
        for p in range(2):
            scaleds.left(p)
        for gathered in (points, vectors, scaleds):
            gathered.sent()
        for it in range(2):
            p_all(it).wait_send()
        for stage in range(2):
            g_all(0, stage).wait_send()
    with jax.named_scope("gram_second2"):
        gram_second(1)
    with jax.named_scope("gram_last2"):
        g_all(1, 0).wait_send()
        last = gram_last(1)
    with jax.named_scope("eliminate2"):
        ortho = eliminate(last, scaled)
        out_ref[...] = ortho[:, 0:OWN]

    with jax.named_scope("drain"):
        g_all(1, 1).wait_send()


def solution(mesh):
    dma = pltpu.SemaphoreType.DMA

    def shards(points, start_vectors):
        return pl.pallas_call(
            kernel,
            out_shape=jax.ShapeDtypeStruct((K, OWN), F32),
            in_specs=[pl.BlockSpec(memory_space=pltpu.HBM)] * 2,
            out_specs=pl.BlockSpec(memory_space=pltpu.VMEM),
            scratch_shapes=[
                pltpu.VMEM((F, OWN), BF16),
                pltpu.VMEM((K, OWN), BF16),
                pltpu.VMEM((F + K, 2 * LANES), F32),
                pltpu.VMEM((NZ, 80, LANES), BF16),
                pltpu.VMEM((2, NXY, 80, LANES), BF16),
                pltpu.VMEM((2, NXY, K + 8, LANES), BF16),
                pltpu.VMEM((LANES, ROWS_I), BF16),
                pltpu.VMEM((2 * GROUP, LANES), BF16),
                pltpu.VMEM((2 * K, COLS_J), BF16),
                pltpu.VMEM((COLS_J, ROWS_I), BF16),
                pltpu.VMEM((2 * K, ROWS_I), F32),
                pltpu.VMEM((K + 16, LANES), F32),
                pltpu.VMEM((2, NZ, K + 16, LANES), BF16),
                pltpu.VMEM((2, NZ, K + 16, LANES), BF16),
                pltpu.VMEM((2, NXY, K + 8, LANES), BF16),
                pltpu.VMEM((2, 2, 8, LANES), F32),
                pltpu.VMEM((2, 2, 16, 8, LANES), F32),
                dma((2,)),
                dma, dma((NZ,)),
                dma((2,)), dma((2,)), dma((2,)), dma((2,)),
                dma((2,)), dma((2,)), dma((2,)), dma((2,)),
                dma((2,)), dma((2,)),
                dma((2,)), dma((2,)), dma((2,)), dma((2,)),
                dma((2, 2)), dma((2, 2)),
            ],
            compiler_params=pltpu.CompilerParams(
                collective_id=0, has_side_effects=True, vmem_limit_bytes=48 * 1024 * 1024
            ),
        )(*(pltpu.with_memory_space_constraint(v.T, pltpu.HBM) for v in (points, start_vectors))).T

    spec = P(("row", "col"), None)
    return jax.shard_map(
        shards, mesh=mesh, in_specs=(spec, spec), out_specs=spec, check_vma=False
    )
```

```python
import functools
import math

import jax
import jax.numpy as jnp
from jax import lax
from jax.experimental import pallas as pl
from jax.experimental.pallas import tpu as pltpu
from jax.sharding import PartitionSpec as P

MESH = pl.DeviceIdType.MESH
F32 = jnp.float32
BF16 = jnp.bfloat16
HIGHEST = lax.Precision.HIGHEST

KERNEL_SCALE = 5.12
F = 64
K = 32
OWN = 160
LANES = 128
TAIL = OWN - LANES
GROUP = 4 * OWN
NZ = 8
NX = 4
NY = 4
NXY = NX * NY
NCOL = 2 * NZ
FAR_FIRST = (8, 7, 9, 6, 10, 5, 11, 4, 12, 3, 13, 2, 14, 1, 15)
ROWS_I = NZ * OWN
COLS_J = 2 * NXY * OWN
TOTAL = 256 * OWN


def roll_lanes(x, shift):
    shift = shift % LANES
    return x if shift == 0 else pltpu.roll(x, shift, 1)


def pick(blocks, pieces):
    out = pieces[3]
    for b in (2, 1, 0):
        out = jnp.where(blocks == b, pieces[b], out)
    return out


def transposed_blocks(tiles):
    rows = tiles[0].shape[0]
    blocks = lax.broadcasted_iota(jnp.int32, (rows, LANES), 1) // TAIL
    return [
        pick(blocks, [roll_lanes(tiles[b], TAIL * (b - g)) for b in range(4)]) for g in range(4)
    ]


def packed_tail(tail, rows):
    groups = tail.shape[0] // rows
    return sum(roll_lanes(tail[g * rows : (g + 1) * rows], TAIL * g) for g in range(groups))


def unpacked_tail(packed, groups):
    rows = packed.shape[0]
    keep = lax.broadcasted_iota(jnp.int32, (rows, LANES), 1) < TAIL
    return jnp.concatenate(
        [jnp.where(keep, roll_lanes(packed, -TAIL * g), 0.0) for g in range(groups)], axis=0
    )


def bf16_pieces(x):
    hi = x.astype(BF16).astype(F32)
    rest = x - hi
    mid = rest.astype(BF16).astype(F32)
    return hi, mid, rest - mid


def extended(x, for_rows):
    hi, mid, lo = bf16_pieces(jnp.sum(x * x, axis=0, keepdims=True))
    r = lax.broadcasted_iota(jnp.int32, (8, LANES), 0)
    if for_rows:
        x = 2.0 * x
        head = jnp.where(r == 3, -hi, jnp.where(r == 4, -mid, jnp.where(r == 5, -lo, 0.0)))
        extra = jnp.where(r < 3, -1.0, head)
    else:
        head = jnp.where(r == 0, hi, jnp.where(r == 1, mid, jnp.where(r == 2, lo, 0.0)))
        extra = jnp.where((r >= 3) & (r < 6), 1.0, head)
    return jnp.concatenate([x, extra, jnp.zeros((LANES - F - 8, LANES), F32)], axis=0)


def eliminate(gram, right):
    cols = [jnp.broadcast_to(gram[:, m : m + 1], (K, LANES)) for m in range(K)]
    width = right.shape[1] // LANES
    sub = lax.broadcasted_iota(jnp.int32, (8, LANES), 0)
    cols = [[c[8 * g : 8 * g + 8] for g in range(4)] for c in cols]
    rt = [
        [right[8 * g : 8 * g + 8, w * LANES : (w + 1) * LANES] for w in range(width)]
        for g in range(4)
    ]
    out_rows = []
    for k in range(K):
        kg, kr = k // 8, k % 8
        pivot = cols[k][kg][kr : kr + 1]
        inv = 1.0 / pivot
        factor = [None] * 4
        for g in range(kg, 4):
            f = cols[k][g] * inv
            if g == kg:
                f = jnp.where(sub > kr, f, 0.0)
            factor[g] = f
        for m in range(k + 1, K):
            mg, mr = m // 8, m % 8
            upper = cols[k][mg][mr : mr + 1]
            for g in range(mg, 4):
                cols[m][g] = cols[m][g] - factor[g] * upper
        rows = [rt[kg][w][kr : kr + 1] for w in range(width)]
        scale = lax.rsqrt(pivot)
        out_rows.append([row * scale for row in rows])
        for g in range(kg, 4):
            for w in range(width):
                rt[g][w] = rt[g][w] - factor[g] * rows[w]
    tiles = []
    for g in range(4):
        tile = []
        for w in range(width):
            acc = jnp.broadcast_to(out_rows[8 * g][w], (8, LANES))
            for r in range(1, 8):
                acc = jnp.where(sub == r, out_rows[8 * g + r][w], acc)
            tile.append(acc)
        tiles.append(jnp.concatenate(tile, axis=1) if width > 1 else tile[0])
    return jnp.concatenate(tiles, axis=0)


def kernel(
    pts_hbm, vec_hbm, out_ref,
    pts_ref, vec_ref, stage, zbuf, jbuf, vbuf, xi, xj, panel, aff, acc, kept, psend, precv, psend2, precv2, sbuf, gsend, grecv,
    in_s, z_s, z_r, xy_s, xy_r, f_s, f_r, v_s, v_r, vf_s, vf_r,
    p_s, p_r, s_s, s_r, sf_s, sf_r, g_s, g_r,
):
    row = lax.axis_index("row")
    col = lax.axis_index("col")
    x, y = row // NY, lax.rem(row, NY)
    z, core = col // 2, lax.rem(col, 2)

    def xy_peer(e):
        q = e // NY
        to_x = lax.rem(x + q + (q // 2) * (5 - 2 * q), NX)
        to_y = lax.rem(y + e % NY, NY)
        return (to_x * NY + to_y, col)

    def z_peer(d):
        return (row, lax.rem(z + d + NZ, NZ) * 2 + core)

    def col_peer(d):
        return (row, lax.rem(col + d, NCOL))

    partner = (row, z * 2 + 1 - core)

    def remote(src, dst, send, recv, to):
        return pltpu.make_async_remote_copy(
            src_ref=src, dst_ref=dst, send_sem=send, recv_sem=recv,
            device_id=to, device_id_type=MESH,
        )

    pts_copy = pltpu.make_async_copy(pts_hbm, pts_ref, in_s.at[0])
    vec_copy = pltpu.make_async_copy(vec_hbm, vec_ref, in_s.at[1])
    pts_copy.start()
    vec_copy.start()
    barrier = pltpu.get_barrier_semaphore()
    with jax.named_scope("signal"):
        for d in FAR_FIRST:
            pl.semaphore_signal(barrier, inc=1, device_id=col_peer(d), device_id_type=MESH)
        for e in range(NXY - 1, 0, -1):
            pl.semaphore_signal(barrier, inc=1, device_id=xy_peer(e), device_id_type=MESH)

    with jax.named_scope("prepare"):
        stage[...] = jnp.zeros_like(stage)
        pts_copy.wait()
        vec_copy.wait()
        stage[0:F, 0:OWN] = pts_ref[...].astype(F32)
        stage[F : F + K, 0:OWN] = vec_ref[...].astype(F32)
        t = stage[...]
        jbuf[0, 0, 0:64, :] = t[0:F, 0:LANES].astype(BF16)
        jbuf[0, 0, 64:80, :] = packed_tail(t[0:F, LANES:], 16).astype(BF16)
        vbuf[0, 0, 0:32, :] = t[F : F + K, 0:LANES].astype(BF16)
        vbuf[0, 0, K : K + 8, :] = packed_tail(t[F : F + K, LANES:], 8).astype(BF16)
        acc[...] = jnp.zeros_like(acc)
        for h in range(COLS_J // GROUP):
            panel[K : K + 16, h * GROUP : (h + 1) * GROUP] = (
                lax.broadcasted_iota(jnp.int32, (16, GROUP), 0) == 0
            ).astype(F32).astype(BF16)

    with jax.named_scope("barrier_wait"):
        pl.semaphore_wait(barrier, NCOL - 1 + NXY - 1)

    def z_copy(d):
        return remote(jbuf.at[0, 0], zbuf.at[d], z_s, z_r.at[d], z_peer(d))

    class Gathered:
        def __init__(self, buf, send, recv, on_send, on_recv):
            self.buf, self.send, self.recv, self.on_send, self.on_recv = buf, send, recv, on_send, on_recv

        def start(self, p):
            for e in range(max(1, 8 * p), 8 * p + 8):
                remote(
                    self.buf.at[0, 0], self.buf.at[0, e], self.send.at[p], self.recv.at[p], xy_peer(e)
                ).start()

        def piece(self, p):
            first = max(1, 8 * p)
            piece = self.buf.at[0, pl.ds(first, 8 * p + 8 - first)]
            return remote(piece, piece, self.send.at[p], self.recv.at[p], partner)

        def group(self, p):
            pieces = [self.buf.at[half, pl.ds(p * 8, 8)] for half in range(2)]
            return remote(*pieces, self.on_send.at[p], self.on_recv.at[p], partner)

        def arrived(self, p):
            self.piece(p).wait_recv()
            self.group(p).start()

        def forwarded(self, p):
            self.group(p).wait_recv()

        def left(self, p):
            self.piece(p).wait_send()

        def sent(self):
            for p in range(2):
                self.group(p).wait_send()

    points = Gathered(jbuf, xy_s, xy_r, f_s, f_r)
    vectors = Gathered(vbuf, v_s, v_r, vf_s, vf_r)
    scaleds = Gathered(sbuf, s_s, s_r, sf_s, sf_r)

    with jax.named_scope("send_points"):
        for d in (4, 3, 5, 2, 6, 1, 7):
            z_copy(d).start()
        points.start(0)
    with jax.named_scope("left_points"):
        points.left(0)
        vectors.start(0)
        points.start(1)
        vectors.left(0)
        vectors.start(1)

    def tails_of(tiles):
        return transposed_blocks([tile.astype(F32) for tile in tiles])

    with jax.named_scope("first_points"):
        points.arrived(0)

    with jax.named_scope("row_side"):
        for d in (0, 1, 7, 2, 6, 3, 5, 4):
            if d == 0:
                src = jbuf[0, 0, 0:64, :]
            else:
                z_copy(d).wait_recv()
                src = zbuf[d, 0:64, :]
            xi[:, d * LANES : (d + 1) * LANES] = extended(src.astype(F32), True).astype(BF16)
        for q in range(NZ // 4):
            tiles = [
                jbuf[0, 0, 64:80, :] if 4 * q + b == 0 else zbuf[4 * q + b, 64:80, :]
                for b in range(4)
            ]
            tile = jnp.concatenate(tails_of(tiles), axis=0)
            at = NZ * LANES + q * LANES
            xi[:, at : at + LANES] = extended(tile, True).astype(BF16)

    def slots(h, sub):
        return [(h % 2, h // 2 * 8 + sub * 4 + b) for b in range(4)]

    def affinity(h):
        base = pl.multiple_of(h * 2 * GROUP, 2 * GROUP)
        for sub in range(2):
            for b, (core_set, e) in enumerate(slots(h, sub)):
                at = sub * GROUP + b * LANES
                src = jbuf[core_set, e, 0:64, :].astype(F32)
                xj[at : at + LANES, :] = extended(src, False).astype(BF16).T
            at = sub * GROUP + 4 * LANES
            tile = tails_of([jbuf[core_set, e, 64:80, :] for core_set, e in slots(h, sub)])
            xj[at : at + LANES, :] = extended(jnp.concatenate(tile, axis=0), False).astype(BF16).T
        for c in range(ROWS_I // 256):
            here = slice(c * 256, (c + 1) * 256)
            dist = jnp.dot(xj[...], xi[:, here], preferred_element_type=F32)
            weights = jnp.exp2(dist * (KERNEL_SCALE / F * math.log2(math.e)))
            aff[pl.ds(base, 2 * GROUP), here] = weights.astype(BF16)

    def vector_tiles(h, src):
        base = pl.multiple_of(h * 2 * GROUP, 2 * GROUP)
        for sub in range(2):
            for b, (core_set, e) in enumerate(slots(h, sub)):
                at = base + sub * GROUP + b * LANES
                panel[0:K, pl.ds(at, LANES)] = src[core_set, e, 0:K, :]
            tile = tails_of([src[core_set, e, K : K + 8, :] for core_set, e in slots(h, sub)])
            at = base + sub * GROUP + 4 * LANES
            panel[0:K, pl.ds(at, LANES)] = jnp.concatenate(tile, axis=0).astype(BF16)

    def product(h, rows, chunks=range(ROWS_I // 256)):
        base = pl.multiple_of(h * 2 * GROUP, 2 * GROUP)
        for c in chunks:
            here = slice(c * 256, (c + 1) * 256)
            acc[0:rows, here] += jnp.dot(
                panel[0:rows, pl.ds(base, 2 * GROUP)],
                aff[pl.ds(base, 2 * GROUP), here],
                preferred_element_type=F32,
            )

    def first_step(h, carry):
        with jax.named_scope("a_wait"):

            @pl.when(h == 1)
            def _():
                points.forwarded(0)
                vectors.arrived(0)

            @pl.when(h == 2)
            def _():
                points.arrived(1)
                vectors.forwarded(0)

            @pl.when(h == 3)
            def _():
                points.forwarded(1)
                vectors.arrived(1)

        with jax.named_scope("a_work"):
            vector_tiles(h - 1, vbuf)
            product(h - 1, K + 16)
            affinity(h)
        return carry

    with jax.named_scope("a_first"):
        affinity(0)
    lax.fori_loop(1, 4, first_step, 0)
    def p_bufs(it):
        return (psend, precv) if it == 0 else (psend2, precv2)

    def p_copy(it, d):
        src, dst = p_bufs(it)
        return remote(src.at[d], dst.at[d], p_s.at[it], p_r.at[it], z_peer(-d))

    def p_all(it):
        pieces = [buf.at[pl.ds(1, NZ - 1)] for buf in p_bufs(it)]
        return remote(*pieces, p_s.at[it], p_r.at[it], partner)

    blocks16 = lax.broadcasted_iota(jnp.int32, (16, LANES), 1) // TAIL
    rows16 = lax.broadcasted_iota(jnp.int32, (16, LANES), 0)

    def send_piece(it, d):
        b, at = d % 4, NZ * LANES + d // 4 * LANES
        here = slice(d * LANES, (d + 1) * LANES)
        last = jnp.zeros((16, LANES), F32)
        if it == 0:
            hi, mid, _ = bf16_pieces(acc[K : K + 8, here])
            hi_t, mid_t, _ = bf16_pieces(acc[K : K + 8, at : at + LANES])
            lines = [
                roll_lanes(hi_t, TAIL * (2 - b)), roll_lanes(mid_t, TAIL * (2 - b)),
                roll_lanes(hi, 64), hi, roll_lanes(mid, 64), mid,
            ]
            for r, line in enumerate(lines):
                last = jnp.where(rows16 == r, line[0:1], last)
            last = jnp.where(blocks16 == 0, roll_lanes(acc[0:16, at : at + LANES], -TAIL * b), last)
            last = jnp.where(blocks16 == 1, roll_lanes(acc[16:32, at : at + LANES], TAIL * (1 - b)), last)
        else:
            last = pick(
                blocks16[0:8],
                [roll_lanes(acc[8 * g : 8 * g + 8, at : at + LANES], TAIL * (g - b)) for g in range(4)],
            )
        rows = K + last.shape[0]
        if d == 0:
            kept[0:K, :] = acc[0:K, here]
            kept[K:rows, :] = last
        else:
            p_bufs(it)[0][d, 0:K, :] = acc[0:K, here].astype(BF16)
            p_bufs(it)[0][d, K:rows, :] = last.astype(BF16)
            p_copy(it, d).start()

    def last_product(it, rows):
        for chunks, pieces in (((4, 2, 1), (4, 3, 5, 2)), ((3, 0), (6, 7, 1, 0))):
            product(3, rows, chunks)
            for d in pieces:
                send_piece(it, d)

    def received_product(it):
        p_all(it).wait_recv()
        total = kept[0 : K + 16 - 8 * it, :]
        for d in range(1, NZ):
            total = total + p_bufs(it)[1][d].astype(F32)
        return total

    def degree_of(total):
        tail = roll_lanes(total[K : K + 1] + total[K + 1 : K + 2], 64)
        low = roll_lanes(total[K + 2 : K + 3] + total[K + 4 : K + 5], 64)
        high = total[K + 3 : K + 4] + total[K + 5 : K + 6]
        lane = lax.broadcasted_iota(jnp.int32, (1, LANES), 1)
        return jnp.where(lane < 64, low, high), jnp.where(lane < TAIL, tail, 1.0)

    def gram_of(scaled):
        wide = jnp.concatenate([scaled, jnp.zeros((LANES - K, 2 * LANES), F32)], axis=0)
        part = lax.dot_general(
            scaled, wide, (((1,), (1,)), ((), ())), precision=HIGHEST, preferred_element_type=F32
        )
        return packed_tail(part, 8)

    def g_copy(it, stage, n, to):
        return remote(gsend.at[it, stage], grecv.at[it, stage, n], g_s.at[it, stage], g_r.at[it, stage], to)

    def g_all(it, stage):
        piece = grecv.at[it, stage, pl.ds(1, 15)]
        return remote(piece, piece, g_s.at[it, stage], g_r.at[it, stage], partner)

    def g_total(it, stage):
        g_all(it, stage).wait_recv()
        terms = [gsend[it, stage]] + [grecv[it, stage, n] for n in range(1, 16)]
        while len(terms) > 1:
            terms = [a + b for a, b in zip(terms[::2], terms[1::2])]
        return terms[0]

    def gram_first(it, scaled):
        gsend[it, 0] = gram_of(scaled)
        for d in FAR_FIRST:
            g_copy(it, 0, d, col_peer(d)).start()

    def gram_second(it):
        gsend[it, 1] = g_total(it, 0)
        for e in range(NXY - 1, 0, -1):
            g_copy(it, 1, e, xy_peer(e)).start()

    def gram_last(it):
        return unpacked_tail(g_total(it, 1), 4) * (1.0 / TOTAL)

    with jax.named_scope("a_last_wait"):
        vectors.forwarded(1)
    with jax.named_scope("a_last"):
        vector_tiles(3, vbuf)
        last_product(0, K + 16)
    with jax.named_scope("reduce1"):
        total = received_product(0)
    with jax.named_scope("scale1"):
        deg_main, deg_tail = degree_of(total)
        scaled_main = total[0:K] / deg_main
        scaled_tail = unpacked_tail(total[K : K + 16], 2) / deg_tail
        scaled = jnp.concatenate([scaled_main, scaled_tail], axis=1)

        sbuf[0, 0, 0:K, :] = scaled[:, 0:LANES].astype(BF16)
        sbuf[0, 0, K : K + 8, :] = packed_tail(scaled[:, LANES:], 8).astype(BF16)
        scaleds.start(0)
    with jax.named_scope("gram_first1"):
        gram_first(0, scaled)

    scaleds.start(1)
    with jax.named_scope("b_left"):
        lo = (scaled - scaled.astype(BF16).astype(F32)).astype(BF16)
        acc[0:K, :] = jnp.dot(lo[:, 0:LANES], aff[0:LANES, :], preferred_element_type=F32) + jnp.dot(
            lo[:, LANES:], aff[4 * LANES : 5 * LANES, :], preferred_element_type=F32
        )
    def second_step(h):
        with jax.named_scope("b_work"):
            vector_tiles(h, sbuf)
            product(h, K)

    scaleds.arrived(0)
    second_step(0)
    scaleds.forwarded(0)
    second_step(1)
    scaleds.arrived(1)
    second_step(2)
    gram_second(0)
    scaleds.forwarded(1)
    with jax.named_scope("b_last"):
        vector_tiles(3, sbuf)
        last_product(1, K)

    eye = (
        lax.broadcasted_iota(jnp.int32, (K, LANES), 0)
        == lax.broadcasted_iota(jnp.int32, (K, LANES), 1)
    ).astype(F32)
    with jax.named_scope("gram_last1"):
        last = gram_last(0)
    with jax.named_scope("eliminate1"):
        inverse = eliminate(last, eye)
    with jax.named_scope("reduce2"):
        total = received_product(1)
    with jax.named_scope("scale2"):
        scaled = jnp.concatenate(
            [total[0:K] / deg_main, unpacked_tail(total[K : K + 8], 4) / deg_tail], axis=1
        )
        tall = jnp.concatenate([scaled, jnp.zeros((LANES - K, 2 * LANES), F32)], axis=0)
        scaled = jnp.dot(inverse, tall, precision=HIGHEST, preferred_element_type=F32)
    with jax.named_scope("gram_first2"):
        gram_first(1, scaled)
    with jax.named_scope("sent"):
        piece = zbuf.at[pl.ds(1, NZ - 1)]
        remote(piece, piece, z_s, z_r.at[0], partner).wait_send()
        points.left(1)
        vectors.left(1)
        for p in range(2):
            scaleds.left(p)
        for gathered in (points, vectors, scaleds):
            gathered.sent()
        for it in range(2):
            p_all(it).wait_send()
        for stage in range(2):
            g_all(0, stage).wait_send()
    with jax.named_scope("gram_second2"):
        gram_second(1)
    with jax.named_scope("gram_last2"):
        g_all(1, 0).wait_send()
        last = gram_last(1)
    with jax.named_scope("eliminate2"):
        ortho = eliminate(last, scaled)
        out_ref[...] = ortho[:, 0:OWN]

    with jax.named_scope("drain"):
        g_all(1, 1).wait_send()


def solution(mesh):
    dma = pltpu.SemaphoreType.DMA

    def shards(points, start_vectors):
        return pl.pallas_call(
            kernel,
            out_shape=jax.ShapeDtypeStruct((K, OWN), F32),
            in_specs=[pl.BlockSpec(memory_space=pltpu.HBM)] * 2,
            out_specs=pl.BlockSpec(memory_space=pltpu.VMEM),
            scratch_shapes=[
                pltpu.VMEM((F, OWN), BF16),
                pltpu.VMEM((K, OWN), BF16),
                pltpu.VMEM((F + K, 2 * LANES), F32),
                pltpu.VMEM((NZ, 80, LANES), BF16),
                pltpu.VMEM((2, NXY, 80, LANES), BF16),
                pltpu.VMEM((2, NXY, K + 8, LANES), BF16),
                pltpu.VMEM((LANES, ROWS_I), BF16),
                pltpu.VMEM((2 * GROUP, LANES), BF16),
                pltpu.VMEM((2 * K, COLS_J), BF16),
                pltpu.VMEM((COLS_J, ROWS_I), BF16),
                pltpu.VMEM((2 * K, ROWS_I), F32),
                pltpu.VMEM((K + 16, LANES), F32),
                pltpu.VMEM((NZ, K + 16, LANES), BF16),
                pltpu.VMEM((NZ, K + 16, LANES), BF16),
                pltpu.VMEM((NZ, K + 8, LANES), BF16),
                pltpu.VMEM((NZ, K + 8, LANES), BF16),
                pltpu.VMEM((2, NXY, K + 8, LANES), BF16),
                pltpu.VMEM((2, 2, 8, LANES), F32),
                pltpu.VMEM((2, 2, 16, 8, LANES), F32),
                dma((2,)),
                dma, dma((NZ,)),
                dma((2,)), dma((2,)), dma((2,)), dma((2,)),
                dma((2,)), dma((2,)), dma((2,)), dma((2,)),
                dma((2,)), dma((2,)),
                dma((2,)), dma((2,)), dma((2,)), dma((2,)),
                dma((2, 2)), dma((2, 2)),
            ],
            compiler_params=pltpu.CompilerParams(
                collective_id=0, has_side_effects=True, vmem_limit_bytes=48 * 1024 * 1024
            ),
        )(*(pltpu.with_memory_space_constraint(v.T, pltpu.HBM) for v in (points, start_vectors))).T

    spec = P(("row", "col"), None)
    return jax.shard_map(
        shards, mesh=mesh, in_specs=(spec, spec), out_specs=spec, check_vma=False
    )
```
